128 devices in a mesh: grp: 8 (over z, y_lo), slab: 16 (over y_hi, x, core).
Axes of the slice: x: 4, y: 4 (y_hi: 2, y_lo: 2; y = y_hi * 2 + y_lo), z: 4, core: 2. Of those that a mesh axis runs over, the one named last changes fastest.
Arguments:
- orbitals: float32 [16, 96, 9216], P('grp', 'slab'), may hold values from -6 to 6
- occupation: int32 [16], P('grp'), may hold values from 1 to 4
- kernel_hat: float32 [192, 36864], P('slab'), may hold values from 0.02 to 1200, as said below
- pair_mask: int32 [1], replicated, may hold values from 1 to 7
Outputs:
- exchange_terms: float32 [16, 96, 9216], P('grp', 'slab')
The draws below stay inside these ranges and needn't reach their ends.
Inputs may be any that keep to these rules, and one draw needn't show every extreme that they name: In this round group g is paired with group g XOR pair_mask. kernel_hat is positive, and unchanged when each frequency index k is replaced by (192 - k) mod 192 in all three dimensions at once.
All inputs are finite; a program needn't handle non-finite values.
Results may differ from the reference program's by a relative error of at most 0.0001.
Values sent between devices are 32-bit elements; how exact they have to be, the bound alone decides.
No kernel may reach another device: no remote copies, remote signals or barrier semaphores. Data moves between devices by JAX's collectives and lax.ppermute only.
A program may use at most 64 MiB of HBM per device.

```python
import math
import jax
import jax.numpy as jnp
from jax import lax

G = 96
P_SIZE = 192
ORBS = 2
ORBITALS = 16
N_GRP = 8


screening = 0.0025


def draw_kernel_hat(key, part):
    factors = jax.random.uniform(key, (P_SIZE, P_SIZE, P_SIZE), jnp.float32, 0.5, 1.5)
    mirrored = jnp.roll(jnp.flip(factors, (0, 1, 2)), 1, (0, 1, 2))
    even_factors = 0.5 * (factors + mirrored)
    wave_index = jnp.arange(P_SIZE, dtype=jnp.int32)
    folded = jnp.minimum(wave_index, P_SIZE - wave_index).astype(jnp.float32)
    eigen_line = 4.0 * jnp.sin(math.pi * folded / P_SIZE) ** 2
    eigen_sum = eigen_line[:, None, None] + eigen_line[None, :, None] + eigen_line[None, None, :]
    return (even_factors / (eigen_sum + screening)).reshape(P_SIZE, P_SIZE * P_SIZE)


def plant(entries, own_key, smallest, largest):
    spot = [jax.random.randint(jax.random.fold_in(own_key, axis), (), 0, length) for axis, length in enumerate(entries.shape)]
    main_axis = entries.shape.index(max(entries.shape))
    neighbour = spot[:main_axis] + [(spot[main_axis] + 1) % entries.shape[main_axis]] + spot[main_axis + 1:]
    return entries.at[tuple(spot)].set(smallest).at[tuple(neighbour)].set(largest)


def shard_levels(rng, dims, split, least, top_value):
    def one(position, blocks):
        steps = jax.random.uniform(jax.random.fold_in(jax.random.fold_in(rng, 6), position), (blocks,), jnp.float32, least / len(split), top_value / len(split))
        return jnp.repeat(jnp.exp(steps), dims[position] // blocks).reshape((-1,) + (1,) * (len(dims) - position - 1))

    loudness = one(*split[0])
    for cut in split[1:]:
        loudness = loudness * one(*cut)
    return loudness


def scatter_about(rng, dims, scale, reach, cuts=(), kind=jnp.bfloat16):
    level = shard_levels(rng, dims, cuts, -0.22, 0.18) if cuts else 1.0
    array = jax.random.normal(rng, dims, jnp.float32) * scale * level
    return jnp.minimum(jnp.maximum(array, -reach), reach).astype(kind)


def setup_inputs(seed: int = 0) -> dict:
    key_of = jax.random.split(jax.random.key(seed), 5)
    return {
        "orbitals": scatter_about(key_of[0], (ORBITALS, G, G * G), 1.0, 6.0, ((0, 8), (1, 16)), jnp.float32),
        "occupation": plant(jax.random.randint(key_of[1], (ORBITALS,), 1, 5), jax.random.fold_in(key_of[1], 1), 1, 4).astype(jnp.int32),
        "kernel_hat": draw_kernel_hat(jax.random.fold_in(key_of[4], 71), 0),
        "pair_mask": jax.random.randint(key_of[3], (1,), 1, N_GRP).astype(jnp.int32),
    }


def pair_potential(density, kernel_half):
    padded = jnp.pad(density, ((0, G), (0, G), (0, G)))
    spectrum = jnp.fft.rfftn(padded)
    field = jnp.fft.irfftn(spectrum * kernel_half, s=(P_SIZE, P_SIZE, P_SIZE))
    return field[:G, :G, :G]


def reference(orbitals, occupation, kernel_hat, pair_mask):
    fields = orbitals.reshape(N_GRP, ORBS, G, G, G)
    weights = (0.25 * occupation.astype(jnp.float32)).reshape(N_GRP, ORBS)
    kernel_cube = kernel_hat.reshape(P_SIZE, P_SIZE, P_SIZE)
    kernel_half = jnp.transpose(kernel_cube, (2, 1, 0))[:, :, : P_SIZE // 2 + 1]
    pair_bits = pair_mask[0].astype(jnp.int32)
    high_bit = jnp.zeros((), jnp.int32)
    for shift_level in range(1, 31):
        high_bit = high_bit + (jnp.right_shift(pair_bits, shift_level) > 0).astype(jnp.int32)
    low_bits = jnp.left_shift(jnp.ones((), jnp.int32), high_bit) - 1

    def pair_step(flat_index, sums):
        flat_index = flat_index.astype(jnp.int32)
        pair_index = flat_index // (ORBS * ORBS)
        first = (flat_index // ORBS) % ORBS
        second = flat_index % ORBS
        lower_group = jnp.bitwise_or(
            jnp.left_shift(jnp.right_shift(pair_index, high_bit), high_bit + 1),
            jnp.bitwise_and(pair_index, low_bits))
        upper_group = jnp.bitwise_xor(lower_group, pair_bits)
        left_field = fields[lower_group, first]
        right_field = fields[upper_group, second]
        potential = pair_potential(left_field * right_field, kernel_half)
        sums = sums.at[lower_group, first].add(-weights[upper_group, second] * potential * right_field)
        sums = sums.at[upper_group, second].add(-weights[lower_group, first] * potential * left_field)
        return sums

    total_pairs = (N_GRP // 2) * ORBS * ORBS
    sums = lax.fori_loop(0, total_pairs, pair_step, jnp.zeros((N_GRP, ORBS, G, G, G), jnp.float32))
    return sums.reshape(N_GRP * ORBS, G, G * G)
```

```python
import math

import jax
import jax.numpy as jnp
from jax import lax
from jax.sharding import PartitionSpec as P

G = 96


def to_partner(value, pair_bits):
    group_count = lax.axis_size("grp")

    def by_mask(mask):
        pairs = [(source, source ^ mask) for source in range(group_count)]
        return lambda sent: lax.ppermute(sent, "grp", pairs)

    branches = [by_mask(mask) for mask in range(1, group_count)]
    return lax.switch(pair_bits - 1, branches, value)


def dft_tables(size_in, size_out, period):
    row_index = lax.broadcasted_iota(jnp.int32, (size_in, size_out), 0)
    col_index = lax.broadcasted_iota(jnp.int32, (size_in, size_out), 1)
    phase_angle = (row_index * col_index % period).astype(jnp.float32) * (2.0 * math.pi / period)
    return (jnp.cos(phase_angle), jnp.sin(phase_angle))


def contract(form, left, right):
    return jnp.einsum(
        form, left, right, precision=lax.Precision.HIGH, preferred_element_type=jnp.float32
    )


def local(orbitals, occupation, kernel_hat, pair_mask):
    orbit_count = orbitals.shape[0]
    half_count = orbit_count // 2
    plane_count = orbitals.shape[1]
    grid_len = G
    padded_len = 2 * G
    kernel_cube = kernel_hat.reshape(kernel_hat.shape[0], padded_len, padded_len)
    cos_fwd, sin_fwd = dft_tables(grid_len, padded_len, padded_len)
    cos_inv, sin_inv = dft_tables(padded_len, grid_len, padded_len)
    cos_inv = cos_inv / padded_len
    sin_inv = sin_inv / padded_len
    forward_pair = jnp.stack([jnp.stack([cos_fwd, -sin_fwd]), jnp.stack([sin_fwd, cos_fwd])])
    inverse_pair = jnp.stack([jnp.stack([cos_inv, sin_inv]), jnp.stack([-sin_inv, cos_inv])])

    def line_work(pencils):
        y_spectra = contract("nckxy,cdyl->ndkxl", pencils, forward_pair)
        spectra = contract("nckxl,cdxm->ndklm", y_spectra, forward_pair)
        spectra = spectra * kernel_cube[None, None]
        x_back = contract("ncklm,cdmx->ndklx", spectra, inverse_pair)
        return contract("ncklx,cdly->ndkxy", x_back, inverse_pair)

    def packed_potential(density_pair):
        spread = contract("ncxyz,cdzk->ndkxy", density_pair, forward_pair)
        planes = lax.all_to_all(
            line_work(lax.all_to_all(spread, "slab", split_axis=2, concat_axis=3, tiled=True)),
            "slab",
            split_axis=3,
            concat_axis=2,
            tiled=True,
        )
        return contract("nckxy,cdkz->ndxyz", planes, inverse_pair)

    pair_bits = pair_mask[0]
    own_group = lax.axis_index("grp")
    partner_group = jnp.bitwise_xor(own_group, pair_bits)
    upper_side = (own_group > partner_group).astype(jnp.int32)
    weights = 0.25 * occupation.astype(jnp.float32)
    root_weights = jnp.sqrt(weights)
    scaled = orbitals * root_weights[:, None, None]
    theirs = to_partner(scaled, pair_bits)
    paired = theirs
    first = jnp.where(upper_side == 1, theirs[1], theirs[0])
    second = jnp.where(upper_side == 1, theirs[0], theirs[1])
    density_pair = jnp.stack([scaled[0] * first, scaled[1] * second])[None]
    density_pair = density_pair.reshape(half_count, 2, plane_count, grid_len, grid_len)
    fields = packed_potential(density_pair).reshape(2, plane_count, grid_len * grid_len)
    kept_rows = jnp.stack([fields[0] * first, fields[1] * second])
    sent_first = fields[0] * scaled[0]
    sent_second = fields[1] * scaled[1]
    outgoing = jnp.stack(
        [
            jnp.where(upper_side == 1, sent_second, sent_first),
            jnp.where(upper_side == 1, sent_first, sent_second),
        ]
    )
    incoming = to_partner(outgoing, pair_bits)
    return (kept_rows + incoming) * (-1.0 / root_weights)[:, None, None]


def solution(mesh):
    return jax.shard_map(
        local,
        mesh=mesh,
        in_specs=(P("grp", "slab", None), P("grp"), P("slab", None), P()),
        out_specs=P("grp", "slab", None),
        check_vma=False,
    )
```

```python
import functools
import math

import jax
import jax.numpy as jnp
import numpy as np
from jax import lax
from jax.experimental import pallas as pl
from jax.experimental.pallas import tpu as pltpu
from jax.sharding import PartitionSpec as P

G = 96
N = 192
SLABS = 16
XS = 6
KP = 6
ROWS = 112

Y_ORDER = np.array([4 * (i % 24) + i // 24 for i in range(G)])
X_ORDER = np.array([6 * (i % SLABS) + i // SLABS for i in range(G)])


def split(table):
    table = jnp.asarray(table, jnp.float32)
    high = table.astype(jnp.bfloat16)
    low = (table - high.astype(jnp.float32)).astype(jnp.bfloat16)
    return high, low


def np_split(table):
    bf16 = jnp.bfloat16
    high = table.astype(np.float32).astype(bf16)
    low = (table - high.astype(np.float64)).astype(np.float32).astype(bf16)
    return np.stack([high, low])


def waves(freq, cell):
    angle = (np.outer(freq, cell) % N) * (2.0 * math.pi / N)
    return np.cos(angle), np.sin(angle)


@functools.cache
def tables():
    pair_major = np.array([[12 * d + 2 * kp for d in range(SLABS)] for kp in range(KP)]).reshape(-1)
    tz = np.zeros((384, 256))
    tv = np.zeros((256, 384))
    wy = np.zeros((2, 256, 512))
    wi = np.zeros((2, 512, 256))
    for kz2 in range(2):
        cos, sin = waves(pair_major + kz2, np.arange(G))
        re, im = 192 * kz2, 192 * kz2 + 96
        tz[re : re + 96, 0:96], tz[re : re + 96, 128:224] = cos, sin
        tz[im : im + 96, 0:96], tz[im : im + 96, 128:224] = -sin, cos
        tv[0:96, re : re + 96], tv[0:96, im : im + 96] = cos.T / N, -sin.T / N
        tv[128:224, re : re + 96], tv[128:224, im : im + 96] = sin.T / N, cos.T / N
        cos, sin = waves(Y_ORDER, np.arange(N))
        re, im = 64 * kz2, 64 * kz2 + 96
        wy[kz2, re : re + 96, 0:192], wy[kz2, re : re + 96, 256:448] = cos, -sin
        wy[kz2, im : im + 96, 0:192], wy[kz2, im : im + 96, 256:448] = sin, cos
        wi[kz2, 0:192, re : re + 96], wi[kz2, 0:192, im : im + 96] = cos.T / N, sin.T / N
        wi[kz2, 256:448, re : re + 96], wi[kz2, 256:448, im : im + 96] = -sin.T / N, cos.T / N
    cos, sin = waves(np.arange(N), X_ORDER)
    tx = np.block([[cos, sin], [-sin, cos]])
    ti = np.block([[cos.T, -sin.T], [sin.T, cos.T]]) / N
    return [np_split(t) for t in (tz, wy, tx, ti, wi, tv)]


def mm(left, right, form=(1, 0)):
    def one(a, b):
        return lax.dot_general(
            a, b, (((form[0],), (form[1],)), ((), ())), preferred_element_type=jnp.float32
        )

    return one(left[0], right[0]) + (one(left[0], right[1]) + one(left[1], right[0]))


def plane(ref, x, orbital):
    base = 144 * x + orbital
    tiles = [ref[pl.ds(base + 2 * tile, 24, stride=6), :] for tile in range(3)]
    return jnp.concatenate(tiles, axis=1)


def lines(dense):
    return jnp.concatenate([dense[:, 96 * q : 96 * q + 96] for q in range(4)], axis=0)


def dense_of(rows):
    return jnp.concatenate([rows[24 * q : 24 * q + 24] for q in range(4)], axis=1)


def spread_kernel(upper_ref, own_ref, their_ref, tz_ref, out_ref):
    upper = upper_ref[0] == 1
    table = (tz_ref[0], tz_ref[1])
    pad = jnp.zeros((G, 32), jnp.float32)
    for x in range(XS):
        theirs = [plane(their_ref, x, o) for o in range(2)]
        first = jnp.where(upper, theirs[1], theirs[0])
        second = jnp.where(upper, theirs[0], theirs[1])
        one = lines(plane(own_ref, x, 0) * first)
        two = lines(plane(own_ref, x, 1) * second)
        density = jnp.concatenate([one, pad, two, pad], axis=1)
        lined = mm(table, split(density), (1, 1))
        wide = jnp.concatenate([lined[96 * j : 96 * j + 96] for j in range(4)], axis=1)
        for kp in range(KP):
            for tile in range(3):
                out_ref[pl.ds(36 * tile + 6 * x + kp, SLABS, stride=ROWS), :] = wide[
                    16 * kp : 16 * kp + 16, 128 * tile : 128 * tile + 128
                ]


def line_kernel(in_ref, hat_ref, wy_ref, tx_ref, ti_ref, wi_ref, out_ref, y_ref, u_ref):
    pieces = []
    for kp in range(KP):
        for x in range(XS):
            pieces.append(
                jnp.concatenate(
                    [
                        in_ref[pl.ds(36 * tile + 6 * x + kp, SLABS, stride=ROWS), :]
                        for tile in range(3)
                    ],
                    axis=1,
                )
            )
    data = split(jnp.concatenate(pieces, axis=0))
    for kz2 in range(2):
        window = [part[:, 128 * kz2 : 128 * kz2 + 256] for part in data]
        result = mm(window, (wy_ref[0, kz2], wy_ref[1, kz2]))
        for kp in range(KP):
            rows = result[96 * kp : 96 * kp + 96]
            y_ref[2 * kp + kz2] = jnp.concatenate([rows[:, :256], rows[:, 256:]], axis=0)

    def one_frequency(kz, carry):
        lined = split(y_ref[kz])
        spectrum = mm((tx_ref[0], tx_ref[1]), lined)
        hat = hat_ref[kz]
        scaled = jnp.concatenate([spectrum[:N] * hat, spectrum[N:] * hat], axis=0)
        u_ref[kz] = mm((ti_ref[0], ti_ref[1]), split(scaled))
        return carry

    lax.fori_loop(0, 2 * KP, one_frequency, 0)
    sides = []
    for kz2 in range(2):
        rows = [
            jnp.concatenate([u_ref[2 * kp + kz2, :G], u_ref[2 * kp + kz2, G:]], axis=1)
            for kp in range(KP)
        ]
        back = jnp.concatenate(rows, axis=0)
        sides.append(mm(split(back), (wi_ref[0, kz2], wi_ref[1, kz2])))
    wide = [sides[0][:, :128], sides[0][:, 128:] + sides[1][:, :128], sides[1][:, 128:]]
    for kp in range(KP):
        for x in range(XS):
            for tile in range(3):
                row = 96 * kp + 16 * x
                out_ref[pl.ds(36 * tile + 6 * x + kp, SLABS, stride=ROWS), :] = wide[tile][
                    row : row + 16
                ]


def term_kernel(upper_ref, weight_ref, in_ref, own_ref, their_ref, tv_ref, kept_ref, sent_ref):
    upper = upper_ref[0] == 1
    table = (tv_ref[0], tv_ref[1])
    for x in range(XS):
        pieces = [
            jnp.concatenate(
                [
                    in_ref[pl.ds(36 * tile + 6 * x + kp, SLABS, stride=ROWS), :]
                    for tile in range(3)
                ],
                axis=1,
            )
            for kp in range(KP)
        ]
        wide = jnp.concatenate(pieces, axis=0)
        stacked = jnp.concatenate([wide[:, 96 * j : 96 * j + 96] for j in range(4)], axis=0)
        fields = mm(table, split(stacked)).T
        one = dense_of(fields[:, :96])
        two = dense_of(fields[:, 128:224])
        theirs = [plane(their_ref, x, o) for o in range(2)]
        first = jnp.where(upper, theirs[1], theirs[0])
        second = jnp.where(upper, theirs[0], theirs[1])
        kept = [one * first, two * second]
        mine_one = one * plane(own_ref, x, 0) * weight_ref[0]
        mine_two = two * plane(own_ref, x, 1) * weight_ref[1]
        sent = [jnp.where(upper, mine_two, mine_one), jnp.where(upper, mine_one, mine_two)]
        for o in range(2):
            for tile in range(3):
                place = pl.ds(144 * x + o + 2 * tile, 24, stride=6)
                kept_ref[place, :] = kept[o][:, 128 * tile : 128 * tile + 128]
                sent_ref[place, :] = sent[o][:, 128 * tile : 128 * tile + 128]
    row = lax.broadcasted_iota(jnp.int32, (8, 128), 0)
    sent_ref[864:872, :] = jnp.where(row % 2 == 1, weight_ref[1], weight_ref[0])


def sum_kernel(upper_ref, kept_ref, come_ref, out_ref):
    upper = upper_ref[0] == 1
    even = jnp.where(upper, come_ref[865:866, :], come_ref[864:865, :])
    odd = jnp.where(upper, come_ref[864:865, :], come_ref[865:866, :])
    row = lax.broadcasted_iota(jnp.int32, (864, 128), 0)
    weight = jnp.where(row % 2 == 0, even, odd)
    out_ref[...] = -(kept_ref[...] * weight + come_ref[0:864, :])


SMEM = pl.BlockSpec(memory_space=pltpu.SMEM)
VMEM = pl.BlockSpec(memory_space=pltpu.VMEM)


def call(kernel, ins, outs, args, scratch=()):
    shapes = [jax.ShapeDtypeStruct(s, jnp.float32) for s in outs]
    return pl.pallas_call(
        kernel,
        out_shape=shapes if len(shapes) > 1 else shapes[0],
        in_specs=ins,
        out_specs=[VMEM] * len(outs) if len(outs) > 1 else VMEM,
        scratch_shapes=scratch,
        compiler_params=pltpu.CompilerParams(vmem_limit_bytes=48 * 1024 * 1024),
    )(*args)


def to_partner(value, pair_bits):
    group_count = lax.axis_size("grp")

    def by_mask(mask):
        pairs = [(source, source ^ mask) for source in range(group_count)]
        return lambda sent: lax.ppermute(sent, "grp", pairs)

    branches = [by_mask(mask) for mask in range(1, group_count)]
    return lax.switch(pair_bits - 1, branches, value)


def to_rows(planes):
    return planes.reshape(2, XS, 72, 128).transpose(1, 2, 0, 3).reshape(864, 128)


def from_rows(rows):
    return rows.reshape(XS, 72, 2, 128).transpose(2, 0, 1, 3).reshape(2, XS, G * G)


def exchange(chunks):
    chunks = chunks.reshape(SLABS, ROWS, 128)
    moved = lax.all_to_all(chunks, "slab", split_axis=0, concat_axis=0, tiled=True)
    return moved.reshape(SLABS * ROWS, 128)


def local(orbitals, occupation, kernel_hat, pair_mask):
    tz, wy, tx, ti, wi, tv = [jnp.asarray(t) for t in tables()]
    pair_bits = pair_mask[0]
    own_group = lax.axis_index("grp")
    upper = (own_group > jnp.bitwise_xor(own_group, pair_bits)).astype(jnp.int32).reshape(1)
    weights = 0.25 * occupation.astype(jnp.float32)
    own = to_rows(orbitals)
    theirs = to_partner(own, pair_bits)
    chunk = (SLABS * ROWS, 128)
    spread = call(spread_kernel, [SMEM, VMEM, VMEM, VMEM], [chunk], (upper, own, theirs, tz))
    hat = kernel_hat.reshape(2 * KP, N, N).transpose(0, 2, 1)
    hat = jnp.pad(hat, ((0, 0), (0, 0), (0, 256 - N)))
    scratch = [pltpu.VMEM((2 * KP, N, 256), jnp.float32)] * 2
    lined = call(
        line_kernel, [VMEM] * 6, [chunk], (exchange(spread), hat, wy, tx, ti, wi), scratch
    )
    back = exchange(lined)
    kept, sent = call(
        term_kernel,
        [SMEM, SMEM, VMEM, VMEM, VMEM, VMEM],
        [(864, 128), (872, 128)],
        (upper, weights, back, own, theirs, tv),
    )
    come = to_partner(sent, pair_bits)
    return from_rows(call(sum_kernel, [SMEM, VMEM, VMEM], [(864, 128)], (upper, kept, come)))


def solution(mesh):
    return jax.shard_map(
        local,
        mesh=mesh,
        in_specs=(P("grp", "slab", None), P("grp"), P("slab", None), P()),
        out_specs=P("grp", "slab", None),
        check_vma=False,
    )
```

```python
import functools
import math

import jax
import jax.numpy as jnp
import numpy as np
from jax import lax
from jax.experimental import pallas as pl
from jax.experimental.pallas import tpu as pltpu
from jax.sharding import PartitionSpec as P

G = 96
N = 192
SLABS = 16
XS = 6
KP = 6
ROWS = 112

Y_ORDER = np.array([4 * (i % 24) + i // 24 for i in range(G)])
X_ORDER = np.array([6 * (i % SLABS) + i // SLABS for i in range(G)])


WY, WI, TX, TI, LINES = 0, 640, 1664, 2048, 2432


def split(table):
    table = jnp.asarray(table, jnp.float32)
    high = table.astype(jnp.bfloat16)
    low = (table - high.astype(jnp.float32)).astype(jnp.bfloat16)
    return high, low


def np_split(table):
    bf16 = jnp.bfloat16
    high = table.astype(np.float32).astype(bf16)
    low = (table - high.astype(np.float64)).astype(np.float32).astype(bf16)
    return np.stack([high, low])


def waves(freq, cell):
    angle = (np.outer(freq, cell) % N) * (2.0 * math.pi / N)
    return np.cos(angle), np.sin(angle)


@functools.cache
def tables():
    pair_major = np.array([[12 * d + 2 * kp for d in range(SLABS)] for kp in range(KP)]).reshape(-1)
    tz = np.zeros((384, 256))
    tv = np.zeros((256, 384))
    wy = np.zeros((320, 512))
    wi = np.zeros((2, 512, 256))
    for kz2 in range(2):
        cos, sin = waves(pair_major + kz2, np.arange(G))
        re, im = 192 * kz2, 192 * kz2 + 96
        tz[re : re + 96, 0:96], tz[re : re + 96, 128:224] = cos, sin
        tz[im : im + 96, 0:96], tz[im : im + 96, 128:224] = -sin, cos
        tv[0:96, re : re + 96], tv[0:96, im : im + 96] = cos.T / N, -sin.T / N
        tv[128:224, re : re + 96], tv[128:224, im : im + 96] = sin.T / N, cos.T / N
        cos, sin = waves(Y_ORDER, np.arange(N))
        wy[64:160, 0:192], wy[64:160, 256:448] = cos, -sin
        wy[160:256, 0:192], wy[160:256, 256:448] = sin, cos
        re, im = 64 * kz2, 64 * kz2 + 96
        wi[kz2, 0:192, re : re + 96], wi[kz2, 0:192, im : im + 96] = cos.T / N, sin.T / N
        wi[kz2, 256:448, re : re + 96], wi[kz2, 256:448, im : im + 96] = -sin.T / N, cos.T / N
    cos, sin = waves(np.arange(N), X_ORDER)
    tx = np.block([[cos, sin], [-sin, cos]])
    ti = np.block([[cos.T, -sin.T], [sin.T, cos.T]]) / N
    lines = [wy[:, :256], wy[:, 256:], wi[0], wi[1], widened(tx), widened(ti[:, :N]), widened(ti[:, N:])]
    return [np_split(t) for t in (tz, np.concatenate(lines, axis=0), tv)]


def widened(table):
    return np.pad(table, ((0, 0), (0, 256 - N)))


def mm(left, right, form=(1, 0)):
    def one(a, b):
        return lax.dot_general(
            a, b, (((form[0],), (form[1],)), ((), ())), preferred_element_type=jnp.float32
        )

    return one(left[0], right[0]) + (one(left[0], right[1]) + one(left[1], right[0]))


def plane(ref, x, orbital):
    base = 144 * x + orbital
    tiles = [ref[pl.ds(base + 2 * tile, 24, stride=6), :] for tile in range(3)]
    return jnp.concatenate(tiles, axis=1)


def lines(dense):
    return jnp.concatenate([dense[:, 96 * q : 96 * q + 96] for q in range(4)], axis=0)


def dense_of(rows):
    return jnp.concatenate([rows[24 * q : 24 * q + 24] for q in range(4)], axis=1)


def spread_kernel(upper_ref, own_ref, their_ref, tz_ref, out_ref):
    upper = upper_ref[0] == 1
    table = (tz_ref[0], tz_ref[1])
    pad = jnp.zeros((G, 32), jnp.float32)
    for x in range(XS):
        theirs = [plane(their_ref, x, o) for o in range(2)]
        first = jnp.where(upper, theirs[1], theirs[0])
        second = jnp.where(upper, theirs[0], theirs[1])
        one = lines(plane(own_ref, x, 0) * first)
        two = lines(plane(own_ref, x, 1) * second)
        density = jnp.concatenate([one, pad, two, pad], axis=1)
        lined = mm(table, split(density), (1, 1))
        wide = jnp.concatenate([lined[96 * j : 96 * j + 96] for j in range(4)], axis=1)
        for kp in range(KP):
            for tile in range(3):
                out_ref[pl.ds(36 * tile + 6 * x + kp, SLABS, stride=ROWS), :] = wide[
                    16 * kp : 16 * kp + 16, 128 * tile : 128 * tile + 128
                ]


def line_kernel(in_ref, hat_ref, table_ref, out_ref, y_ref, u_ref, hat_vmem, hat_sem):
    fetch = pltpu.make_async_copy(hat_ref, hat_vmem, hat_sem)
    fetch.start()

    def table(row, count, columns=256):
        return [table_ref[part, row : row + count, :columns] for part in range(2)]

    pieces = []
    for kp in range(KP):
        for x in range(XS):
            pieces.append(
                jnp.concatenate(
                    [
                        in_ref[pl.ds(36 * tile + 6 * x + kp, SLABS, stride=ROWS), :]
                        for tile in range(3)
                    ],
                    axis=1,
                )
            )
    data = split(jnp.concatenate(pieces, axis=0))
    for kz2 in range(2):
        window = [part[:, 128 * kz2 : 128 * kz2 + 256] for part in data]
        for c in range(2):
            result = mm(window, table(WY + 320 * c + 64 * (1 - kz2), 256))
            for kp in range(KP):
                y_ref[2 * kp + kz2, 96 * c : 96 * c + 96, :] = result[96 * kp : 96 * kp + 96]
    fetch.wait()
    for kz in range(2 * KP):
        lined = split(y_ref[kz])
        spectrum = mm(table(TX, 384, N), lined)
        hat = hat_vmem[kz]
        u_ref[kz] = mm(table(TI, N, N), split(spectrum[:N] * hat)) + mm(
            table(TI + N, N, N), split(spectrum[N:] * hat)
        )
    sides = []
    for kz2 in range(2):
        rows = [
            jnp.concatenate([u_ref[2 * kp + kz2, :G], u_ref[2 * kp + kz2, G:]], axis=1)
            for kp in range(KP)
        ]
        back = jnp.concatenate(rows, axis=0)
        sides.append(mm(split(back), table(WI + 512 * kz2, 512)))
    wide = [sides[0][:, :128], sides[0][:, 128:] + sides[1][:, :128], sides[1][:, 128:]]
    for kp in range(KP):
        for x in range(XS):
            for tile in range(3):
                row = 96 * kp + 16 * x
                out_ref[pl.ds(36 * tile + 6 * x + kp, SLABS, stride=ROWS), :] = wide[tile][
                    row : row + 16
                ]


def term_kernel(upper_ref, weight_ref, in_ref, own_ref, their_ref, tv_ref, kept_ref, sent_ref):
    upper = upper_ref[0] == 1
    table = (tv_ref[0], tv_ref[1])
    for x in range(XS):
        pieces = [
            jnp.concatenate(
                [
                    in_ref[pl.ds(36 * tile + 6 * x + kp, SLABS, stride=ROWS), :]
                    for tile in range(3)
                ],
                axis=1,
            )
            for kp in range(KP)
        ]
        wide = jnp.concatenate(pieces, axis=0)
        stacked = jnp.concatenate([wide[:, 96 * j : 96 * j + 96] for j in range(4)], axis=0)
        fields = mm(table, split(stacked)).T
        one = dense_of(fields[:, :96])
        two = dense_of(fields[:, 128:224])
        theirs = [plane(their_ref, x, o) for o in range(2)]
        first = jnp.where(upper, theirs[1], theirs[0])
        second = jnp.where(upper, theirs[0], theirs[1])
        kept = [one * first, two * second]
        mine_one = one * plane(own_ref, x, 0) * weight_ref[0]
        mine_two = two * plane(own_ref, x, 1) * weight_ref[1]
        sent = [jnp.where(upper, mine_two, mine_one), jnp.where(upper, mine_one, mine_two)]
        for o in range(2):
            for tile in range(3):
                place = pl.ds(144 * x + o + 2 * tile, 24, stride=6)
                kept_ref[place, :] = kept[o][:, 128 * tile : 128 * tile + 128]
                sent_ref[place, :] = sent[o][:, 128 * tile : 128 * tile + 128]
    row = lax.broadcasted_iota(jnp.int32, (8, 128), 0)
    sent_ref[864:872, :] = jnp.where(row % 2 == 1, weight_ref[1], weight_ref[0])


def sum_kernel(upper_ref, kept_ref, come_ref, out_ref):
    upper = upper_ref[0] == 1
    even = jnp.where(upper, come_ref[865:866, :], come_ref[864:865, :])
    odd = jnp.where(upper, come_ref[864:865, :], come_ref[865:866, :])
    row = lax.broadcasted_iota(jnp.int32, (864, 128), 0)
    weight = jnp.where(row % 2 == 0, even, odd)
    out_ref[...] = -(kept_ref[...] * weight + come_ref[0:864, :])


SMEM = pl.BlockSpec(memory_space=pltpu.SMEM)
VMEM = pl.BlockSpec(memory_space=pltpu.VMEM)
ANY = pl.BlockSpec(memory_space=pl.ANY)


def call(kernel, ins, outs, args, scratch=()):
    shapes = [jax.ShapeDtypeStruct(s, jnp.float32) for s in outs]
    return pl.pallas_call(
        kernel,
        out_shape=shapes if len(shapes) > 1 else shapes[0],
        in_specs=ins,
        out_specs=[VMEM] * len(outs) if len(outs) > 1 else VMEM,
        scratch_shapes=scratch,
        compiler_params=pltpu.CompilerParams(vmem_limit_bytes=48 * 1024 * 1024),
    )(*args)


def to_partner(value, pair_bits):
    group_count = lax.axis_size("grp")

    def by_mask(mask):
        pairs = [(source, source ^ mask) for source in range(group_count)]
        return lambda sent: lax.ppermute(sent, "grp", pairs)

    branches = [by_mask(mask) for mask in range(1, group_count)]
    return lax.switch(pair_bits - 1, branches, value)


def to_rows(planes):
    return planes.reshape(2, XS, 72, 128).transpose(1, 2, 0, 3).reshape(864, 128)


def from_rows(rows):
    return rows.reshape(XS, 72, 2, 128).transpose(2, 0, 1, 3).reshape(2, XS, G * G)


def exchange(chunks):
    chunks = chunks.reshape(SLABS, ROWS, 128)
    moved = lax.all_to_all(chunks, "slab", split_axis=0, concat_axis=0, tiled=True)
    return moved.reshape(SLABS * ROWS, 128)


def local(orbitals, occupation, kernel_hat, pair_mask):
    tz, lines_table, tv = [jnp.asarray(t) for t in tables()]
    pair_bits = pair_mask[0]
    own_group = lax.axis_index("grp")
    upper = (own_group > jnp.bitwise_xor(own_group, pair_bits)).astype(jnp.int32).reshape(1)
    weights = 0.25 * occupation.astype(jnp.float32)
    own = to_rows(orbitals)
    theirs = to_partner(own, pair_bits)
    chunk = (SLABS * ROWS, 128)
    spread = call(spread_kernel, [SMEM, VMEM, VMEM, VMEM], [chunk], (upper, own, theirs, tz))
    hat = kernel_hat.reshape(2 * KP, N, N).transpose(0, 2, 1)
    hat = jnp.pad(hat, ((0, 0), (0, 0), (0, 256 - N)))
    scratch = [pltpu.VMEM((2 * KP, N, 256), jnp.float32)] * 3 + [pltpu.SemaphoreType.DMA]
    lined = call(
        line_kernel, [VMEM, ANY, VMEM], [chunk], (exchange(spread), hat, lines_table), scratch
    )
    back = exchange(lined)
    kept, sent = call(
        term_kernel,
        [SMEM, SMEM, VMEM, VMEM, VMEM, VMEM],
        [(864, 128), (872, 128)],
        (upper, weights, back, own, theirs, tv),
    )
    come = to_partner(sent, pair_bits)
    return from_rows(call(sum_kernel, [SMEM, VMEM, VMEM], [(864, 128)], (upper, kept, come)))


def solution(mesh):
    return jax.shard_map(
        local,
        mesh=mesh,
        in_specs=(P("grp", "slab", None), P("grp"), P("slab", None), P()),
        out_specs=P("grp", "slab", None),
        check_vma=False,
    )
```

```python
import functools
import math

import jax
import jax.numpy as jnp
import numpy as np
from jax import lax
from jax.experimental import pallas as pl
from jax.experimental.pallas import tpu as pltpu
from jax.sharding import PartitionSpec as P

G = 96
N = 192
SLABS = 16
XS = 6
KP = 6
ROWS = 112

Y_ORDER = np.array([4 * (i % 24) + i // 24 for i in range(G)])
X_ORDER = np.array([6 * (i % SLABS) + i // SLABS for i in range(G)])


WY, WI, TX, TI, LINES = 0, 640, 1664, 2048, 2432


def split(table):
    table = jnp.asarray(table, jnp.float32)
    high = table.astype(jnp.bfloat16)
    low = (table - high.astype(jnp.float32)).astype(jnp.bfloat16)
    return high, low


def np_split(table):
    bf16 = jnp.bfloat16
    high = table.astype(np.float32).astype(bf16)
    low = (table - high.astype(np.float64)).astype(np.float32).astype(bf16)
    return np.stack([high, low])


def waves(freq, cell):
    angle = (np.outer(freq, cell) % N) * (2.0 * math.pi / N)
    return np.cos(angle), np.sin(angle)


@functools.cache
def tables():
    pair_major = np.array([[12 * d + 2 * kp for d in range(SLABS)] for kp in range(KP)]).reshape(-1)
    tz = np.zeros((384, 256))
    tv = np.zeros((256, 384))
    wy = np.zeros((320, 512))
    wi = np.zeros((2, 512, 256))
    for kz2 in range(2):
        cos, sin = waves(pair_major + kz2, np.arange(G))
        re, im = 192 * kz2, 192 * kz2 + 96
        tz[re : re + 96, 0:96], tz[re : re + 96, 128:224] = cos, sin
        tz[im : im + 96, 0:96], tz[im : im + 96, 128:224] = -sin, cos
        tv[0:96, re : re + 96], tv[0:96, im : im + 96] = cos.T / N, -sin.T / N
        tv[128:224, re : re + 96], tv[128:224, im : im + 96] = sin.T / N, cos.T / N
        cos, sin = waves(Y_ORDER, np.arange(N))
        wy[64:160, 0:192], wy[64:160, 256:448] = cos, -sin
        wy[160:256, 0:192], wy[160:256, 256:448] = sin, cos
        re, im = 64 * kz2, 64 * kz2 + 96
        wi[kz2, 0:192, re : re + 96], wi[kz2, 0:192, im : im + 96] = cos.T / N, sin.T / N
        wi[kz2, 256:448, re : re + 96], wi[kz2, 256:448, im : im + 96] = -sin.T / N, cos.T / N
    cos, sin = waves(np.arange(N), X_ORDER)
    tx = np.block([[cos, sin], [-sin, cos]])
    ti = np.block([[cos.T, -sin.T], [sin.T, cos.T]]) / N
    lines = [wy[:, :256], wy[:, 256:], wi[0], wi[1], widened(tx), widened(ti[:, :N]), widened(ti[:, N:])]
    return [np_split(t) for t in (tz, np.concatenate(lines, axis=0), tv)]


def widened(table):
    return np.pad(table, ((0, 0), (0, 256 - N)))


def mm(left, right, form=(1, 0)):
    def one(a, b):
        return lax.dot_general(
            a, b, (((form[0],), (form[1],)), ((), ())), preferred_element_type=jnp.float32
        )

    return one(left[0], right[0]) + (one(left[0], right[1]) + one(left[1], right[0]))


def plane(ref, x, orbital):
    base = 144 * x + orbital
    tiles = [ref[pl.ds(base + 2 * tile, 24, stride=6), :] for tile in range(3)]
    return jnp.concatenate(tiles, axis=1)


def lines(dense):
    return jnp.concatenate([dense[:, 96 * q : 96 * q + 96] for q in range(4)], axis=0)


def dense_of(rows):
    return jnp.concatenate([rows[24 * q : 24 * q + 24] for q in range(4)], axis=1)


def spread_kernel(
    upper_ref, own_hbm, their_hbm, tz_hbm, out_hbm, own_ref, their_ref, tz_ref, out_ref, sems
):
    table_in = pltpu.make_async_copy(tz_hbm, tz_ref, sems.at[0])
    table_in.start()
    halves = []
    for half in range(2):
        rows = pl.ds(432 * half, 432)
        for k, (hbm, ref) in enumerate(((their_hbm, their_ref), (own_hbm, own_ref))):
            halves.append(
                pltpu.make_async_copy(hbm.at[rows], ref.at[rows], sems.at[1 + 2 * half + k])
            )
            halves[-1].start()
    upper = upper_ref[0] == 1
    pad = jnp.zeros((G, 32), jnp.float32)
    outs = []
    for x in range(XS):
        if x % 3 == 0:
            for copy in halves[2 * (x // 3) : 2 * (x // 3) + 2]:
                copy.wait()
        theirs = [plane(their_ref, x, o) for o in range(2)]
        first = jnp.where(upper, theirs[1], theirs[0])
        second = jnp.where(upper, theirs[0], theirs[1])
        one = lines(plane(own_ref, x, 0) * first)
        two = lines(plane(own_ref, x, 1) * second)
        density = jnp.concatenate([one, pad, two, pad], axis=1)
        if x == 0:
            table_in.wait()
        lined = mm((tz_ref[0], tz_ref[1]), split(density), (1, 1))
        wide = jnp.concatenate([lined[96 * j : 96 * j + 96] for j in range(4)], axis=1)
        for kp in range(KP):
            for tile in range(3):
                out_ref[pl.ds(18 * x + 6 * tile + kp, SLABS, stride=ROWS), :] = wide[
                    16 * kp : 16 * kp + 16, 128 * tile : 128 * tile + 128
                ]
        if x in (3, 5):
            first_row, count = (0, 72) if x == 3 else (72, 40)
            if x == 5:
                for slab in range(SLABS):
                    out_ref[ROWS * slab + 108 : ROWS * slab + 112, :] = jnp.zeros((4, 128), jnp.float32)
            for slab in range(SLABS):
                place = pl.ds(ROWS * slab + first_row, count)
                outs.append(
                    pltpu.make_async_copy(out_ref.at[place], out_hbm.at[place], sems.at[5 + len(outs)])
                )
                outs[-1].start()
    for copy in outs:
        copy.wait()


def line_kernel(in_ref, hat_ref, table_hbm, out_ref, y_ref, u_ref, table_ref, sems):
    parts = ((WY, WI - WY), (TX, LINES - TX), (WI, TX - WI))
    fetches = []
    for k, (row, count) in enumerate(parts):
        place = (slice(None), pl.ds(row, count))
        fetches.append(pltpu.make_async_copy(table_hbm.at[place], table_ref.at[place], sems.at[k]))
        fetches[-1].start()
    def table(row, count, columns=256):
        return [table_ref[part, row : row + count, :columns] for part in range(2)]

    pieces = []
    for kp in range(KP):
        for x in range(XS):
            pieces.append(
                jnp.concatenate(
                    [
                        in_ref[pl.ds(18 * x + 6 * tile + kp, SLABS, stride=ROWS), :]
                        for tile in range(3)
                    ],
                    axis=1,
                )
            )
    data = split(jnp.concatenate(pieces, axis=0))
    fetches[0].wait()
    for kz2 in range(2):
        window = [part[:, 128 * kz2 : 128 * kz2 + 256] for part in data]
        for c in range(2):
            result = mm(window, table(WY + 320 * c + 64 * (1 - kz2), 256))
            for kp in range(KP):
                y_ref[2 * kp + kz2, 96 * c : 96 * c + 96, :] = result[96 * kp : 96 * kp + 96]
    fetches[1].wait()
    for kz in range(2 * KP):
        lined = split(y_ref[kz])
        spectrum = mm(table(TX, 384, N), lined)
        hat = hat_ref[kz]
        u_ref[kz] = mm(table(TI, N, N), split(spectrum[:N] * hat)) + mm(
            table(TI + N, N, N), split(spectrum[N:] * hat)
        )
    fetches[2].wait()
    sides = []
    for kz2 in range(2):
        rows = [
            jnp.concatenate([u_ref[2 * kp + kz2, :G], u_ref[2 * kp + kz2, G:]], axis=1)
            for kp in range(KP)
        ]
        back = jnp.concatenate(rows, axis=0)
        sides.append(mm(split(back), table(WI + 512 * kz2, 512)))
    wide = [sides[0][:, :128], sides[0][:, 128:] + sides[1][:, :128], sides[1][:, 128:]]
    for kp in range(KP):
        for x in range(XS):
            for tile in range(3):
                row = 96 * kp + 16 * x
                out_ref[pl.ds(18 * x + 6 * tile + kp, SLABS, stride=ROWS), :] = wide[tile][
                    row : row + 16
                ]


def term_kernel(
    upper_ref, occupation_ref, in_ref, own_ref, their_hbm, tv_ref, kept_ref, sent_ref, their_ref, sem
):
    fetch = pltpu.make_async_copy(their_hbm, their_ref, sem)
    fetch.start()
    upper = upper_ref[0] == 1
    table = (tv_ref[0], tv_ref[1])
    weight = [0.25 * occupation_ref[o].astype(jnp.float32) for o in range(2)]
    for x in range(XS):
        pieces = [
            jnp.concatenate(
                [
                    in_ref[pl.ds(18 * x + 6 * tile + kp, SLABS, stride=ROWS), :]
                    for tile in range(3)
                ],
                axis=1,
            )
            for kp in range(KP)
        ]
        wide = jnp.concatenate(pieces, axis=0)
        stacked = jnp.concatenate([wide[:, 96 * j : 96 * j + 96] for j in range(4)], axis=0)
        fields = mm(table, split(stacked)).T
        one = dense_of(fields[:, :96])
        two = dense_of(fields[:, 128:224])
        if x == 0:
            fetch.wait()
        theirs = [plane(their_ref, x, o) for o in range(2)]
        first = jnp.where(upper, theirs[1], theirs[0])
        second = jnp.where(upper, theirs[0], theirs[1])
        kept = [one * first, two * second]
        mine_one = one * plane(own_ref, x, 0) * weight[0]
        mine_two = two * plane(own_ref, x, 1) * weight[1]
        sent = [jnp.where(upper, mine_two, mine_one), jnp.where(upper, mine_one, mine_two)]
        for o in range(2):
            for tile in range(3):
                place = pl.ds(144 * x + o + 2 * tile, 24, stride=6)
                kept_ref[place, :] = kept[o][:, 128 * tile : 128 * tile + 128]
                sent_ref[place, :] = sent[o][:, 128 * tile : 128 * tile + 128]
    row = lax.broadcasted_iota(jnp.int32, (8, 128), 0)
    sent_ref[864:872, :] = jnp.where(row % 2 == 1, weight[1], weight[0])


PARTS = ((864, 8), (0, 216), (216, 216), (432, 216), (648, 216))


def sum_kernel(upper_ref, kept_ref, come_hbm, out_hbm, come_ref, out_ref, sems):
    fetches, outs = [], []
    for k, (row, count) in enumerate(PARTS):
        place = pl.ds(row, count)
        fetches.append(pltpu.make_async_copy(come_hbm.at[place], come_ref.at[place], sems.at[k]))
        fetches[-1].start()
    upper = upper_ref[0] == 1
    odd_row = lax.broadcasted_iota(jnp.int32, (216, 128), 0) % 2 == 1
    fetches[0].wait()
    even = jnp.where(upper, come_ref[865:866, :], come_ref[864:865, :])
    odd = jnp.where(upper, come_ref[864:865, :], come_ref[865:866, :])
    weight = jnp.where(odd_row, odd, even)
    for k, (row, count) in enumerate(PARTS[1:], 1):
        place = pl.ds(row, count)
        fetches[k].wait()
        out_ref[place, :] = -(kept_ref[place, :] * weight + come_ref[place, :])
        outs.append(pltpu.make_async_copy(out_ref.at[place], out_hbm.at[place], sems.at[4 + k]))
        outs[-1].start()
    for copy in outs:
        copy.wait()


SMEM = pl.BlockSpec(memory_space=pltpu.SMEM)
VMEM = pl.BlockSpec(memory_space=pltpu.VMEM)
HBM = pl.BlockSpec(memory_space=pltpu.HBM)


def call(kernel, ins, outs, args, scratch=(), out_spec=VMEM, limit=28_000_000):
    shapes = [o if isinstance(o, jax.ShapeDtypeStruct) else jax.ShapeDtypeStruct(o, jnp.float32) for o in outs]
    many = len(shapes) > 1
    return pl.pallas_call(
        kernel,
        out_shape=shapes if many else shapes[0],
        in_specs=ins,
        out_specs=[out_spec] * len(outs) if many else out_spec,
        scratch_shapes=scratch,
        compiler_params=pltpu.CompilerParams(vmem_limit_bytes=limit),
    )(*args)


def to_partner(value, pair_bits):
    group_count = lax.axis_size("grp")

    def by_mask(mask):
        pairs = [(source, source ^ mask) for source in range(group_count)]
        return lambda sent: lax.ppermute(sent, "grp", pairs)

    branches = [by_mask(mask) for mask in range(1, group_count)]
    return lax.switch(pair_bits - 1, branches, value)


def to_rows(planes):
    return planes.reshape(2, XS, 72, 128).transpose(1, 2, 0, 3).reshape(864, 128)


def from_rows(rows):
    return rows.reshape(XS, 72, 2, 128).transpose(2, 0, 1, 3).reshape(2, XS, G * G)


def exchange(chunks):
    chunks = chunks.reshape(SLABS, ROWS, 128)
    moved = lax.all_to_all(chunks, "slab", split_axis=0, concat_axis=0, tiled=True)
    return moved.reshape(SLABS * ROWS, 128)


def local(orbitals, occupation, kernel_hat, pair_mask):
    tz, lines_table, tv = [jnp.asarray(t) for t in tables()]
    pair_bits = pair_mask[0]
    own_group = lax.axis_index("grp")
    upper = (own_group > jnp.bitwise_xor(own_group, pair_bits)).astype(jnp.int32).reshape(1)
    own = to_rows(orbitals)
    theirs = to_partner(own, pair_bits)
    chunk = (SLABS * ROWS, 128)
    rows = pltpu.VMEM((864, 128), jnp.float32)
    spread = call(
        spread_kernel,
        [SMEM, HBM, HBM, HBM],
        [chunk],
        (upper, own, theirs, tz),
        [rows, rows, pltpu.VMEM(tz.shape, tz.dtype), pltpu.VMEM(chunk, jnp.float32)]
        + [pltpu.SemaphoreType.DMA((5 + 2 * SLABS,))],
        HBM,
        66_800_000,
    )
    hat = kernel_hat.reshape(2 * KP, N, N).transpose(0, 2, 1)
    hat = jnp.pad(hat, ((0, 0), (0, 0), (0, 256 - N)))
    scratch = [pltpu.VMEM((2 * KP, N, 256), jnp.float32)] * 2
    scratch += [pltpu.VMEM(lines_table.shape, lines_table.dtype), pltpu.SemaphoreType.DMA((3,))]
    lined = call(
        line_kernel,
        [VMEM, VMEM, HBM],
        [chunk],
        (exchange(spread), hat, lines_table),
        scratch,
        limit=62_500_000,
    )
    back = exchange(lined)
    kept, sent = call(
        term_kernel,
        [SMEM, SMEM, VMEM, VMEM, HBM, VMEM],
        [(864, 128), (872, 128)],
        (upper, occupation, back, own, theirs, tv),
        [rows, pltpu.SemaphoreType.DMA],
    )

    come = to_partner(sent, pair_bits)
    scratch = [pltpu.VMEM((872, 128), jnp.float32), rows, pltpu.SemaphoreType.DMA((9,))]
    total = call(sum_kernel, [SMEM, VMEM, HBM], [(864, 128)], (upper, kept, come), scratch, HBM)
    return from_rows(total)


def solution(mesh):
    return jax.shard_map(
        local,
        mesh=mesh,
        in_specs=(P("grp", "slab", None), P("grp"), P("slab", None), P()),
        out_specs=P("grp", "slab", None),
        check_vma=False,
    )
```

```python
import functools
import math

import jax
import jax.numpy as jnp
import numpy as np
from jax import lax
from jax.experimental import pallas as pl
from jax.experimental.pallas import tpu as pltpu
from jax.sharding import PartitionSpec as P

G = 96
N = 192
SLABS = 16
XS = 6
KP = 6
ROWS = 112

Y_ORDER = np.array([4 * (i % 24) + i // 24 for i in range(G)])
X_ORDER = np.array([6 * (i % SLABS) + i // SLABS for i in range(G)])


WY, WI, TX, TI, LINES = 0, 640, 1664, 2048, 2432


def split(table):
    table = jnp.asarray(table, jnp.float32)
    high = table.astype(jnp.bfloat16)
    low = (table - high.astype(jnp.float32)).astype(jnp.bfloat16)
    return high, low


def np_split(table):
    bf16 = jnp.bfloat16
    high = table.astype(np.float32).astype(bf16)
    low = (table - high.astype(np.float64)).astype(np.float32).astype(bf16)
    return np.stack([high, low])


def waves(freq, cell):
    angle = (np.outer(freq, cell) % N) * (2.0 * math.pi / N)
    return np.cos(angle), np.sin(angle)


@functools.cache
def tables():
    pair_major = np.array([[12 * d + 2 * kp for d in range(SLABS)] for kp in range(KP)]).reshape(-1)
    tz = np.zeros((384, 256))
    tv = np.zeros((256, 384))
    wy = np.zeros((320, 512))
    wi = np.zeros((2, 512, 256))
    for kz2 in range(2):
        cos, sin = waves(pair_major + kz2, np.arange(G))
        re, im = 192 * kz2, 192 * kz2 + 96
        tz[re : re + 96, 0:96], tz[re : re + 96, 128:224] = cos, sin
        tz[im : im + 96, 0:96], tz[im : im + 96, 128:224] = -sin, cos
        tv[0:96, re : re + 96], tv[0:96, im : im + 96] = cos.T / N, -sin.T / N
        tv[128:224, re : re + 96], tv[128:224, im : im + 96] = sin.T / N, cos.T / N
        cos, sin = waves(Y_ORDER, np.arange(N))
        wy[64:160, 0:192], wy[64:160, 256:448] = cos, -sin
        wy[160:256, 0:192], wy[160:256, 256:448] = sin, cos
        re, im = 64 * kz2, 64 * kz2 + 96
        wi[kz2, 0:192, re : re + 96], wi[kz2, 0:192, im : im + 96] = cos.T / N, sin.T / N
        wi[kz2, 256:448, re : re + 96], wi[kz2, 256:448, im : im + 96] = -sin.T / N, cos.T / N
    cos, sin = waves(np.arange(N), X_ORDER)
    tx = np.block([[cos, sin], [-sin, cos]])
    ti = np.block([[cos.T, -sin.T], [sin.T, cos.T]]) / N
    lines = [wy[:, :256], wy[:, 256:], wi[0], wi[1], widened(tx), widened(ti[:, :N]), widened(ti[:, N:])]
    return [np_split(t) for t in (tz, np.concatenate(lines, axis=0), tv)]


def widened(table):
    return np.pad(table, ((0, 0), (0, 256 - N)))


def mm(left, right, form=(1, 0)):
    def one(a, b):
        return lax.dot_general(
            a, b, (((form[0],), (form[1],)), ((), ())), preferred_element_type=jnp.float32
        )

    return one(left[0], right[0]) + (one(left[0], right[1]) + one(left[1], right[0]))


def plane(ref, x, orbital):
    base = 144 * x + orbital
    tiles = [ref[pl.ds(base + 2 * tile, 24, stride=6), :] for tile in range(3)]
    return jnp.concatenate(tiles, axis=1)


def lines(dense):
    return jnp.concatenate([dense[:, 96 * q : 96 * q + 96] for q in range(4)], axis=0)


def dense_of(rows):
    return jnp.concatenate([rows[24 * q : 24 * q + 24] for q in range(4)], axis=1)


def spread_kernel(
    upper_ref, own_hbm, their_hbm, tz_hbm, out_hbm, own_ref, their_ref, tz_ref, out_ref, sems
):
    table_in = pltpu.make_async_copy(tz_hbm, tz_ref, sems.at[0])
    table_in.start()
    halves = []
    for half in range(2):
        rows = pl.ds(432 * half, 432)
        for k, (hbm, ref) in enumerate(((their_hbm, their_ref), (own_hbm, own_ref))):
            halves.append(
                pltpu.make_async_copy(hbm.at[rows], ref.at[rows], sems.at[1 + 2 * half + k])
            )
            halves[-1].start()
    upper = upper_ref[0] == 1
    pad = jnp.zeros((G, 32), jnp.float32)
    outs = []
    for x in range(XS):
        if x % 3 == 0:
            for copy in halves[2 * (x // 3) : 2 * (x // 3) + 2]:
                copy.wait()
        theirs = [plane(their_ref, x, o) for o in range(2)]
        first = jnp.where(upper, theirs[1], theirs[0])
        second = jnp.where(upper, theirs[0], theirs[1])
        one = lines(plane(own_ref, x, 0) * first)
        two = lines(plane(own_ref, x, 1) * second)
        density = jnp.concatenate([one, pad, two, pad], axis=1)
        if x == 0:
            table_in.wait()
        lined = mm((tz_ref[0], tz_ref[1]), split(density), (1, 1))
        wide = jnp.concatenate([lined[96 * j : 96 * j + 96] for j in range(4)], axis=1)
        for kp in range(KP):
            for tile in range(3):
                out_ref[pl.ds(18 * x + 6 * tile + kp, SLABS, stride=ROWS), :] = wide[
                    16 * kp : 16 * kp + 16, 128 * tile : 128 * tile + 128
                ]
        if x in (3, 5):
            first_row, count = (0, 72) if x == 3 else (72, 40)
            if x == 5:
                for slab in range(SLABS):
                    out_ref[ROWS * slab + 108 : ROWS * slab + 112, :] = jnp.zeros((4, 128), jnp.float32)
            for slab in range(SLABS):
                place = pl.ds(ROWS * slab + first_row, count)
                outs.append(
                    pltpu.make_async_copy(out_ref.at[place], out_hbm.at[place], sems.at[5 + len(outs)])
                )
                outs[-1].start()
    for copy in outs:
        copy.wait()


def line_kernel(in_ref, hat_hbm, table_hbm, out_ref, y_ref, u_ref, hat_ref, table_ref, sems):
    parts = ((WY, WI - WY), (TX, LINES - TX), (WI, TX - WI))
    fetches = []
    for k, (row, count) in enumerate(parts):
        place = (slice(None), pl.ds(row, count))
        fetches.append(pltpu.make_async_copy(table_hbm.at[place], table_ref.at[place], sems.at[k]))
        fetches[-1].start()
    def table(row, count, columns=256):
        return [table_ref[part, row : row + count, :columns] for part in range(2)]

    hats = []
    for k in range(4):
        place = pl.ds(3 * k, 3)
        hats.append(pltpu.make_async_copy(hat_hbm.at[place], hat_ref.at[place], sems.at[3 + k]))
        hats[-1].start()
    pieces = []
    for kp in range(KP):
        for x in range(XS):
            pieces.append(
                jnp.concatenate(
                    [
                        in_ref[pl.ds(18 * x + 6 * tile + kp, SLABS, stride=ROWS), :]
                        for tile in range(3)
                    ],
                    axis=1,
                )
            )
    data = split(jnp.concatenate(pieces, axis=0))
    fetches[0].wait()
    for kz2 in range(2):
        window = [part[:, 128 * kz2 : 128 * kz2 + 256] for part in data]
        for c in range(2):
            result = mm(window, table(WY + 320 * c + 64 * (1 - kz2), 256))
            for kp in range(KP):
                y_ref[2 * kp + kz2, 96 * c : 96 * c + 96, :] = result[96 * kp : 96 * kp + 96]
    fetches[1].wait()
    for kz in range(2 * KP):
        if kz % 3 == 0:
            hats[kz // 3].wait()
        lined = split(y_ref[kz])
        spectrum = mm(table(TX, 384, N), lined)
        hat = hat_ref[kz]
        u_ref[kz] = mm(table(TI, N, N), split(spectrum[:N] * hat)) + mm(
            table(TI + N, N, N), split(spectrum[N:] * hat)
        )
    fetches[2].wait()
    sides = []
    for kz2 in range(2):
        rows = [
            jnp.concatenate([u_ref[2 * kp + kz2, :G], u_ref[2 * kp + kz2, G:]], axis=1)
            for kp in range(KP)
        ]
        back = jnp.concatenate(rows, axis=0)
        sides.append(mm(split(back), table(WI + 512 * kz2, 512)))
    wide = [sides[0][:, :128], sides[0][:, 128:] + sides[1][:, :128], sides[1][:, 128:]]
    for kp in range(KP):
        for x in range(XS):
            for tile in range(3):
                row = 96 * kp + 16 * x
                out_ref[pl.ds(18 * x + 6 * tile + kp, SLABS, stride=ROWS), :] = wide[tile][
                    row : row + 16
                ]


def term_kernel(
    upper_ref, occupation_ref, in_ref, own_ref, their_hbm, tv_ref, kept_ref, sent_ref, their_ref, sem
):
    fetch = pltpu.make_async_copy(their_hbm, their_ref, sem)
    fetch.start()
    upper = upper_ref[0] == 1
    table = (tv_ref[0], tv_ref[1])
    weight = [0.25 * occupation_ref[o].astype(jnp.float32) for o in range(2)]
    for x in range(XS):
        pieces = [
            jnp.concatenate(
                [
                    in_ref[pl.ds(18 * x + 6 * tile + kp, SLABS, stride=ROWS), :]
                    for tile in range(3)
                ],
                axis=1,
            )
            for kp in range(KP)
        ]
        wide = jnp.concatenate(pieces, axis=0)
        stacked = jnp.concatenate([wide[:, 96 * j : 96 * j + 96] for j in range(4)], axis=0)
        fields = mm(table, split(stacked)).T
        one = dense_of(fields[:, :96])
        two = dense_of(fields[:, 128:224])
        if x == 0:
            fetch.wait()
        theirs = [plane(their_ref, x, o) for o in range(2)]
        first = jnp.where(upper, theirs[1], theirs[0])
        second = jnp.where(upper, theirs[0], theirs[1])
        kept = [one * first, two * second]
        mine_one = one * plane(own_ref, x, 0) * weight[0]
        mine_two = two * plane(own_ref, x, 1) * weight[1]
        sent = [jnp.where(upper, mine_two, mine_one), jnp.where(upper, mine_one, mine_two)]
        for o in range(2):
            for tile in range(3):
                place = pl.ds(144 * x + o + 2 * tile, 24, stride=6)
                kept_ref[place, :] = kept[o][:, 128 * tile : 128 * tile + 128]
                sent_ref[place, :] = sent[o][:, 128 * tile : 128 * tile + 128]
    row = lax.broadcasted_iota(jnp.int32, (8, 128), 0)
    sent_ref[864:872, :] = jnp.where(row % 2 == 1, weight[1], weight[0])


PARTS = ((864, 8), (0, 216), (216, 216), (432, 216), (648, 216))


def sum_kernel(upper_ref, kept_ref, come_hbm, out_hbm, come_ref, out_ref, sems):
    fetches, outs = [], []
    for k, (row, count) in enumerate(PARTS):
        place = pl.ds(row, count)
        fetches.append(pltpu.make_async_copy(come_hbm.at[place], come_ref.at[place], sems.at[k]))
        fetches[-1].start()
    upper = upper_ref[0] == 1
    odd_row = lax.broadcasted_iota(jnp.int32, (216, 128), 0) % 2 == 1
    fetches[0].wait()
    even = jnp.where(upper, come_ref[865:866, :], come_ref[864:865, :])
    odd = jnp.where(upper, come_ref[864:865, :], come_ref[865:866, :])
    weight = jnp.where(odd_row, odd, even)
    for k, (row, count) in enumerate(PARTS[1:], 1):
        place = pl.ds(row, count)
        fetches[k].wait()
        out_ref[place, :] = -(kept_ref[place, :] * weight + come_ref[place, :])
        outs.append(pltpu.make_async_copy(out_ref.at[place], out_hbm.at[place], sems.at[4 + k]))
        outs[-1].start()
    for copy in outs:
        copy.wait()


SMEM = pl.BlockSpec(memory_space=pltpu.SMEM)
VMEM = pl.BlockSpec(memory_space=pltpu.VMEM)
HBM = pl.BlockSpec(memory_space=pltpu.HBM)


def call(kernel, ins, outs, args, scratch=(), out_spec=VMEM, limit=28_000_000):
    shapes = [o if isinstance(o, jax.ShapeDtypeStruct) else jax.ShapeDtypeStruct(o, jnp.float32) for o in outs]
    many = len(shapes) > 1
    return pl.pallas_call(
        kernel,
        out_shape=shapes if many else shapes[0],
        in_specs=ins,
        out_specs=[out_spec] * len(outs) if many else out_spec,
        scratch_shapes=scratch,
        compiler_params=pltpu.CompilerParams(vmem_limit_bytes=limit),
    )(*args)


def to_partner(value, pair_bits):
    group_count = lax.axis_size("grp")

    def by_mask(mask):
        pairs = [(source, source ^ mask) for source in range(group_count)]
        return lambda sent: lax.ppermute(sent, "grp", pairs)

    branches = [by_mask(mask) for mask in range(1, group_count)]
    return lax.switch(pair_bits - 1, branches, value)


def to_rows(planes):
    return planes.reshape(2, XS, 72, 128).transpose(1, 2, 0, 3).reshape(864, 128)


def from_rows(rows):
    return rows.reshape(XS, 72, 2, 128).transpose(2, 0, 1, 3).reshape(2, XS, G * G)


def exchange(chunks):
    chunks = chunks.reshape(SLABS, ROWS, 128)
    moved = lax.all_to_all(chunks, "slab", split_axis=0, concat_axis=0, tiled=True)
    return moved.reshape(SLABS * ROWS, 128)


def local(orbitals, occupation, kernel_hat, pair_mask):
    tz, lines_table, tv = [jnp.asarray(t) for t in tables()]
    pair_bits = pair_mask[0]
    own_group = lax.axis_index("grp")
    upper = (own_group > jnp.bitwise_xor(own_group, pair_bits)).astype(jnp.int32).reshape(1)
    own = to_rows(orbitals)
    theirs = to_partner(own, pair_bits)
    chunk = (SLABS * ROWS, 128)
    rows = pltpu.VMEM((864, 128), jnp.float32)
    spread = call(
        spread_kernel,
        [SMEM, HBM, HBM, HBM],
        [chunk],
        (upper, own, theirs, tz),
        [rows, rows, pltpu.VMEM(tz.shape, tz.dtype), pltpu.VMEM(chunk, jnp.float32)]
        + [pltpu.SemaphoreType.DMA((5 + 2 * SLABS,))],
        HBM,
        66_800_000,
    )
    hat = kernel_hat.reshape(2 * KP, N, N).transpose(0, 2, 1)
    hat = jnp.pad(hat, ((0, 0), (0, 0), (0, 256 - N)))
    scratch = [pltpu.VMEM((2 * KP, N, 256), jnp.float32)] * 3
    scratch += [pltpu.VMEM(lines_table.shape, lines_table.dtype), pltpu.SemaphoreType.DMA((7,))]
    lined = call(
        line_kernel,
        [VMEM, HBM, HBM],
        [chunk],
        (exchange(spread), hat, lines_table),
        scratch,
        limit=54_000_000,
    )
    back = exchange(lined)
    kept, sent = call(
        term_kernel,
        [SMEM, SMEM, VMEM, VMEM, HBM, VMEM],
        [(864, 128), (872, 128)],
        (upper, occupation, back, own, theirs, tv),
        [rows, pltpu.SemaphoreType.DMA],
    )

    come = to_partner(sent, pair_bits)
    scratch = [pltpu.VMEM((872, 128), jnp.float32), rows, pltpu.SemaphoreType.DMA((9,))]
    total = call(sum_kernel, [SMEM, VMEM, HBM], [(864, 128)], (upper, kept, come), scratch, HBM)
    return from_rows(total)


def solution(mesh):
    return jax.shard_map(
        local,
        mesh=mesh,
        in_specs=(P("grp", "slab", None), P("grp"), P("slab", None), P()),
        out_specs=P("grp", "slab", None),
        check_vma=False,
    )
```

```python
import functools
import math

import jax
import jax.numpy as jnp
import numpy as np
from jax import lax
from jax.experimental import pallas as pl
from jax.experimental.pallas import tpu as pltpu
from jax.sharding import PartitionSpec as P

G = 96
N = 192
SLABS = 16
XS = 6
KP = 6
ROWS = 112

Y_ORDER = np.array([4 * (i % 24) + i // 24 for i in range(G)])
X_ORDER = np.array([6 * (i % SLABS) + i // SLABS for i in range(G)])


WY, WI, TX, TI, LINES = 0, 640, 1664, 2048, 2432


def split(table):
    table = jnp.asarray(table, jnp.float32)
    high = table.astype(jnp.bfloat16)
    low = (table - high.astype(jnp.float32)).astype(jnp.bfloat16)
    return high, low


def np_split(table):
    bf16 = jnp.bfloat16
    high = table.astype(np.float32).astype(bf16)
    low = (table - high.astype(np.float64)).astype(np.float32).astype(bf16)
    return np.stack([high, low])


def waves(freq, cell):
    angle = (np.outer(freq, cell) % N) * (2.0 * math.pi / N)
    return np.cos(angle), np.sin(angle)


@functools.cache
def tables():
    pair_major = np.array([[12 * d + 2 * kp for d in range(SLABS)] for kp in range(KP)]).reshape(-1)
    tz = np.zeros((384, 256))
    tv = np.zeros((256, 384))
    wy = np.zeros((320, 512))
    wi = np.zeros((2, 512, 256))
    for kz2 in range(2):
        cos, sin = waves(pair_major + kz2, np.arange(G))
        re, im = 192 * kz2, 192 * kz2 + 96
        tz[re : re + 96, 0:96], tz[re : re + 96, 128:224] = cos, sin
        tz[im : im + 96, 0:96], tz[im : im + 96, 128:224] = -sin, cos
        tv[0:96, re : re + 96], tv[0:96, im : im + 96] = cos.T / N, -sin.T / N
        tv[128:224, re : re + 96], tv[128:224, im : im + 96] = sin.T / N, cos.T / N
        cos, sin = waves(Y_ORDER, np.arange(N))
        wy[64:160, 0:192], wy[64:160, 256:448] = cos, -sin
        wy[160:256, 0:192], wy[160:256, 256:448] = sin, cos
        re, im = 64 * kz2, 64 * kz2 + 96
        wi[kz2, 0:192, re : re + 96], wi[kz2, 0:192, im : im + 96] = cos.T / N, sin.T / N
        wi[kz2, 256:448, re : re + 96], wi[kz2, 256:448, im : im + 96] = -sin.T / N, cos.T / N
    cos, sin = waves(np.arange(N), X_ORDER)
    tx = np.block([[cos, sin], [-sin, cos]])
    ti = np.block([[cos.T, -sin.T], [sin.T, cos.T]]) / N
    lines = [wy[:, :256], wy[:, 256:], wi[0], wi[1], widened(tx), widened(ti[:, :N]), widened(ti[:, N:])]
    return [np_split(t) for t in (tz, np.concatenate(lines, axis=0), tv)]


def widened(table):
    return np.pad(table, ((0, 0), (0, 256 - N)))


def mm(left, right, form=(1, 0)):
    def one(a, b):
        return lax.dot_general(
            a, b, (((form[0],), (form[1],)), ((), ())), preferred_element_type=jnp.float32
        )

    return one(left[0], right[0]) + (one(left[0], right[1]) + one(left[1], right[0]))


def plane(ref, x, orbital):
    base = 144 * x + orbital
    tiles = [ref[pl.ds(base + 2 * tile, 24, stride=6), :] for tile in range(3)]
    return jnp.concatenate(tiles, axis=1)


def lines(dense):
    return jnp.concatenate([dense[:, 96 * q : 96 * q + 96] for q in range(4)], axis=0)


def dense_of(rows):
    return jnp.concatenate([rows[24 * q : 24 * q + 24] for q in range(4)], axis=1)


def spread_kernel(
    upper_ref, own_hbm, their_hbm, tz_hbm, out_hbm, own_ref, their_ref, tz_ref, out_ref, sems
):
    table_in = pltpu.make_async_copy(tz_hbm, tz_ref, sems.at[0])
    table_in.start()
    halves = []
    for half in range(2):
        rows = pl.ds(432 * half, 432)
        for k, (hbm, ref) in enumerate(((their_hbm, their_ref), (own_hbm, own_ref))):
            halves.append(
                pltpu.make_async_copy(hbm.at[rows], ref.at[rows], sems.at[1 + 2 * half + k])
            )
            halves[-1].start()
    upper = upper_ref[0] == 1
    pad = jnp.zeros((G, 32), jnp.float32)
    outs = []
    for x in range(XS):
        if x % 3 == 0:
            for copy in halves[2 * (x // 3) : 2 * (x // 3) + 2]:
                copy.wait()
        theirs = [plane(their_ref, x, o) for o in range(2)]
        first = jnp.where(upper, theirs[1], theirs[0])
        second = jnp.where(upper, theirs[0], theirs[1])
        one = lines(plane(own_ref, x, 0) * first)
        two = lines(plane(own_ref, x, 1) * second)
        density = jnp.concatenate([one, pad, two, pad], axis=1)
        if x == 0:
            table_in.wait()
        lined = mm((tz_ref[0], tz_ref[1]), split(density), (1, 1))
        wide = jnp.concatenate([lined[96 * j : 96 * j + 96] for j in range(4)], axis=1)
        for kp in range(KP):
            for tile in range(3):
                out_ref[pl.ds(18 * x + 6 * tile + kp, SLABS, stride=ROWS), :] = wide[
                    16 * kp : 16 * kp + 16, 128 * tile : 128 * tile + 128
                ]
        if x in (3, 5):
            first_row, count = (0, 72) if x == 3 else (72, 40)
            if x == 5:
                for slab in range(SLABS):
                    out_ref[ROWS * slab + 108 : ROWS * slab + 112, :] = jnp.zeros((4, 128), jnp.float32)
            for slab in range(SLABS):
                place = pl.ds(ROWS * slab + first_row, count)
                outs.append(
                    pltpu.make_async_copy(out_ref.at[place], out_hbm.at[place], sems.at[5 + len(outs)])
                )
                outs[-1].start()
    for copy in outs:
        copy.wait()


def line_kernel(in_ref, hat_ref, table_hbm, out_ref, y_ref, u_ref, table_ref, sems):
    fetches = []
    for row, count in ((WY, WI - WY), (TX, LINES - TX), (WI, TX - WI)):
        place = (slice(None), pl.ds(row, count))
        pair = (table_hbm.at[place], table_ref.at[place])
        fetches.append(pltpu.make_async_copy(*pair, sems.at[len(fetches)]))
    for copy in fetches:
        copy.start()
    def table(row, count, columns=256):
        return [table_ref[part, row : row + count, :columns] for part in range(2)]

    pieces = []
    for kp in range(KP):
        for x in range(XS):
            pieces.append(
                jnp.concatenate(
                    [
                        in_ref[pl.ds(18 * x + 6 * tile + kp, SLABS, stride=ROWS), :]
                        for tile in range(3)
                    ],
                    axis=1,
                )
            )
    data = split(jnp.concatenate(pieces, axis=0))
    fetches[0].wait()
    for kz2 in range(2):
        window = [part[:, 128 * kz2 : 128 * kz2 + 256] for part in data]
        for c in range(2):
            result = mm(window, table(WY + 320 * c + 64 * (1 - kz2), 256))
            for kp in range(KP):
                y_ref[2 * kp + kz2, 96 * c : 96 * c + 96, :] = result[96 * kp : 96 * kp + 96]
    for copy in fetches[1:]:
        copy.wait()
    for kz in range(2 * KP):
        lined = split(y_ref[kz, :, :N])
        spectrum = mm(table(TX, 384, N), lined)
        hat = hat_ref[kz]
        u_ref[kz, :, :N] = mm(table(TI, N, N), split(spectrum[:N] * hat)) + mm(
            table(TI + N, N, N), split(spectrum[N:] * hat)
        )
    sides = []
    for kz2 in range(2):
        rows = [
            [u_ref[2 * kp + kz2, G * c : G * c + G, :N] for kp in range(KP)] for c in range(2)
        ]
        re, im = [split(jnp.concatenate(part, axis=0)) for part in rows]
        first = WI + 512 * kz2
        sides.append(mm(re, table(first, N)) + mm(im, table(first + 256, N)))
    wide = [sides[0][:, :128], sides[0][:, 128:] + sides[1][:, :128], sides[1][:, 128:]]
    for kp in range(KP):
        for x in range(XS):
            for tile in range(3):
                row = 96 * kp + 16 * x
                out_ref[pl.ds(18 * x + 6 * tile + kp, SLABS, stride=ROWS), :] = wide[tile][
                    row : row + 16
                ]


def term_kernel(
    upper_ref, occupation_ref, in_ref, own_ref, their_hbm, tv_ref, kept_ref, sent_ref, their_ref, sem
):
    fetch = pltpu.make_async_copy(their_hbm, their_ref, sem)
    fetch.start()
    upper = upper_ref[0] == 1
    table = (tv_ref[0], tv_ref[1])
    weight = [0.25 * occupation_ref[o].astype(jnp.float32) for o in range(2)]
    for x in range(XS):
        pieces = [
            jnp.concatenate(
                [
                    in_ref[pl.ds(18 * x + 6 * tile + kp, SLABS, stride=ROWS), :]
                    for tile in range(3)
                ],
                axis=1,
            )
            for kp in range(KP)
        ]
        wide = jnp.concatenate(pieces, axis=0)
        stacked = jnp.concatenate([wide[:, 96 * j : 96 * j + 96] for j in range(4)], axis=0)
        fields = mm(table, split(stacked)).T
        one = dense_of(fields[:, :96])
        two = dense_of(fields[:, 128:224])
        if x == 0:
            fetch.wait()
        theirs = [plane(their_ref, x, o) for o in range(2)]
        first = jnp.where(upper, theirs[1], theirs[0])
        second = jnp.where(upper, theirs[0], theirs[1])
        kept = [one * first, two * second]
        mine_one = one * plane(own_ref, x, 0) * weight[0]
        mine_two = two * plane(own_ref, x, 1) * weight[1]
        sent = [jnp.where(upper, mine_two, mine_one), jnp.where(upper, mine_one, mine_two)]
        for o in range(2):
            for tile in range(3):
                place = pl.ds(144 * x + o + 2 * tile, 24, stride=6)
                kept_ref[place, :] = kept[o][:, 128 * tile : 128 * tile + 128]
                sent_ref[place, :] = sent[o][:, 128 * tile : 128 * tile + 128]
    row = lax.broadcasted_iota(jnp.int32, (8, 128), 0)
    sent_ref[864:872, :] = jnp.where(row % 2 == 1, weight[1], weight[0])


PARTS = ((864, 8), (0, 216), (216, 216), (432, 216), (648, 216))


def sum_kernel(upper_ref, kept_ref, come_hbm, out_hbm, come_ref, out_ref, sems):
    fetches, outs = [], []
    for k, (row, count) in enumerate(PARTS):
        place = pl.ds(row, count)
        fetches.append(pltpu.make_async_copy(come_hbm.at[place], come_ref.at[place], sems.at[k]))
        fetches[-1].start()
    upper = upper_ref[0] == 1
    odd_row = lax.broadcasted_iota(jnp.int32, (216, 128), 0) % 2 == 1
    fetches[0].wait()
    even = jnp.where(upper, come_ref[865:866, :], come_ref[864:865, :])
    odd = jnp.where(upper, come_ref[864:865, :], come_ref[865:866, :])
    weight = jnp.where(odd_row, odd, even)
    for k, (row, count) in enumerate(PARTS[1:], 1):
        place = pl.ds(row, count)
        fetches[k].wait()
        out_ref[place, :] = -(kept_ref[place, :] * weight + come_ref[place, :])
        outs.append(pltpu.make_async_copy(out_ref.at[place], out_hbm.at[place], sems.at[4 + k]))
        outs[-1].start()
    for copy in outs:
        copy.wait()


SMEM = pl.BlockSpec(memory_space=pltpu.SMEM)
VMEM = pl.BlockSpec(memory_space=pltpu.VMEM)
HBM = pl.BlockSpec(memory_space=pltpu.HBM)


def call(kernel, ins, outs, args, scratch=(), out_spec=VMEM, limit=28_000_000):
    shapes = [o if isinstance(o, jax.ShapeDtypeStruct) else jax.ShapeDtypeStruct(o, jnp.float32) for o in outs]
    many = len(shapes) > 1
    return pl.pallas_call(
        kernel,
        out_shape=shapes if many else shapes[0],
        in_specs=ins,
        out_specs=[out_spec] * len(outs) if many else out_spec,
        scratch_shapes=scratch,
        compiler_params=pltpu.CompilerParams(vmem_limit_bytes=limit),
    )(*args)


def to_partner(value, pair_bits):
    group_count = lax.axis_size("grp")

    def by_mask(mask):
        pairs = [(source, source ^ mask) for source in range(group_count)]
        return lambda sent: lax.ppermute(sent, "grp", pairs)

    branches = [by_mask(mask) for mask in range(1, group_count)]
    return lax.switch(pair_bits - 1, branches, value)


def to_rows(planes):
    return planes.reshape(2, XS, 72, 128).transpose(1, 2, 0, 3).reshape(864, 128)


def from_rows(rows):
    return rows.reshape(XS, 72, 2, 128).transpose(2, 0, 1, 3).reshape(2, XS, G * G)


def exchange(chunks):
    chunks = chunks.reshape(SLABS, ROWS, 128)
    moved = lax.all_to_all(chunks, "slab", split_axis=0, concat_axis=0, tiled=True)
    return moved.reshape(SLABS * ROWS, 128)


def local(orbitals, occupation, kernel_hat, pair_mask):
    tz, lines_table, tv = [jnp.asarray(t) for t in tables()]
    pair_bits = pair_mask[0]
    own_group = lax.axis_index("grp")
    upper = (own_group > jnp.bitwise_xor(own_group, pair_bits)).astype(jnp.int32).reshape(1)
    own = to_rows(orbitals)
    theirs = to_partner(own, pair_bits)
    chunk = (SLABS * ROWS, 128)
    rows = pltpu.VMEM((864, 128), jnp.float32)
    spread = call(
        spread_kernel,
        [SMEM, HBM, HBM, HBM],
        [chunk],
        (upper, own, theirs, tz),
        [rows, rows, pltpu.VMEM(tz.shape, tz.dtype), pltpu.VMEM(chunk, jnp.float32)]
        + [pltpu.SemaphoreType.DMA((5 + 2 * SLABS,))],
        HBM,
        66_800_000,
    )
    hat = kernel_hat.reshape(2 * KP, N, N).transpose(0, 2, 1)
    scratch = [pltpu.VMEM((2 * KP, N, 256), jnp.float32)] * 2
    scratch += [pltpu.VMEM(lines_table.shape, lines_table.dtype), pltpu.SemaphoreType.DMA((3,))]
    lined = call(
        line_kernel,
        [VMEM, VMEM, HBM],
        [chunk],
        (exchange(spread), hat, lines_table),
        scratch,
        limit=51_000_000,
    )
    back = exchange(lined)
    kept, sent = call(
        term_kernel,
        [SMEM, SMEM, VMEM, VMEM, HBM, VMEM],
        [(864, 128), (872, 128)],
        (upper, occupation, back, own, theirs, tv),
        [rows, pltpu.SemaphoreType.DMA],
    )

    come = to_partner(sent, pair_bits)
    scratch = [pltpu.VMEM((872, 128), jnp.float32), rows, pltpu.SemaphoreType.DMA((9,))]
    total = call(sum_kernel, [SMEM, VMEM, HBM], [(864, 128)], (upper, kept, come), scratch, HBM)
    return from_rows(total)


def solution(mesh):
    return jax.shard_map(
        local,
        mesh=mesh,
        in_specs=(P("grp", "slab", None), P("grp"), P("slab", None), P()),
        out_specs=P("grp", "slab", None),
        check_vma=False,
    )
```

```python
import functools
import math

import jax
import jax.numpy as jnp
import numpy as np
from jax import lax
from jax.experimental import pallas as pl
from jax.experimental.pallas import tpu as pltpu
from jax.sharding import PartitionSpec as P

G = 96
N = 192
SLABS = 16
XS = 6
KP = 6
ROWS = 112

Y_ORDER = np.array([4 * (i % 24) + i // 24 for i in range(G)])
X_ORDER = np.array([6 * (i % SLABS) + i // SLABS for i in range(G)])


WY, WI, TX, TI, LINES = 0, 640, 1664, 2048, 2432


def split(table):
    table = jnp.asarray(table, jnp.float32)
    high = table.astype(jnp.bfloat16)
    low = (table - high.astype(jnp.float32)).astype(jnp.bfloat16)
    return high, low


def np_split(table):
    bf16 = jnp.bfloat16
    high = table.astype(np.float32).astype(bf16)
    low = (table - high.astype(np.float64)).astype(np.float32).astype(bf16)
    return np.stack([high, low])


def waves(freq, cell):
    angle = (np.outer(freq, cell) % N) * (2.0 * math.pi / N)
    return np.cos(angle), np.sin(angle)


@functools.cache
def tables():
    pair_major = np.array([[12 * d + 2 * kp for d in range(SLABS)] for kp in range(KP)]).reshape(-1)
    tz = np.zeros((384, 256))
    tv = np.zeros((256, 384))
    wy = np.zeros((320, 512))
    wi = np.zeros((2, 512, 256))
    for kz2 in range(2):
        cos, sin = waves(pair_major + kz2, np.arange(G))
        re, im = 192 * kz2, 192 * kz2 + 96
        tz[re : re + 96, 0:96], tz[re : re + 96, 128:224] = cos, sin
        tz[im : im + 96, 0:96], tz[im : im + 96, 128:224] = -sin, cos
        tv[0:96, re : re + 96], tv[0:96, im : im + 96] = cos.T / N, -sin.T / N
        tv[128:224, re : re + 96], tv[128:224, im : im + 96] = sin.T / N, cos.T / N
        cos, sin = waves(Y_ORDER, np.arange(N))
        wy[64:160, 0:192], wy[64:160, 256:448] = cos, -sin
        wy[160:256, 0:192], wy[160:256, 256:448] = sin, cos
        re, im = 64 * kz2, 64 * kz2 + 96
        wi[kz2, 0:192, re : re + 96], wi[kz2, 0:192, im : im + 96] = cos.T / N, sin.T / N
        wi[kz2, 256:448, re : re + 96], wi[kz2, 256:448, im : im + 96] = -sin.T / N, cos.T / N
    cos, sin = waves(np.arange(N), X_ORDER)
    tx = np.block([[cos, sin], [-sin, cos]])
    ti = np.block([[cos.T, -sin.T], [sin.T, cos.T]]) / N
    lines = [wy[:, :256], wy[:, 256:], wi[0], wi[1], widened(tx), widened(ti[:, :N]), widened(ti[:, N:])]
    return [np_split(t) for t in (tz, np.concatenate(lines, axis=0), tv)]


def widened(table):
    return np.pad(table, ((0, 0), (0, 256 - N)))


def mm(left, right, form=(1, 0)):
    def one(a, b):
        return lax.dot_general(
            a, b, (((form[0],), (form[1],)), ((), ())), preferred_element_type=jnp.float32
        )

    return one(left[0], right[0]) + (one(left[0], right[1]) + one(left[1], right[0]))


def plane(ref, x, orbital):
    base = 144 * x + orbital
    tiles = [ref[pl.ds(base + 2 * tile, 24, stride=6), :] for tile in range(3)]
    return jnp.concatenate(tiles, axis=1)


def lines(dense):
    return jnp.concatenate([dense[:, 96 * q : 96 * q + 96] for q in range(4)], axis=0)


def dense_of(rows):
    return jnp.concatenate([rows[24 * q : 24 * q + 24] for q in range(4)], axis=1)


def spread_kernel(
    upper_ref, own_hbm, their_hbm, tz_hbm, out_hbm, own_ref, their_ref, tz_ref, out_ref, sems
):
    table_in = pltpu.make_async_copy(tz_hbm, tz_ref, sems.at[0])
    table_in.start()
    halves = []
    for half in range(2):
        rows = pl.ds(432 * half, 432)
        for k, (hbm, ref) in enumerate(((their_hbm, their_ref), (own_hbm, own_ref))):
            halves.append(
                pltpu.make_async_copy(hbm.at[rows], ref.at[rows], sems.at[1 + 2 * half + k])
            )
            halves[-1].start()
    upper = upper_ref[0] == 1
    pad = jnp.zeros((G, 32), jnp.float32)
    outs = []
    for x in range(XS):
        if x % 3 == 0:
            for copy in halves[2 * (x // 3) : 2 * (x // 3) + 2]:
                copy.wait()
        theirs = [plane(their_ref, x, o) for o in range(2)]
        first = jnp.where(upper, theirs[1], theirs[0])
        second = jnp.where(upper, theirs[0], theirs[1])
        one = lines(plane(own_ref, x, 0) * first)
        two = lines(plane(own_ref, x, 1) * second)
        density = jnp.concatenate([one, pad, two, pad], axis=1)
        if x == 0:
            table_in.wait()
        lined = mm((tz_ref[0], tz_ref[1]), split(density), (1, 1))
        wide = jnp.concatenate([lined[96 * j : 96 * j + 96] for j in range(4)], axis=1)
        for kp in range(KP):
            for tile in range(3):
                out_ref[pl.ds(18 * x + 6 * tile + kp, SLABS, stride=ROWS), :] = wide[
                    16 * kp : 16 * kp + 16, 128 * tile : 128 * tile + 128
                ]
        if x in (3, 5):
            first_row, count = (0, 72) if x == 3 else (72, 40)
            if x == 5:
                for slab in range(SLABS):
                    out_ref[ROWS * slab + 108 : ROWS * slab + 112, :] = jnp.zeros((4, 128), jnp.float32)
            for slab in range(SLABS):
                place = pl.ds(ROWS * slab + first_row, count)
                outs.append(
                    pltpu.make_async_copy(out_ref.at[place], out_hbm.at[place], sems.at[5 + len(outs)])
                )
                outs[-1].start()
    for copy in outs:
        copy.wait()


def line_kernel(in_ref, hat_ref, table_hbm, out_ref, y_ref, u_ref, table_ref, sems):
    fetches = []
    for row, count in ((WY, WI - WY), (TX, LINES - TX), (WI, TX - WI)):
        place = (slice(None), pl.ds(row, count))
        pair = (table_hbm.at[place], table_ref.at[place])
        fetches.append(pltpu.make_async_copy(*pair, sems.at[len(fetches)]))
    for copy in fetches:
        copy.start()
    def table(row, count, columns=256):
        return [table_ref[part, row : row + count, :columns] for part in range(2)]

    pieces = []
    for kp in range(KP):
        for x in range(XS):
            pieces.append(
                jnp.concatenate(
                    [
                        in_ref[pl.ds(18 * x + 6 * tile + kp, SLABS, stride=ROWS), :]
                        for tile in range(3)
                    ],
                    axis=1,
                )
            )
    data = split(jnp.concatenate(pieces, axis=0))
    fetches[0].wait()
    for kz2 in range(2):
        window = [part[:, 128 * kz2 : 128 * kz2 + 256] for part in data]
        for c in range(2):
            result = mm(window, table(WY + 320 * c + 64 * (1 - kz2), 256))
            for kp in range(KP):
                y_ref[2 * kp + kz2, 96 * c : 96 * c + 96, :] = result[96 * kp : 96 * kp + 96]
    for copy in fetches[1:]:
        copy.wait()
    for kz in range(2 * KP):
        lined = split(y_ref[kz, :, :N])
        spectrum = mm(table(TX, 384, N), lined)
        hat = hat_ref[kz]
        u_ref[kz, :, :N] = mm(table(TI, N, N), split(spectrum[:N] * hat)) + mm(
            table(TI + N, N, N), split(spectrum[N:] * hat)
        )
    sides = []
    for kz2 in range(2):
        rows = [
            [u_ref[2 * kp + kz2, G * c : G * c + G, :N] for kp in range(KP)] for c in range(2)
        ]
        re, im = [split(jnp.concatenate(part, axis=0)) for part in rows]
        first = WI + 512 * kz2
        sides.append(mm(re, table(first, N)) + mm(im, table(first + 256, N)))
    wide = [sides[0][:, :128], sides[0][:, 128:] + sides[1][:, :128], sides[1][:, 128:]]
    for kp in range(KP):
        for x in range(XS):
            for tile in range(3):
                row = 96 * kp + 16 * x
                out_ref[pl.ds(18 * x + 6 * tile + kp, SLABS, stride=ROWS), :] = wide[tile][
                    row : row + 16
                ]


def term_kernel(
    upper_ref, occupation_ref, in_ref, own_ref, their_hbm, tv_ref, kept_ref, sent_ref, their_ref, sem
):
    fetch = pltpu.make_async_copy(their_hbm, their_ref, sem)
    fetch.start()
    upper = upper_ref[0] == 1
    table = (tv_ref[0], tv_ref[1])
    weight = [0.25 * occupation_ref[o].astype(jnp.float32) for o in range(2)]
    for x in range(XS):
        pieces = [
            jnp.concatenate(
                [
                    in_ref[pl.ds(18 * x + 6 * tile + kp, SLABS, stride=ROWS), :]
                    for tile in range(3)
                ],
                axis=1,
            )
            for kp in range(KP)
        ]
        wide = jnp.concatenate(pieces, axis=0)
        stacked = jnp.concatenate([wide[:, 96 * j : 96 * j + 96] for j in range(4)], axis=0)
        fields = mm(table, split(stacked)).T
        one = dense_of(fields[:, :96])
        two = dense_of(fields[:, 128:224])
        if x == 0:
            fetch.wait()
        theirs = [plane(their_ref, x, o) for o in range(2)]
        first = jnp.where(upper, theirs[1], theirs[0])
        second = jnp.where(upper, theirs[0], theirs[1])
        kept = [one * first, two * second]
        mine_one = one * plane(own_ref, x, 0) * weight[0]
        mine_two = two * plane(own_ref, x, 1) * weight[1]
        sent = [jnp.where(upper, mine_two, mine_one), jnp.where(upper, mine_one, mine_two)]
        for o in range(2):
            for tile in range(3):
                place = pl.ds(144 * x + o + 2 * tile, 24, stride=6)
                kept_ref[place, :] = kept[o][:, 128 * tile : 128 * tile + 128]
                sent_ref[place, :] = sent[o][:, 128 * tile : 128 * tile + 128]
    row = lax.broadcasted_iota(jnp.int32, (8, 128), 0)
    sent_ref[864:872, :] = jnp.where(row % 2 == 1, weight[1], weight[0])


PARTS = ((864, 8), (0, 216), (216, 216), (432, 216), (648, 216))


def sum_kernel(upper_ref, kept_ref, come_hbm, out_hbm, come_ref, out_ref, sems):
    fetches, outs = [], []
    for k, (row, count) in enumerate(PARTS):
        place = pl.ds(row, count)
        fetches.append(pltpu.make_async_copy(come_hbm.at[place], come_ref.at[place], sems.at[k]))
        fetches[-1].start()
    upper = upper_ref[0] == 1
    odd_row = lax.broadcasted_iota(jnp.int32, (216, 128), 0) % 2 == 1
    fetches[0].wait()
    even = jnp.where(upper, come_ref[865:866, :], come_ref[864:865, :])
    odd = jnp.where(upper, come_ref[864:865, :], come_ref[865:866, :])
    weight = jnp.where(odd_row, odd, even)
    for k, (row, count) in enumerate(PARTS[1:], 1):
        place = pl.ds(row, count)
        fetches[k].wait()
        out_ref[place, :] = -(kept_ref[place, :] * weight + come_ref[place, :])
        outs.append(pltpu.make_async_copy(out_ref.at[place], out_hbm.at[place], sems.at[4 + k]))
        outs[-1].start()
    for copy in outs:
        copy.wait()


SMEM = pl.BlockSpec(memory_space=pltpu.SMEM)
VMEM = pl.BlockSpec(memory_space=pltpu.VMEM)
HBM = pl.BlockSpec(memory_space=pltpu.HBM)


def call(kernel, ins, outs, args, scratch=(), out_spec=VMEM, limit=28_000_000):
    shapes = [o if isinstance(o, jax.ShapeDtypeStruct) else jax.ShapeDtypeStruct(o, jnp.float32) for o in outs]
    many = len(shapes) > 1
    return pl.pallas_call(
        kernel,
        out_shape=shapes if many else shapes[0],
        in_specs=ins,
        out_specs=[out_spec] * len(outs) if many else out_spec,
        scratch_shapes=scratch,
        compiler_params=pltpu.CompilerParams(vmem_limit_bytes=limit),
    )(*args)


def to_partner(value, pair_bits):
    group_count = lax.axis_size("grp")

    def by_mask(mask):
        pairs = [(source, source ^ mask) for source in range(group_count)]
        return lambda sent: lax.ppermute(sent, "grp", pairs)

    branches = [by_mask(mask) for mask in range(1, group_count)]
    return lax.switch(pair_bits - 1, branches, value)


def from_partner(own, pair_bits):
    group_count = lax.axis_size("grp")
    slabs = lax.axis_size("slab")
    sets = [list(range(first, first + slabs // 2)) for first in (0, slabs // 2)]

    def by_mask(mask):
        pairs = [(source, source ^ mask) for source in range(group_count)]

        def branch(operands):
            sent, bits = operands
            come = lax.ppermute(sent, "grp", pairs)
            said = jnp.full((slabs // 2, 8, 128), bits.astype(jnp.float32))
            heard = lax.all_to_all(said, "slab", 0, 0, tiled=True, axis_index_groups=sets)
            bits = heard[0, 0, 0].astype(jnp.int32)
            group = lax.axis_index("grp")
            return come, (group > jnp.bitwise_xor(group, bits)).astype(jnp.int32).reshape(1)

        return branch

    branches = [by_mask(mask) for mask in range(1, group_count)]
    return lax.switch(pair_bits - 1, branches, (own, pair_bits))


def to_rows(planes):
    return planes.reshape(2, XS, 72, 128).transpose(1, 2, 0, 3).reshape(864, 128)


def from_rows(rows):
    return rows.reshape(XS, 72, 2, 128).transpose(2, 0, 1, 3).reshape(2, XS, G * G)


def exchange(chunks):
    chunks = chunks.reshape(SLABS, ROWS, 128)
    moved = lax.all_to_all(chunks, "slab", split_axis=0, concat_axis=0, tiled=True)
    return moved.reshape(SLABS * ROWS, 128)


def local(orbitals, occupation, kernel_hat, pair_mask):
    tz, lines_table, tv = [jnp.asarray(t) for t in tables()]
    pair_bits = pair_mask[0]
    own = to_rows(orbitals)
    theirs, upper = from_partner(own, pair_bits)
    chunk = (SLABS * ROWS, 128)
    rows = pltpu.VMEM((864, 128), jnp.float32)
    spread = call(
        spread_kernel,
        [SMEM, HBM, HBM, HBM],
        [chunk],
        (upper, own, theirs, tz),
        [rows, rows, pltpu.VMEM(tz.shape, tz.dtype), pltpu.VMEM(chunk, jnp.float32)]
        + [pltpu.SemaphoreType.DMA((5 + 2 * SLABS,))],
        HBM,
        66_800_000,
    )
    hat = kernel_hat.reshape(2 * KP, N, N).transpose(0, 2, 1)
    scratch = [pltpu.VMEM((2 * KP, N, 256), jnp.float32)] * 2
    scratch += [pltpu.VMEM(lines_table.shape, lines_table.dtype), pltpu.SemaphoreType.DMA((3,))]
    lined = call(
        line_kernel,
        [VMEM, VMEM, HBM],
        [chunk],
        (exchange(spread), hat, lines_table),
        scratch,
        limit=51_000_000,
    )
    back = exchange(lined)
    kept, sent = call(
        term_kernel,
        [SMEM, SMEM, VMEM, VMEM, HBM, VMEM],
        [(864, 128), (872, 128)],
        (upper, occupation, back, own, theirs, tv),
        [rows, pltpu.SemaphoreType.DMA],
    )

    come = to_partner(sent, pair_bits)
    scratch = [pltpu.VMEM((872, 128), jnp.float32), rows, pltpu.SemaphoreType.DMA((9,))]
    total = call(sum_kernel, [SMEM, VMEM, HBM], [(864, 128)], (upper, kept, come), scratch, HBM)
    return from_rows(total)


def solution(mesh):
    return jax.shard_map(
        local,
        mesh=mesh,
        in_specs=(P("grp", "slab", None), P("grp"), P("slab", None), P()),
        out_specs=P("grp", "slab", None),
        check_vma=False,
    )
```

```python
import functools
import math

import jax
import jax.numpy as jnp
import numpy as np
from jax import lax
from jax.experimental import pallas as pl
from jax.experimental.pallas import tpu as pltpu
from jax.sharding import PartitionSpec as P

G = 96
N = 192
SLABS = 16
XS = 6
KP = 6
ROWS = 112

Y_ORDER = np.array([4 * (i % 24) + i // 24 for i in range(G)])
X_ORDER = np.array([6 * (i % SLABS) + i // SLABS for i in range(G)])


WY, WI, TX, TI, LINES = 0, 640, 1664, 2048, 2432


def split(table):
    table = jnp.asarray(table, jnp.float32)
    high = table.astype(jnp.bfloat16)
    low = (table - high.astype(jnp.float32)).astype(jnp.bfloat16)
    return high, low


def np_split(table):
    bf16 = jnp.bfloat16
    high = table.astype(np.float32).astype(bf16)
    low = (table - high.astype(np.float64)).astype(np.float32).astype(bf16)
    return np.stack([high, low])


def waves(freq, cell):
    angle = (np.outer(freq, cell) % N) * (2.0 * math.pi / N)
    return np.cos(angle), np.sin(angle)


@functools.cache
def tables():
    pair_major = np.array([[12 * d + 2 * kp for d in range(SLABS)] for kp in range(KP)]).reshape(-1)
    tz = np.zeros((384, 256))
    tv = np.zeros((256, 384))
    wy = np.zeros((320, 512))
    wi = np.zeros((2, 512, 256))
    for kz2 in range(2):
        cos, sin = waves(pair_major + kz2, np.arange(G))
        re, im = 192 * kz2, 192 * kz2 + 96
        tz[re : re + 96, 0:96], tz[re : re + 96, 128:224] = cos, sin
        tz[im : im + 96, 0:96], tz[im : im + 96, 128:224] = -sin, cos
        tv[0:96, re : re + 96], tv[0:96, im : im + 96] = cos.T / N, -sin.T / N
        tv[128:224, re : re + 96], tv[128:224, im : im + 96] = sin.T / N, cos.T / N
        cos, sin = waves(Y_ORDER, np.arange(N))
        wy[64:160, 0:192], wy[64:160, 256:448] = cos, -sin
        wy[160:256, 0:192], wy[160:256, 256:448] = sin, cos
        re, im = 64 * kz2, 64 * kz2 + 96
        wi[kz2, 0:192, re : re + 96], wi[kz2, 0:192, im : im + 96] = cos.T / N, sin.T / N
        wi[kz2, 256:448, re : re + 96], wi[kz2, 256:448, im : im + 96] = -sin.T / N, cos.T / N
    cos, sin = waves(np.arange(N), X_ORDER)
    tx = np.block([[cos, sin], [-sin, cos]])
    ti = np.block([[cos.T, -sin.T], [sin.T, cos.T]]) / N
    lines = [wy[:, :256], wy[:, 256:], wi[0], wi[1], widened(tx), widened(ti[:, :N]), widened(ti[:, N:])]
    return [np_split(t) for t in (tz, np.concatenate(lines, axis=0), tv)]


def widened(table):
    return np.pad(table, ((0, 0), (0, 256 - N)))


def mm(left, right, form=(1, 0)):
    def one(a, b):
        return lax.dot_general(
            a, b, (((form[0],), (form[1],)), ((), ())), preferred_element_type=jnp.float32
        )

    return one(left[0], right[0]) + (one(left[0], right[1]) + one(left[1], right[0]))


def plane(ref, x, orbital):
    base = 144 * x + orbital
    tiles = [ref[pl.ds(base + 2 * tile, 24, stride=6), :] for tile in range(3)]
    return jnp.concatenate(tiles, axis=1)


def lines(dense):
    return jnp.concatenate([dense[:, 96 * q : 96 * q + 96] for q in range(4)], axis=0)


def dense_of(rows):
    return jnp.concatenate([rows[24 * q : 24 * q + 24] for q in range(4)], axis=1)


def spread_kernel(
    upper_ref, own_hbm, their_hbm, tz_hbm, out_hbm, own_ref, their_ref, tz_ref, out_ref, sems
):
    table_in = pltpu.make_async_copy(tz_hbm, tz_ref, sems.at[0])
    table_in.start()
    halves = []
    for half in range(2):
        rows = pl.ds(432 * half, 432)
        for k, (hbm, ref) in enumerate(((their_hbm, their_ref), (own_hbm, own_ref))):
            halves.append(
                pltpu.make_async_copy(hbm.at[rows], ref.at[rows], sems.at[1 + 2 * half + k])
            )
            halves[-1].start()
    upper = upper_ref[0] == 1
    pad = jnp.zeros((G, 32), jnp.float32)
    outs = []
    for x in range(XS):
        if x % 3 == 0:
            for copy in halves[2 * (x // 3) : 2 * (x // 3) + 2]:
                copy.wait()
        theirs = [plane(their_ref, x, o) for o in range(2)]
        first = jnp.where(upper, theirs[1], theirs[0])
        second = jnp.where(upper, theirs[0], theirs[1])
        one = lines(plane(own_ref, x, 0) * first)
        two = lines(plane(own_ref, x, 1) * second)
        density = jnp.concatenate([one, pad, two, pad], axis=1)
        if x == 0:
            table_in.wait()
        lined = mm((tz_ref[0], tz_ref[1]), split(density), (1, 1))
        wide = jnp.concatenate([lined[96 * j : 96 * j + 96] for j in range(4)], axis=1)
        for kp in range(KP):
            for tile in range(3):
                out_ref[pl.ds(18 * x + 6 * tile + kp, SLABS, stride=ROWS), :] = wide[
                    16 * kp : 16 * kp + 16, 128 * tile : 128 * tile + 128
                ]
        if x in (3, 5):
            first_row, count = (0, 72) if x == 3 else (72, 40)
            if x == 5:
                for slab in range(SLABS):
                    out_ref[ROWS * slab + 108 : ROWS * slab + 112, :] = jnp.zeros((4, 128), jnp.float32)
            for slab in range(SLABS):
                place = pl.ds(ROWS * slab + first_row, count)
                outs.append(
                    pltpu.make_async_copy(out_ref.at[place], out_hbm.at[place], sems.at[5 + len(outs)])
                )
                outs[-1].start()
    for copy in outs:
        copy.wait()


def line_kernel(in_ref, hat_ref, table_hbm, out_ref, y_ref, u_ref, table_ref, sems):
    fetches = []
    for row, count in ((WY, WI - WY), (TX, LINES - TX), (WI, TX - WI)):
        place = (slice(None), pl.ds(row, count))
        pair = (table_hbm.at[place], table_ref.at[place])
        fetches.append(pltpu.make_async_copy(*pair, sems.at[len(fetches)]))
    for copy in fetches:
        copy.start()
    def table(row, count, columns=256):
        return [table_ref[part, row : row + count, :columns] for part in range(2)]

    pieces = []
    for kp in range(KP):
        for x in range(XS):
            pieces.append(
                jnp.concatenate(
                    [
                        in_ref[pl.ds(18 * x + 6 * tile + kp, SLABS, stride=ROWS), :]
                        for tile in range(3)
                    ],
                    axis=1,
                )
            )
    data = split(jnp.concatenate(pieces, axis=0))
    fetches[0].wait()
    for kz2 in range(2):
        window = [part[:, 128 * kz2 : 128 * kz2 + 256] for part in data]
        for c in range(2):
            result = mm(window, table(WY + 320 * c + 64 * (1 - kz2), 256))
            for kp in range(KP):
                y_ref[2 * kp + kz2, 96 * c : 96 * c + 96, :] = result[96 * kp : 96 * kp + 96]
    for copy in fetches[1:]:
        copy.wait()
    for kz in range(2 * KP):
        lined = split(y_ref[kz, :, :N])
        spectrum = mm(table(TX, 384, N), lined)
        hat = hat_ref[kz]
        u_ref[kz, :, :N] = mm(table(TI, N, N), split(spectrum[:N] * hat)) + mm(
            table(TI + N, N, N), split(spectrum[N:] * hat)
        )
    sides = []
    for kz2 in range(2):
        rows = [
            [u_ref[2 * kp + kz2, G * c : G * c + G, :N] for kp in range(KP)] for c in range(2)
        ]
        re, im = [split(jnp.concatenate(part, axis=0)) for part in rows]
        first = WI + 512 * kz2
        sides.append(mm(re, table(first, N)) + mm(im, table(first + 256, N)))
    wide = [sides[0][:, :128], sides[0][:, 128:] + sides[1][:, :128], sides[1][:, 128:]]
    for kp in range(KP):
        for x in range(XS):
            for tile in range(3):
                row = 96 * kp + 16 * x
                out_ref[pl.ds(18 * x + 6 * tile + kp, SLABS, stride=ROWS), :] = wide[tile][
                    row : row + 16
                ]


def term_kernel(
    upper_ref, occupation_ref, in_ref, own_ref, their_hbm, tv_ref, kept_ref, sent_ref, their_ref,
    field_ref, sem
):
    fetch = pltpu.make_async_copy(their_hbm, their_ref, sem)
    fetch.start()
    upper = upper_ref[0] == 1
    table = (tv_ref[0], tv_ref[1])
    weight = [0.25 * occupation_ref[o].astype(jnp.float32) for o in range(2)]
    for x in range(XS):
        pieces = [
            jnp.concatenate(
                [
                    in_ref[pl.ds(18 * x + 6 * tile + kp, SLABS, stride=ROWS), :]
                    for tile in range(3)
                ],
                axis=1,
            )
            for kp in range(KP)
        ]
        wide = jnp.concatenate(pieces, axis=0)
        stacked = jnp.concatenate([wide[:, 96 * j : 96 * j + 96] for j in range(4)], axis=0)
        fields = mm(table, split(stacked)).T
        field_ref[0, x] = dense_of(fields[:, :96])
        field_ref[1, x] = dense_of(fields[:, 128:224])
    fetch.wait()
    for x in range(XS):
        one, two = field_ref[0, x], field_ref[1, x]
        theirs = [plane(their_ref, x, o) for o in range(2)]
        first = jnp.where(upper, theirs[1], theirs[0])
        second = jnp.where(upper, theirs[0], theirs[1])
        kept = [one * first, two * second]
        mine_one = one * plane(own_ref, x, 0) * weight[0]
        mine_two = two * plane(own_ref, x, 1) * weight[1]
        sent = [jnp.where(upper, mine_two, mine_one), jnp.where(upper, mine_one, mine_two)]
        for o in range(2):
            for tile in range(3):
                place = pl.ds(144 * x + o + 2 * tile, 24, stride=6)
                kept_ref[place, :] = kept[o][:, 128 * tile : 128 * tile + 128]
                sent_ref[place, :] = sent[o][:, 128 * tile : 128 * tile + 128]
    row = lax.broadcasted_iota(jnp.int32, (8, 128), 0)
    sent_ref[864:872, :] = jnp.where(row % 2 == 1, weight[1], weight[0])


PARTS = ((864, 8), (0, 216), (216, 216), (432, 216), (648, 216))


def sum_kernel(upper_ref, kept_ref, come_hbm, out_hbm, come_ref, out_ref, sems):
    fetches, outs = [], []
    for k, (row, count) in enumerate(PARTS):
        place = pl.ds(row, count)
        fetches.append(pltpu.make_async_copy(come_hbm.at[place], come_ref.at[place], sems.at[k]))
        fetches[-1].start()
    upper = upper_ref[0] == 1
    odd_row = lax.broadcasted_iota(jnp.int32, (216, 128), 0) % 2 == 1
    fetches[0].wait()
    even = jnp.where(upper, come_ref[865:866, :], come_ref[864:865, :])
    odd = jnp.where(upper, come_ref[864:865, :], come_ref[865:866, :])
    weight = jnp.where(odd_row, odd, even)
    for k, (row, count) in enumerate(PARTS[1:], 1):
        place = pl.ds(row, count)
        fetches[k].wait()
        out_ref[place, :] = -(kept_ref[place, :] * weight + come_ref[place, :])
        outs.append(pltpu.make_async_copy(out_ref.at[place], out_hbm.at[place], sems.at[4 + k]))
        outs[-1].start()
    for copy in outs:
        copy.wait()


SMEM = pl.BlockSpec(memory_space=pltpu.SMEM)
VMEM = pl.BlockSpec(memory_space=pltpu.VMEM)
HBM = pl.BlockSpec(memory_space=pltpu.HBM)


def call(kernel, ins, outs, args, scratch=(), out_spec=VMEM, limit=28_000_000):
    shapes = [o if isinstance(o, jax.ShapeDtypeStruct) else jax.ShapeDtypeStruct(o, jnp.float32) for o in outs]
    many = len(shapes) > 1
    return pl.pallas_call(
        kernel,
        out_shape=shapes if many else shapes[0],
        in_specs=ins,
        out_specs=[out_spec] * len(outs) if many else out_spec,
        scratch_shapes=scratch,
        compiler_params=pltpu.CompilerParams(vmem_limit_bytes=limit),
    )(*args)


def to_partner(value, pair_bits):
    group_count = lax.axis_size("grp")

    def by_mask(mask):
        pairs = [(source, source ^ mask) for source in range(group_count)]
        return lambda sent: lax.ppermute(sent, "grp", pairs)

    branches = [by_mask(mask) for mask in range(1, group_count)]
    return lax.switch(pair_bits - 1, branches, value)


def to_rows(planes):
    return planes.reshape(2, XS, 72, 128).transpose(1, 2, 0, 3).reshape(864, 128)


def from_rows(rows):
    return rows.reshape(XS, 72, 2, 128).transpose(2, 0, 1, 3).reshape(2, XS, G * G)


def exchange(chunks):
    chunks = chunks.reshape(SLABS, ROWS, 128)
    moved = lax.all_to_all(chunks, "slab", split_axis=0, concat_axis=0, tiled=True)
    return moved.reshape(SLABS * ROWS, 128)


def local(orbitals, occupation, kernel_hat, pair_mask):
    tz, lines_table, tv = [jnp.asarray(t) for t in tables()]
    pair_bits = pair_mask[0]
    own_group = lax.axis_index("grp")
    upper = (own_group > jnp.bitwise_xor(own_group, pair_bits)).astype(jnp.int32).reshape(1)
    own = to_rows(orbitals)
    theirs = to_partner(own, pair_bits)
    chunk = (SLABS * ROWS, 128)
    rows = pltpu.VMEM((864, 128), jnp.float32)
    spread = call(
        spread_kernel,
        [SMEM, HBM, HBM, HBM],
        [chunk],
        (upper, own, theirs, tz),
        [rows, rows, pltpu.VMEM(tz.shape, tz.dtype), pltpu.VMEM(chunk, jnp.float32)]
        + [pltpu.SemaphoreType.DMA((5 + 2 * SLABS,))],
        HBM,
        66_800_000,
    )
    hat = kernel_hat.reshape(2 * KP, N, N).transpose(0, 2, 1)
    scratch = [pltpu.VMEM((2 * KP, N, 256), jnp.float32)] * 2
    scratch += [pltpu.VMEM(lines_table.shape, lines_table.dtype), pltpu.SemaphoreType.DMA((3,))]
    lined = call(
        line_kernel,
        [VMEM, VMEM, HBM],
        [chunk],
        (exchange(spread), hat, lines_table),
        scratch,
        limit=51_000_000,
    )
    back = exchange(lined)
    kept, sent = call(
        term_kernel,
        [SMEM, SMEM, VMEM, VMEM, HBM, VMEM],
        [(864, 128), (872, 128)],
        (upper, occupation, back, own, theirs, tv),
        [rows, pltpu.VMEM((2, XS, 24, 384), jnp.float32), pltpu.SemaphoreType.DMA],
    )

    come = to_partner(sent, pair_bits)
    scratch = [pltpu.VMEM((872, 128), jnp.float32), rows, pltpu.SemaphoreType.DMA((9,))]
    total = call(sum_kernel, [SMEM, VMEM, HBM], [(864, 128)], (upper, kept, come), scratch, HBM)
    return from_rows(total)


def solution(mesh):
    return jax.shard_map(
        local,
        mesh=mesh,
        in_specs=(P("grp", "slab", None), P("grp"), P("slab", None), P()),
        out_specs=P("grp", "slab", None),
        check_vma=False,
    )
```

```python
import functools
import math

import jax
import jax.numpy as jnp
import numpy as np
from jax import lax
from jax.experimental import pallas as pl
from jax.experimental.pallas import tpu as pltpu
from jax.sharding import PartitionSpec as P

G = 96
N = 192
SLABS = 16
XS = 6
KP = 6
ROWS = 112

Y_ORDER = np.array([4 * (i % 24) + i // 24 for i in range(G)])
X_ORDER = np.array([6 * (i % SLABS) + i // SLABS for i in range(G)])


WY, WI, TX, TI, LINES = 0, 640, 1664, 2048, 2432


def split(table):
    table = jnp.asarray(table, jnp.float32)
    high = table.astype(jnp.bfloat16)
    low = (table - high.astype(jnp.float32)).astype(jnp.bfloat16)
    return high, low


def np_split(table):
    bf16 = jnp.bfloat16
    high = table.astype(np.float32).astype(bf16)
    low = (table - high.astype(np.float64)).astype(np.float32).astype(bf16)
    return np.stack([high, low])


def waves(freq, cell):
    angle = (np.outer(freq, cell) % N) * (2.0 * math.pi / N)
    return np.cos(angle), np.sin(angle)


@functools.cache
def tables():
    pair_major = np.array([[12 * d + 2 * kp for d in range(SLABS)] for kp in range(KP)]).reshape(-1)
    tz = np.zeros((384, 256))
    tv = np.zeros((256, 384))
    wy = np.zeros((320, 512))
    wi = np.zeros((2, 512, 256))
    for kz2 in range(2):
        cos, sin = waves(pair_major + kz2, np.arange(G))
        re, im = 192 * kz2, 192 * kz2 + 96
        tz[re : re + 96, 0:96], tz[re : re + 96, 128:224] = cos, sin
        tz[im : im + 96, 0:96], tz[im : im + 96, 128:224] = -sin, cos
        tv[0:96, re : re + 96], tv[0:96, im : im + 96] = cos.T / N, -sin.T / N
        tv[128:224, re : re + 96], tv[128:224, im : im + 96] = sin.T / N, cos.T / N
        cos, sin = waves(Y_ORDER, np.arange(N))
        wy[64:160, 0:192], wy[64:160, 256:448] = cos, -sin
        wy[160:256, 0:192], wy[160:256, 256:448] = sin, cos
        re, im = 64 * kz2, 64 * kz2 + 96
        wi[kz2, 0:192, re : re + 96], wi[kz2, 0:192, im : im + 96] = cos.T / N, sin.T / N
        wi[kz2, 256:448, re : re + 96], wi[kz2, 256:448, im : im + 96] = -sin.T / N, cos.T / N
    cos, sin = waves(np.arange(N), X_ORDER)
    tx = np.block([[cos, sin], [-sin, cos]])
    ti = np.block([[cos.T, -sin.T], [sin.T, cos.T]]) / N
    lines = [wy[:, :256], wy[:, 256:], wi[0], wi[1], widened(tx), widened(ti[:, :N]), widened(ti[:, N:])]
    return [np_split(t) for t in (tz, np.concatenate(lines, axis=0), tv)]


def widened(table):
    return np.pad(table, ((0, 0), (0, 256 - N)))


def mm(left, right, form=(1, 0)):
    def one(a, b):
        return lax.dot_general(
            a, b, (((form[0],), (form[1],)), ((), ())), preferred_element_type=jnp.float32
        )

    return one(left[0], right[0]) + (one(left[0], right[1]) + one(left[1], right[0]))


def plane(ref, x, orbital):
    base = 144 * x + orbital
    tiles = [ref[pl.ds(base + 2 * tile, 24, stride=6), :] for tile in range(3)]
    return jnp.concatenate(tiles, axis=1)


def lines(dense):
    return jnp.concatenate([dense[:, 96 * q : 96 * q + 96] for q in range(4)], axis=0)


def dense_of(rows):
    return jnp.concatenate([rows[24 * q : 24 * q + 24] for q in range(4)], axis=1)


def near_kernel(own_hbm, tz_hbm, own_ref, tz_ref, sems):
    copies = [
        pltpu.make_async_copy(own_hbm, own_ref, sems.at[0]),
        pltpu.make_async_copy(tz_hbm, tz_ref, sems.at[1]),
    ]
    for copy in copies:
        copy.start()
    for copy in copies:
        copy.wait()


def spread_kernel(
    upper_ref, own_ref, their_ref, tz_ref, their_hbm, out_hbm, out_ref, sems, their_sem
):
    kept = pltpu.make_async_copy(their_ref, their_hbm, their_sem)
    kept.start()
    upper = upper_ref[0] == 1
    pad = jnp.zeros((G, 32), jnp.float32)
    outs = []
    for x in range(XS):
        theirs = [plane(their_ref, x, o) for o in range(2)]
        first = jnp.where(upper, theirs[1], theirs[0])
        second = jnp.where(upper, theirs[0], theirs[1])
        one = lines(plane(own_ref, x, 0) * first)
        two = lines(plane(own_ref, x, 1) * second)
        density = jnp.concatenate([one, pad, two, pad], axis=1)
        lined = mm((tz_ref[0], tz_ref[1]), split(density), (1, 1))
        wide = jnp.concatenate([lined[96 * j : 96 * j + 96] for j in range(4)], axis=1)
        for kp in range(KP):
            for tile in range(3):
                out_ref[pl.ds(18 * x + 6 * tile + kp, SLABS, stride=ROWS), :] = wide[
                    16 * kp : 16 * kp + 16, 128 * tile : 128 * tile + 128
                ]
        if x in (3, 5):
            first_row, count = (0, 72) if x == 3 else (72, 40)
            if x == 5:
                for slab in range(SLABS):
                    out_ref[ROWS * slab + 108 : ROWS * slab + 112, :] = jnp.zeros((4, 128), jnp.float32)
            for slab in range(SLABS):
                place = pl.ds(ROWS * slab + first_row, count)
                outs.append(
                    pltpu.make_async_copy(out_ref.at[place], out_hbm.at[place], sems.at[len(outs)])
                )
                outs[-1].start()
    for copy in outs:
        copy.wait()
    kept.wait()


def line_kernel(in_ref, hat_ref, table_hbm, out_ref, y_ref, u_ref, table_ref, sems):
    fetches = []
    for row, count in ((WY, WI - WY), (TX, LINES - TX), (WI, TX - WI)):
        place = (slice(None), pl.ds(row, count))
        pair = (table_hbm.at[place], table_ref.at[place])
        fetches.append(pltpu.make_async_copy(*pair, sems.at[len(fetches)]))
    for copy in fetches:
        copy.start()
    def table(row, count, columns=256):
        return [table_ref[part, row : row + count, :columns] for part in range(2)]

    pieces = []
    for kp in range(KP):
        for x in range(XS):
            pieces.append(
                jnp.concatenate(
                    [
                        in_ref[pl.ds(18 * x + 6 * tile + kp, SLABS, stride=ROWS), :]
                        for tile in range(3)
                    ],
                    axis=1,
                )
            )
    data = split(jnp.concatenate(pieces, axis=0))
    fetches[0].wait()
    for kz2 in range(2):
        window = [part[:, 128 * kz2 : 128 * kz2 + 256] for part in data]
        for c in range(2):
            result = mm(window, table(WY + 320 * c + 64 * (1 - kz2), 256))
            for kp in range(KP):
                y_ref[2 * kp + kz2, 96 * c : 96 * c + 96, :] = result[96 * kp : 96 * kp + 96]
    fetches[1].wait()
    for kz in range(2 * KP):
        lined = split(y_ref[kz, :, :N])
        spectrum = mm(table(TX, 384, N), lined)
        hat = hat_ref[kz]
        u_ref[kz, :, :N] = mm(table(TI, N, N), split(spectrum[:N] * hat)) + mm(
            table(TI + N, N, N), split(spectrum[N:] * hat)
        )
    fetches[2].wait()
    sides = []
    for kz2 in range(2):
        rows = [
            [u_ref[2 * kp + kz2, G * c : G * c + G, :N] for kp in range(KP)] for c in range(2)
        ]
        re, im = [split(jnp.concatenate(part, axis=0)) for part in rows]
        first = WI + 512 * kz2
        sides.append(mm(re, table(first, N)) + mm(im, table(first + 256, N)))
    wide = [sides[0][:, :128], sides[0][:, 128:] + sides[1][:, :128], sides[1][:, 128:]]
    for kp in range(KP):
        for x in range(XS):
            for tile in range(3):
                row = 96 * kp + 16 * x
                out_ref[pl.ds(18 * x + 6 * tile + kp, SLABS, stride=ROWS), :] = wide[tile][
                    row : row + 16
                ]


def term_kernel(
    upper_ref, occupation_ref, in_ref, own_ref, their_hbm, tv_ref, kept_ref, sent_ref, their_ref,
    field_ref, sem
):
    fetch = pltpu.make_async_copy(their_hbm, their_ref, sem)
    fetch.start()
    upper = upper_ref[0] == 1
    table = (tv_ref[0], tv_ref[1])
    weight = [0.25 * occupation_ref[o].astype(jnp.float32) for o in range(2)]
    for x in range(XS):
        pieces = [
            jnp.concatenate(
                [
                    in_ref[pl.ds(18 * x + 6 * tile + kp, SLABS, stride=ROWS), :]
                    for tile in range(3)
                ],
                axis=1,
            )
            for kp in range(KP)
        ]
        wide = jnp.concatenate(pieces, axis=0)
        stacked = jnp.concatenate([wide[:, 96 * j : 96 * j + 96] for j in range(4)], axis=0)
        fields = mm(table, split(stacked)).T
        field_ref[0, x] = dense_of(fields[:, :96])
        field_ref[1, x] = dense_of(fields[:, 128:224])
    fetch.wait()
    for x in range(XS):
        one, two = field_ref[0, x], field_ref[1, x]
        theirs = [plane(their_ref, x, o) for o in range(2)]
        first = jnp.where(upper, theirs[1], theirs[0])
        second = jnp.where(upper, theirs[0], theirs[1])
        kept = [one * first, two * second]
        mine_one = one * plane(own_ref, x, 0) * weight[0]
        mine_two = two * plane(own_ref, x, 1) * weight[1]
        sent = [jnp.where(upper, mine_two, mine_one), jnp.where(upper, mine_one, mine_two)]
        for o in range(2):
            for tile in range(3):
                place = pl.ds(144 * x + o + 2 * tile, 24, stride=6)
                kept_ref[place, :] = kept[o][:, 128 * tile : 128 * tile + 128]
                sent_ref[place, :] = sent[o][:, 128 * tile : 128 * tile + 128]
    row = lax.broadcasted_iota(jnp.int32, (8, 128), 0)
    sent_ref[864:872, :] = jnp.where(row % 2 == 1, weight[1], weight[0])


PARTS = ((864, 8), (0, 216), (216, 216), (432, 216), (648, 216))


def sum_kernel(upper_ref, kept_ref, come_hbm, out_hbm, come_ref, out_ref, sems):
    fetches, outs = [], []
    for k, (row, count) in enumerate(PARTS):
        place = pl.ds(row, count)
        fetches.append(pltpu.make_async_copy(come_hbm.at[place], come_ref.at[place], sems.at[k]))
        fetches[-1].start()
    upper = upper_ref[0] == 1
    odd_row = lax.broadcasted_iota(jnp.int32, (216, 128), 0) % 2 == 1
    fetches[0].wait()
    even = jnp.where(upper, come_ref[865:866, :], come_ref[864:865, :])
    odd = jnp.where(upper, come_ref[864:865, :], come_ref[865:866, :])
    weight = jnp.where(odd_row, odd, even)
    for k, (row, count) in enumerate(PARTS[1:], 1):
        place = pl.ds(row, count)
        fetches[k].wait()
        out_ref[place, :] = -(kept_ref[place, :] * weight + come_ref[place, :])
        outs.append(pltpu.make_async_copy(out_ref.at[place], out_hbm.at[place], sems.at[4 + k]))
        outs[-1].start()
    for copy in outs:
        copy.wait()


SMEM = pl.BlockSpec(memory_space=pltpu.SMEM)
VMEM = pl.BlockSpec(memory_space=pltpu.VMEM)
HBM = pl.BlockSpec(memory_space=pltpu.HBM)


def call(kernel, ins, outs, args, scratch=(), out_spec=VMEM, limit=28_000_000):
    shapes = [o if isinstance(o, jax.ShapeDtypeStruct) else jax.ShapeDtypeStruct(o, jnp.float32) for o in outs]
    many = len(shapes) > 1
    return pl.pallas_call(
        kernel,
        out_shape=shapes if many else shapes[0],
        in_specs=ins,
        out_specs=[out_spec] * len(outs) if many else out_spec,
        scratch_shapes=scratch,
        compiler_params=pltpu.CompilerParams(vmem_limit_bytes=limit),
    )(*args)


def to_partner(value, pair_bits, then=lambda come: come, *others):
    group_count = lax.axis_size("grp")

    def by_mask(mask):
        pairs = [(source, source ^ mask) for source in range(group_count)]
        return lambda given: then(lax.ppermute(given[0], "grp", pairs), *given[1:])

    branches = [by_mask(mask) for mask in range(1, group_count)]
    return lax.switch(pair_bits - 1, branches, (value, *others))


def to_rows(planes):
    return planes.reshape(2, XS, 72, 128).transpose(1, 2, 0, 3).reshape(864, 128)


def from_rows(rows):
    return rows.reshape(XS, 72, 2, 128).transpose(2, 0, 1, 3).reshape(2, XS, G * G)


def exchange(chunks):
    chunks = chunks.reshape(SLABS, ROWS, 128)
    moved = lax.all_to_all(chunks, "slab", split_axis=0, concat_axis=0, tiled=True)
    return moved.reshape(SLABS * ROWS, 128)


def local(orbitals, occupation, kernel_hat, pair_mask):
    tz, lines_table, tv = [jnp.asarray(t) for t in tables()]
    pair_bits = pair_mask[0]
    own_group = lax.axis_index("grp")
    upper = (own_group > jnp.bitwise_xor(own_group, pair_bits)).astype(jnp.int32).reshape(1)
    own = to_rows(orbitals)
    chunk = (SLABS * ROWS, 128)
    rows = pltpu.VMEM((864, 128), jnp.float32)

    def spread_out(theirs, own, upper, tz):
        near = [jax.ShapeDtypeStruct(a.shape, a.dtype) for a in (own, tz)]
        own, tz = call(near_kernel, [HBM] * 2, near, (own, tz), [pltpu.SemaphoreType.DMA((2,))])
        scratch = [pltpu.VMEM(chunk, jnp.float32), pltpu.SemaphoreType.DMA((2 * SLABS,))]
        scratch.append(pltpu.SemaphoreType.DMA)
        operands = (upper, own, theirs, tz)
        outs = [(864, 128), chunk]
        return call(spread_kernel, [SMEM] + [VMEM] * 3, outs, operands, scratch, HBM)

    theirs, spread = to_partner(own, pair_bits, spread_out, own, upper, tz)
    hat = kernel_hat.reshape(2 * KP, N, N).transpose(0, 2, 1)
    scratch = [pltpu.VMEM((2 * KP, N, 256), jnp.float32)] * 2
    scratch += [pltpu.VMEM(lines_table.shape, lines_table.dtype), pltpu.SemaphoreType.DMA((3,))]
    lined = call(
        line_kernel,
        [VMEM, VMEM, HBM],
        [chunk],
        (exchange(spread), hat, lines_table),
        scratch,
        limit=51_000_000,
    )
    back = exchange(lined)
    kept, sent = call(
        term_kernel,
        [SMEM, SMEM, VMEM, VMEM, HBM, VMEM],
        [(864, 128), (872, 128)],
        (upper, occupation, back, own, theirs, tv),
        [rows, pltpu.VMEM((2, XS, 24, 384), jnp.float32), pltpu.SemaphoreType.DMA],
    )

    come = to_partner(sent, pair_bits)
    scratch = [pltpu.VMEM((872, 128), jnp.float32), rows, pltpu.SemaphoreType.DMA((9,))]
    total = call(sum_kernel, [SMEM, VMEM, HBM], [(864, 128)], (upper, kept, come), scratch, HBM)
    return from_rows(total)


def solution(mesh):
    return jax.shard_map(
        local,
        mesh=mesh,
        in_specs=(P("grp", "slab", None), P("grp"), P("slab", None), P()),
        out_specs=P("grp", "slab", None),
        check_vma=False,
    )
```

```python
import functools
import math

import jax
import jax.numpy as jnp
import numpy as np
from jax import lax
from jax.experimental import pallas as pl
from jax.experimental.pallas import tpu as pltpu
from jax.sharding import PartitionSpec as P

G = 96
N = 192
SLABS = 16
XS = 6
KP = 6
ROWS = 112

Y_ORDER = np.array([4 * (i % 24) + i // 24 for i in range(G)])
X_ORDER = np.array([6 * (i % SLABS) + i // SLABS for i in range(G)])


WY, WI, TX, TI, LINES = 0, 640, 1280, 1472, 1664


def split(table):
    table = jnp.asarray(table, jnp.float32)
    high = table.astype(jnp.bfloat16)
    low = (table - high.astype(jnp.float32)).astype(jnp.bfloat16)
    return high, low


def np_split(table):
    bf16 = jnp.bfloat16
    high = table.astype(np.float32).astype(bf16)
    low = (table - high.astype(np.float64)).astype(np.float32).astype(bf16)
    return np.stack([high, low])


def waves(freq, cell):
    angle = (np.outer(freq, cell) % N) * (2.0 * math.pi / N)
    return np.cos(angle), np.sin(angle)


@functools.cache
def tables():
    pair_major = np.array([[12 * d + 2 * kp for d in range(SLABS)] for kp in range(KP)]).reshape(-1)
    tz = np.zeros((384, 256))
    tv = np.zeros((256, 384))
    wy = np.zeros((640, 256))
    wi = np.zeros((640, 256))
    for kz2 in range(2):
        cos, sin = waves(pair_major + kz2, np.arange(G))
        re, im = 192 * kz2, 192 * kz2 + 96
        tz[re : re + 96, 0:96], tz[re : re + 96, 128:224] = cos, sin
        tz[im : im + 96, 0:96], tz[im : im + 96, 128:224] = -sin, cos
        tv[0:96, re : re + 96], tv[0:96, im : im + 96] = cos.T / N, -sin.T / N
        tv[128:224, re : re + 96], tv[128:224, im : im + 96] = sin.T / N, cos.T / N
    cos, sin = waves(Y_ORDER, np.arange(N))
    wy[64:160, :N], wy[160:256, :N] = cos, sin
    wy[384:480, :N], wy[480:576, :N] = -sin, cos
    wi[64:256, 0:96], wi[64:256, 96:192] = cos.T / N, sin.T / N
    wi[384:576, 0:96], wi[384:576, 96:192] = -sin.T / N, cos.T / N
    cos, sin = waves(np.arange(G), X_ORDER)
    sin[0] = waves(np.array([G]), X_ORDER)[0][0]
    tx = np.concatenate([cos, sin], axis=0)
    ti = np.block([[cos.T, -sin.T], [cos.T, sin.T]]) / N
    lines = [wy, wi, widened(tx), widened(ti)]
    return [np_split(t) for t in (tz, np.concatenate(lines, axis=0), tv)]


def widened(table):
    return np.pad(table, ((0, 0), (0, 256 - table.shape[1])))


def mm(left, right, form=(1, 0)):
    def one(a, b):
        return lax.dot_general(
            a, b, (((form[0],), (form[1],)), ((), ())), preferred_element_type=jnp.float32
        )

    return one(left[0], right[0]) + (one(left[0], right[1]) + one(left[1], right[0]))


def plane(ref, x, orbital):
    base = 144 * x + orbital
    tiles = [ref[pl.ds(base + 2 * tile, 24, stride=6), :] for tile in range(3)]
    return jnp.concatenate(tiles, axis=1)


def lines(dense):
    return jnp.concatenate([dense[:, 96 * q : 96 * q + 96] for q in range(4)], axis=0)


def dense_of(rows):
    return jnp.concatenate([rows[24 * q : 24 * q + 24] for q in range(4)], axis=1)


def near_kernel(own_hbm, tz_hbm, own_ref, tz_ref, sems):
    copies = [
        pltpu.make_async_copy(own_hbm, own_ref, sems.at[0]),
        pltpu.make_async_copy(tz_hbm, tz_ref, sems.at[1]),
    ]
    for copy in copies:
        copy.start()
    for copy in copies:
        copy.wait()


def spread_kernel(
    upper_ref, own_ref, their_ref, tz_ref, their_hbm, out_hbm, out_ref, sems, their_sem
):
    kept = pltpu.make_async_copy(their_ref, their_hbm, their_sem)
    kept.start()
    upper = upper_ref[0] == 1
    pad = jnp.zeros((G, 32), jnp.float32)
    outs = []
    for x in range(XS):
        theirs = [plane(their_ref, x, o) for o in range(2)]
        first = jnp.where(upper, theirs[1], theirs[0])
        second = jnp.where(upper, theirs[0], theirs[1])
        one = lines(plane(own_ref, x, 0) * first)
        two = lines(plane(own_ref, x, 1) * second)
        density = jnp.concatenate([one, pad, two, pad], axis=1)
        lined = mm((tz_ref[0], tz_ref[1]), split(density), (1, 1))
        wide = jnp.concatenate([lined[96 * j : 96 * j + 96] for j in range(4)], axis=1)
        for kp in range(KP):
            for tile in range(3):
                out_ref[pl.ds(18 * x + 6 * tile + kp, SLABS, stride=ROWS), :] = wide[
                    16 * kp : 16 * kp + 16, 128 * tile : 128 * tile + 128
                ]
        if x in (3, 5):
            first_row, count = (0, 72) if x == 3 else (72, 40)
            if x == 5:
                for slab in range(SLABS):
                    out_ref[ROWS * slab + 108 : ROWS * slab + 112, :] = jnp.zeros((4, 128), jnp.float32)
            for slab in range(SLABS):
                place = pl.ds(ROWS * slab + first_row, count)
                outs.append(
                    pltpu.make_async_copy(out_ref.at[place], out_hbm.at[place], sems.at[len(outs)])
                )
                outs[-1].start()
    for copy in outs:
        copy.wait()
    kept.wait()


def side_by_side(left, right):
    right = pltpu.roll(right, 64, 1)
    return jnp.concatenate(
        [left[:, :128], left[:, 128:] + right[:, :128], right[:, 128:]], axis=1
    )


def line_kernel(in_ref, hat_hbm, table_hbm, out_ref, y_ref, u_ref, hat_ref, table_ref, sems):
    fetches = []
    for row, count in ((WY, WI - WY), (TX, LINES - TX), (WI, TX - WI)):
        place = (slice(None), pl.ds(row, count))
        pair = (table_hbm.at[place], table_ref.at[place])
        fetches.append(pltpu.make_async_copy(*pair, sems.at[len(fetches)]))
    fetches.insert(2, pltpu.make_async_copy(hat_hbm, hat_ref, sems.at[3]))
    for copy in fetches:
        copy.start()
    def table(row, count, columns=256):
        return [table_ref[part, row : row + count, :columns] for part in range(2)]

    pieces = []
    for kp in range(KP):
        for x in range(XS):
            pieces.append(
                jnp.concatenate(
                    [
                        in_ref[pl.ds(18 * x + 6 * tile + kp, SLABS, stride=ROWS), :]
                        for tile in range(3)
                    ],
                    axis=1,
                )
            )
    data = split(jnp.concatenate(pieces, axis=0))
    fetches[0].wait()
    for c in range(2):
        result = []
        for kz2 in range(2):
            window = [part[:, 128 * kz2 : 128 * kz2 + 256] for part in data]
            result.append(mm(window, table(WY + 320 * c + 64 * (1 - kz2), 256)))
        paired = side_by_side(*result)
        for kp in range(KP):
            lanes = slice(384 * (kp % 2), 384 * (kp % 2) + 384)
            y_ref[kp // 2, c, :, lanes] = paired[96 * kp : 96 * kp + 96]
    fetches[1].wait()
    fetches[2].wait()
    first_row = lax.broadcasted_iota(jnp.int32, (G, 768), 0) == 0
    for q in range(3):
        forward = table(TX, N, G)
        re = mm(forward, split(y_ref[q, 0]))
        im = mm(forward, split(y_ref[q, 1]))
        even, odd = hat_ref[q, :G], hat_ref[q, G:N]
        even_sin = jnp.where(first_row, hat_ref[q, N : N + 1], even)
        cos_re = even * re[:G] + odd * im[G:]
        sin_im = odd * im[:G] - even_sin * re[G:]
        cos_im = even * im[:G] - odd * re[G:]
        sin_re = odd * re[:G] + even_sin * im[G:]
        u_ref[q, 0] = mm(table(TI, G, N), split(jnp.concatenate([cos_re, sin_im], axis=0)))
        u_ref[q, 1] = mm(table(TI + G, G, N), split(jnp.concatenate([cos_im, sin_re], axis=0)))
    fetches[3].wait()
    sides = []
    for kz2 in range(2):
        parts = []
        for c in range(2):
            rows = []
            for kp in range(KP):
                lane = 384 * (kp % 2) + 128 * kz2
                rows.append(u_ref[kp // 2, c, :, lane : lane + 256])
            back = split(jnp.concatenate(rows, axis=0))
            parts.append(mm(back, table(WI + 320 * c + 64 * (1 - kz2), 256)))
        sides.append(parts[0] + parts[1])
    wide = side_by_side(*sides)
    for kp in range(KP):
        for x in range(XS):
            for tile in range(3):
                row = 96 * kp + 16 * x
                out_ref[pl.ds(18 * x + 6 * tile + kp, SLABS, stride=ROWS), :] = wide[
                    row : row + 16, 128 * tile : 128 * tile + 128
                ]


def term_kernel(
    upper_ref, occupation_ref, in_ref, own_ref, their_hbm, tv_ref, kept_ref, sent_ref, their_ref,
    field_ref, sem
):
    fetch = pltpu.make_async_copy(their_hbm, their_ref, sem)
    fetch.start()
    upper = upper_ref[0] == 1
    table = (tv_ref[0], tv_ref[1])
    weight = [0.25 * occupation_ref[o].astype(jnp.float32) for o in range(2)]
    for x in range(XS):
        pieces = [
            jnp.concatenate(
                [
                    in_ref[pl.ds(18 * x + 6 * tile + kp, SLABS, stride=ROWS), :]
                    for tile in range(3)
                ],
                axis=1,
            )
            for kp in range(KP)
        ]
        wide = jnp.concatenate(pieces, axis=0)
        stacked = jnp.concatenate([wide[:, 96 * j : 96 * j + 96] for j in range(4)], axis=0)
        fields = mm(table, split(stacked)).T
        field_ref[0, x] = dense_of(fields[:, :96])
        field_ref[1, x] = dense_of(fields[:, 128:224])
    fetch.wait()
    for x in range(XS):
        one, two = field_ref[0, x], field_ref[1, x]
        theirs = [plane(their_ref, x, o) for o in range(2)]
        first = jnp.where(upper, theirs[1], theirs[0])
        second = jnp.where(upper, theirs[0], theirs[1])
        kept = [one * first, two * second]
        mine_one = one * plane(own_ref, x, 0) * weight[0]
        mine_two = two * plane(own_ref, x, 1) * weight[1]
        sent = [jnp.where(upper, mine_two, mine_one), jnp.where(upper, mine_one, mine_two)]
        for o in range(2):
            for tile in range(3):
                place = pl.ds(144 * x + o + 2 * tile, 24, stride=6)
                kept_ref[place, :] = kept[o][:, 128 * tile : 128 * tile + 128]
                sent_ref[place, :] = sent[o][:, 128 * tile : 128 * tile + 128]
    row = lax.broadcasted_iota(jnp.int32, (8, 128), 0)
    sent_ref[864:872, :] = jnp.where(row % 2 == 1, weight[1], weight[0])


PARTS = ((864, 8), (0, 216), (216, 216), (432, 216), (648, 216))


def sum_kernel(upper_ref, kept_ref, come_hbm, out_hbm, come_ref, out_ref, sems):
    fetches, outs = [], []
    for k, (row, count) in enumerate(PARTS):
        place = pl.ds(row, count)
        fetches.append(pltpu.make_async_copy(come_hbm.at[place], come_ref.at[place], sems.at[k]))
        fetches[-1].start()
    upper = upper_ref[0] == 1
    odd_row = lax.broadcasted_iota(jnp.int32, (216, 128), 0) % 2 == 1
    fetches[0].wait()
    even = jnp.where(upper, come_ref[865:866, :], come_ref[864:865, :])
    odd = jnp.where(upper, come_ref[864:865, :], come_ref[865:866, :])
    weight = jnp.where(odd_row, odd, even)
    for k, (row, count) in enumerate(PARTS[1:], 1):
        place = pl.ds(row, count)
        fetches[k].wait()
        out_ref[place, :] = -(kept_ref[place, :] * weight + come_ref[place, :])
        outs.append(pltpu.make_async_copy(out_ref.at[place], out_hbm.at[place], sems.at[4 + k]))
        outs[-1].start()
    for copy in outs:
        copy.wait()


SMEM = pl.BlockSpec(memory_space=pltpu.SMEM)
VMEM = pl.BlockSpec(memory_space=pltpu.VMEM)
HBM = pl.BlockSpec(memory_space=pltpu.HBM)


def call(kernel, ins, outs, args, scratch=(), out_spec=VMEM, limit=28_000_000):
    shapes = [o if isinstance(o, jax.ShapeDtypeStruct) else jax.ShapeDtypeStruct(o, jnp.float32) for o in outs]
    many = len(shapes) > 1
    return pl.pallas_call(
        kernel,
        out_shape=shapes if many else shapes[0],
        in_specs=ins,
        out_specs=[out_spec] * len(outs) if many else out_spec,
        scratch_shapes=scratch,
        compiler_params=pltpu.CompilerParams(vmem_limit_bytes=limit),
    )(*args)


def to_partner(value, pair_bits, then=lambda come: come, *others):
    group_count = lax.axis_size("grp")

    def by_mask(mask):
        pairs = [(source, source ^ mask) for source in range(group_count)]
        return lambda given: then(lax.ppermute(given[0], "grp", pairs), *given[1:])

    branches = [by_mask(mask) for mask in range(1, group_count)]
    return lax.switch(pair_bits - 1, branches, (value, *others))


def to_rows(planes):
    return planes.reshape(2, XS, 72, 128).transpose(1, 2, 0, 3).reshape(864, 128)


def from_rows(rows):
    return rows.reshape(XS, 72, 2, 128).transpose(2, 0, 1, 3).reshape(2, XS, G * G)


def exchange(chunks):
    chunks = chunks.reshape(SLABS, ROWS, 128)
    moved = lax.all_to_all(chunks, "slab", split_axis=0, concat_axis=0, tiled=True)
    return moved.reshape(SLABS * ROWS, 128)


def fold_table():
    table = np.zeros((200, N), np.float32)
    for k in range(1, G):
        table[k, k] = table[k, N - k] = 1.0
        table[G + k, k], table[G + k, N - k] = 1.0, -1.0
    table[0, 0] = table[N, G] = 1.0
    return table


def local(orbitals, occupation, kernel_hat, pair_mask):
    tz, lines_table, tv = [jnp.asarray(t) for t in tables()]
    pair_bits = pair_mask[0]
    own_group = lax.axis_index("grp")
    upper = (own_group > jnp.bitwise_xor(own_group, pair_bits)).astype(jnp.int32).reshape(1)
    own = to_rows(orbitals)
    chunk = (SLABS * ROWS, 128)
    rows = pltpu.VMEM((864, 128), jnp.float32)

    def spread_out(theirs, own, upper, tz):
        near = [jax.ShapeDtypeStruct(a.shape, a.dtype) for a in (own, tz)]
        own, tz = call(near_kernel, [HBM] * 2, near, (own, tz), [pltpu.SemaphoreType.DMA((2,))])
        scratch = [pltpu.VMEM(chunk, jnp.float32), pltpu.SemaphoreType.DMA((2 * SLABS,))]
        scratch.append(pltpu.SemaphoreType.DMA)
        operands = (upper, own, theirs, tz)
        outs = [(864, 128), chunk]
        return call(spread_kernel, [SMEM] + [VMEM] * 3, outs, operands, scratch, HBM)

    theirs, spread = to_partner(own, pair_bits, spread_out, own, upper, tz)
    hat = jnp.einsum(
        "rx,qnx->qrn",
        jnp.asarray(fold_table()),
        kernel_hat.reshape(3, 4 * N, N),
        precision=lax.Precision.HIGHEST,
    )
    scratch = [pltpu.VMEM((3, 2, G, 4 * N), jnp.float32)] * 2
    scratch += [pltpu.VMEM((3, 200, 4 * N), jnp.float32)]
    scratch += [pltpu.VMEM(lines_table.shape, lines_table.dtype), pltpu.SemaphoreType.DMA((4,))]
    lined = call(
        line_kernel,
        [VMEM, HBM, HBM],
        [chunk],
        (exchange(spread), hat, lines_table),
        scratch,
        limit=53_300_000,
    )
    back = exchange(lined)
    kept, sent = call(
        term_kernel,
        [SMEM, SMEM, VMEM, VMEM, HBM, VMEM],
        [(864, 128), (872, 128)],
        (upper, occupation, back, own, theirs, tv),
        [rows, pltpu.VMEM((2, XS, 24, 384), jnp.float32), pltpu.SemaphoreType.DMA],
    )

    come = to_partner(sent, pair_bits)
    scratch = [pltpu.VMEM((872, 128), jnp.float32), rows, pltpu.SemaphoreType.DMA((9,))]
    total = call(sum_kernel, [SMEM, VMEM, HBM], [(864, 128)], (upper, kept, come), scratch, HBM)
    return from_rows(total)


def solution(mesh):
    return jax.shard_map(
        local,
        mesh=mesh,
        in_specs=(P("grp", "slab", None), P("grp"), P("slab", None), P()),
        out_specs=P("grp", "slab", None),
        check_vma=False,
    )
```

```python
import functools
import math

import jax
import jax.numpy as jnp
import numpy as np
from jax import lax
from jax.experimental import pallas as pl
from jax.experimental.pallas import tpu as pltpu
from jax.sharding import PartitionSpec as P

G = 96
N = 192
SLABS = 16
XS = 6
KP = 6
ROWS = 112

Y_ORDER = np.array([4 * (i % 24) + i // 24 for i in range(G)])
X_ORDER = np.array([6 * (i % SLABS) + i // SLABS for i in range(G)])


WY, WI, TX, TI, LINES = 0, 640, 1280, 1472, 1664


def split(table):
    table = jnp.asarray(table, jnp.float32)
    high = table.astype(jnp.bfloat16)
    low = (table - high.astype(jnp.float32)).astype(jnp.bfloat16)
    return high, low


def np_split(table):
    bf16 = jnp.bfloat16
    high = table.astype(np.float32).astype(bf16)
    low = (table - high.astype(np.float64)).astype(np.float32).astype(bf16)
    return np.stack([high, low])


def waves(freq, cell):
    angle = (np.outer(freq, cell) % N) * (2.0 * math.pi / N)
    return np.cos(angle), np.sin(angle)


@functools.cache
def tables():
    pair_major = np.array([[12 * d + 2 * kp for d in range(SLABS)] for kp in range(KP)]).reshape(-1)
    tz = np.zeros((384, 256))
    tv = np.zeros((256, 384))
    wy = np.zeros((640, 256))
    wi = np.zeros((640, 256))
    for kz2 in range(2):
        cos, sin = waves(pair_major + kz2, np.arange(G))
        re, im = 192 * kz2, 192 * kz2 + 96
        tz[re : re + 96, 0:96], tz[re : re + 96, 128:224] = cos, sin
        tz[im : im + 96, 0:96], tz[im : im + 96, 128:224] = -sin, cos
        tv[0:96, re : re + 96], tv[0:96, im : im + 96] = cos.T / N, -sin.T / N
        tv[128:224, re : re + 96], tv[128:224, im : im + 96] = sin.T / N, cos.T / N
    cos, sin = waves(Y_ORDER, np.arange(N))
    wy[64:160, :N], wy[160:256, :N] = cos, sin
    wy[384:480, :N], wy[480:576, :N] = -sin, cos
    wi[64:256, 0:96], wi[64:256, 96:192] = cos.T / N, sin.T / N
    wi[384:576, 0:96], wi[384:576, 96:192] = -sin.T / N, cos.T / N
    cos, sin = waves(np.arange(G), X_ORDER)
    sin[0] = waves(np.array([G]), X_ORDER)[0][0]
    tx = np.concatenate([cos, sin], axis=0)
    ti = np.block([[cos.T, -sin.T], [cos.T, sin.T]]) / N
    lines = [wy, wi, widened(tx), widened(ti)]
    return [np_split(t) for t in (tz, np.concatenate(lines, axis=0), tv)]


def widened(table):
    return np.pad(table, ((0, 0), (0, 256 - table.shape[1])))


def mm(left, right, form=(1, 0)):
    def one(a, b):
        return lax.dot_general(
            a, b, (((form[0],), (form[1],)), ((), ())), preferred_element_type=jnp.float32
        )

    return one(left[0], right[0]) + (one(left[0], right[1]) + one(left[1], right[0]))


def plane(ref, x, orbital):
    base = 144 * x + orbital
    tiles = [ref[pl.ds(base + 2 * tile, 24, stride=6), :] for tile in range(3)]
    return jnp.concatenate(tiles, axis=1)


def lines(dense):
    return jnp.concatenate([dense[:, 96 * q : 96 * q + 96] for q in range(4)], axis=0)


def dense_of(rows):
    return jnp.concatenate([rows[24 * q : 24 * q + 24] for q in range(4)], axis=1)


def is_upper(mask):
    return jnp.bitwise_and(lax.axis_index("grp"), 1 << (mask.bit_length() - 1)) != 0


def near_kernel(occupation_ref, own_hbm, tz_hbm, own_ref, tz_ref, facts_ref, sems, *, mask):
    row = lax.broadcasted_iota(jnp.int32, (8, 128), 0)
    weight = [0.25 * occupation_ref[o].astype(jnp.float32) for o in range(2)]
    upper = jnp.where(is_upper(mask), 1.0, 0.0)
    facts_ref[...] = jnp.where(row == 0, weight[0], jnp.where(row == 1, weight[1], upper))
    copies = [
        pltpu.make_async_copy(own_hbm, own_ref, sems.at[0]),
        pltpu.make_async_copy(tz_hbm, tz_ref, sems.at[1]),
    ]
    for copy in copies:
        copy.start()
    for copy in copies:
        copy.wait()


def spread_kernel(
    own_ref, their_ref, tz_ref, their_hbm, out_hbm, out_ref, sems, their_sem, *, mask
):
    kept = pltpu.make_async_copy(their_ref, their_hbm, their_sem)
    kept.start()
    upper = is_upper(mask)
    pad = jnp.zeros((G, 32), jnp.float32)
    outs = []
    for x in range(XS):
        theirs = [plane(their_ref, x, o) for o in range(2)]
        first = jnp.where(upper, theirs[1], theirs[0])
        second = jnp.where(upper, theirs[0], theirs[1])
        one = lines(plane(own_ref, x, 0) * first)
        two = lines(plane(own_ref, x, 1) * second)
        density = jnp.concatenate([one, pad, two, pad], axis=1)
        lined = mm((tz_ref[0], tz_ref[1]), split(density), (1, 1))
        wide = jnp.concatenate([lined[96 * j : 96 * j + 96] for j in range(4)], axis=1)
        for kp in range(KP):
            for tile in range(3):
                out_ref[pl.ds(18 * x + 6 * tile + kp, SLABS, stride=ROWS), :] = wide[
                    16 * kp : 16 * kp + 16, 128 * tile : 128 * tile + 128
                ]
        if x in (3, 5):
            first_row, count = (0, 72) if x == 3 else (72, 40)
            if x == 5:
                for slab in range(SLABS):
                    out_ref[ROWS * slab + 108 : ROWS * slab + 112, :] = jnp.zeros((4, 128), jnp.float32)
            for slab in range(SLABS):
                place = pl.ds(ROWS * slab + first_row, count)
                outs.append(
                    pltpu.make_async_copy(out_ref.at[place], out_hbm.at[place], sems.at[len(outs)])
                )
                outs[-1].start()
    for copy in outs:
        copy.wait()
    kept.wait()


def side_by_side(left, right):
    right = pltpu.roll(right, 64, 1)
    return jnp.concatenate(
        [left[:, :128], left[:, 128:] + right[:, :128], right[:, 128:]], axis=1
    )


def line_kernel(in_ref, hat_hbm, table_hbm, out_ref, y_ref, u_ref, hat_ref, table_ref, sems):
    fetches = []
    for row, count in ((WY, WI - WY), (TX, LINES - TX), (WI, TX - WI)):
        place = (slice(None), pl.ds(row, count))
        pair = (table_hbm.at[place], table_ref.at[place])
        fetches.append(pltpu.make_async_copy(*pair, sems.at[len(fetches)]))
    fetches.insert(2, pltpu.make_async_copy(hat_hbm, hat_ref, sems.at[3]))
    for copy in fetches:
        copy.start()
    def table(row, count, columns=256):
        return [table_ref[part, row : row + count, :columns] for part in range(2)]

    pieces = []
    for kp in range(KP):
        for x in range(XS):
            pieces.append(
                jnp.concatenate(
                    [
                        in_ref[pl.ds(18 * x + 6 * tile + kp, SLABS, stride=ROWS), :]
                        for tile in range(3)
                    ],
                    axis=1,
                )
            )
    data = split(jnp.concatenate(pieces, axis=0))
    fetches[0].wait()
    for c in range(2):
        result = []
        for kz2 in range(2):
            window = [part[:, 128 * kz2 : 128 * kz2 + 256] for part in data]
            result.append(mm(window, table(WY + 320 * c + 64 * (1 - kz2), 256)))
        paired = side_by_side(*result)
        for kp in range(KP):
            lanes = slice(384 * (kp % 2), 384 * (kp % 2) + 384)
            y_ref[kp // 2, c, :, lanes] = paired[96 * kp : 96 * kp + 96]
    fetches[1].wait()
    fetches[2].wait()
    first_row = lax.broadcasted_iota(jnp.int32, (G, 768), 0) == 0
    for q in range(3):
        forward = table(TX, N, G)
        re = mm(forward, split(y_ref[q, 0]))
        im = mm(forward, split(y_ref[q, 1]))
        even, odd = hat_ref[q, :G], hat_ref[q, G:N]
        even_sin = jnp.where(first_row, hat_ref[q, N : N + 1], even)
        cos_re = even * re[:G] + odd * im[G:]
        sin_im = odd * im[:G] - even_sin * re[G:]
        cos_im = even * im[:G] - odd * re[G:]
        sin_re = odd * re[:G] + even_sin * im[G:]
        u_ref[q, 0] = mm(table(TI, G, N), split(jnp.concatenate([cos_re, sin_im], axis=0)))
        u_ref[q, 1] = mm(table(TI + G, G, N), split(jnp.concatenate([cos_im, sin_re], axis=0)))
    fetches[3].wait()
    sides = []
    for kz2 in range(2):
        parts = []
        for c in range(2):
            rows = []
            for kp in range(KP):
                lane = 384 * (kp % 2) + 128 * kz2
                rows.append(u_ref[kp // 2, c, :, lane : lane + 256])
            back = split(jnp.concatenate(rows, axis=0))
            parts.append(mm(back, table(WI + 320 * c + 64 * (1 - kz2), 256)))
        sides.append(parts[0] + parts[1])
    wide = side_by_side(*sides)
    for kp in range(KP):
        for x in range(XS):
            for tile in range(3):
                row = 96 * kp + 16 * x
                out_ref[pl.ds(18 * x + 6 * tile + kp, SLABS, stride=ROWS), :] = wide[
                    row : row + 16, 128 * tile : 128 * tile + 128
                ]


def term_kernel(
    in_ref, own_ref, their_hbm, facts_ref, tv_ref, kept_ref, sent_ref, their_ref,
    field_ref, sem
):
    fetch = pltpu.make_async_copy(their_hbm, their_ref, sem)
    fetch.start()
    upper = facts_ref[2:3, :1] > 0.5
    table = (tv_ref[0], tv_ref[1])
    weight = [facts_ref[o : o + 1, :1] for o in range(2)]
    for x in range(XS):
        pieces = [
            jnp.concatenate(
                [
                    in_ref[pl.ds(18 * x + 6 * tile + kp, SLABS, stride=ROWS), :]
                    for tile in range(3)
                ],
                axis=1,
            )
            for kp in range(KP)
        ]
        wide = jnp.concatenate(pieces, axis=0)
        stacked = jnp.concatenate([wide[:, 96 * j : 96 * j + 96] for j in range(4)], axis=0)
        fields = mm(table, split(stacked)).T
        field_ref[0, x] = dense_of(fields[:, :96])
        field_ref[1, x] = dense_of(fields[:, 128:224])
    fetch.wait()
    for x in range(XS):
        one, two = field_ref[0, x], field_ref[1, x]
        theirs = [plane(their_ref, x, o) for o in range(2)]
        first = jnp.where(upper, theirs[1], theirs[0])
        second = jnp.where(upper, theirs[0], theirs[1])
        kept = [one * first, two * second]
        mine_one = one * plane(own_ref, x, 0) * weight[0]
        mine_two = two * plane(own_ref, x, 1) * weight[1]
        sent = [jnp.where(upper, mine_two, mine_one), jnp.where(upper, mine_one, mine_two)]
        for o in range(2):
            for tile in range(3):
                place = pl.ds(144 * x + o + 2 * tile, 24, stride=6)
                kept_ref[place, :] = kept[o][:, 128 * tile : 128 * tile + 128]
                sent_ref[place, :] = sent[o][:, 128 * tile : 128 * tile + 128]
    sent_ref[864:872, :] = facts_ref[...]


def sum_kernel(kept_ref, come_ref, out_hbm, out_ref, sems, *, mask):
    upper = is_upper(mask)
    odd_row = lax.broadcasted_iota(jnp.int32, (216, 128), 0) % 2 == 1
    even = jnp.where(upper, come_ref[865:866, :], come_ref[864:865, :])
    odd = jnp.where(upper, come_ref[864:865, :], come_ref[865:866, :])
    weight = jnp.where(odd_row, odd, even)
    outs = []
    for k in range(4):
        place = pl.ds(216 * k, 216)
        out_ref[place, :] = -(kept_ref[place, :] * weight + come_ref[place, :])
        outs.append(pltpu.make_async_copy(out_ref.at[place], out_hbm.at[place], sems.at[k]))
        outs[-1].start()
    for copy in outs:
        copy.wait()


def same_kernel(in_hbm, out_hbm):
    pass


SMEM = pl.BlockSpec(memory_space=pltpu.SMEM)
VMEM = pl.BlockSpec(memory_space=pltpu.VMEM)
HBM = pl.BlockSpec(memory_space=pltpu.HBM)


def call(kernel, ins, outs, args, scratch=(), out_spec=VMEM, limit=28_000_000, alias=None):
    shapes = [o if isinstance(o, jax.ShapeDtypeStruct) else jax.ShapeDtypeStruct(o, jnp.float32) for o in outs]
    many = len(shapes) > 1
    return pl.pallas_call(
        kernel,
        out_shape=shapes if many else shapes[0],
        in_specs=ins,
        out_specs=[out_spec] * len(outs) if many else out_spec,
        scratch_shapes=scratch,
        input_output_aliases=alias or {},
        compiler_params=pltpu.CompilerParams(vmem_limit_bytes=limit),
    )(*args)


def to_partner(value, pair_bits, then, *others):
    group_count = lax.axis_size("grp")

    def by_mask(mask):
        pairs = [(source, source ^ mask) for source in range(group_count)]
        return lambda given: then(mask, lax.ppermute(given[0], "grp", pairs), *given[1:])

    branches = [by_mask(mask) for mask in range(1, group_count)]
    return lax.switch(pair_bits - 1, branches, (value, *others))


def to_rows(planes):
    return planes.reshape(2, XS, 72, 128).transpose(1, 2, 0, 3).reshape(864, 128)


def from_rows(rows):
    return rows.reshape(XS, 72, 2, 128).transpose(2, 0, 1, 3).reshape(2, XS, G * G)


def exchange(chunks):
    chunks = chunks.reshape(SLABS, ROWS, 128)
    moved = lax.all_to_all(chunks, "slab", split_axis=0, concat_axis=0, tiled=True)
    return moved.reshape(SLABS * ROWS, 128)


def fold_table():
    table = np.zeros((200, N), np.float32)
    for k in range(1, G):
        table[k, k] = table[k, N - k] = 1.0
        table[G + k, k], table[G + k, N - k] = 1.0, -1.0
    table[0, 0] = table[N, G] = 1.0
    return table


def local(orbitals, occupation, kernel_hat, pair_mask):
    tz, lines_table, tv = [jnp.asarray(t) for t in tables()]
    pair_bits = pair_mask[0]
    own = to_rows(orbitals)
    chunk = (SLABS * ROWS, 128)
    rows = pltpu.VMEM((864, 128), jnp.float32)

    def spread_out(mask, theirs, own, occupation, tz):
        near = [jax.ShapeDtypeStruct(a.shape, a.dtype) for a in (own, tz)]
        own, tz, facts = call(
            functools.partial(near_kernel, mask=mask),
            [SMEM, HBM, HBM],
            near + [(8, 128)],
            (occupation, own, tz),
            [pltpu.SemaphoreType.DMA((2,))],
        )
        scratch = [pltpu.VMEM(chunk, jnp.float32), pltpu.SemaphoreType.DMA((2 * SLABS,))]
        scratch.append(pltpu.SemaphoreType.DMA)
        kernel = functools.partial(spread_kernel, mask=mask)
        outs = [(864, 128), chunk]
        return *call(kernel, [VMEM] * 3, outs, (own, theirs, tz), scratch, HBM), facts

    theirs, spread, facts = to_partner(own, pair_bits, spread_out, own, occupation, tz)
    hat = jnp.einsum(
        "rx,qnx->qrn",
        jnp.asarray(fold_table()),
        kernel_hat.reshape(3, 4 * N, N),
        precision=lax.Precision.HIGHEST,
    )
    scratch = [pltpu.VMEM((3, 2, G, 4 * N), jnp.float32)] * 2
    scratch += [pltpu.VMEM((3, 200, 4 * N), jnp.float32)]
    scratch += [pltpu.VMEM(lines_table.shape, lines_table.dtype), pltpu.SemaphoreType.DMA((4,))]
    lined = call(
        line_kernel,
        [VMEM, HBM, HBM],
        [chunk],
        (exchange(spread), hat, lines_table),
        scratch,
        limit=53_300_000,
    )
    back = exchange(lined)
    kept, sent = call(
        term_kernel,
        [VMEM, VMEM, HBM, VMEM, VMEM],
        [(864, 128), (872, 128)],
        (back, own, theirs, facts, tv),
        [rows, pltpu.VMEM((2, XS, 24, 384), jnp.float32), pltpu.SemaphoreType.DMA],
    )

    def total(mask, come, kept):
        kernel = functools.partial(sum_kernel, mask=mask)
        scratch = [rows, pltpu.SemaphoreType.DMA((4,))]
        return call(kernel, [VMEM] * 2, [(864, 128)], (kept, come), scratch, HBM)

    out = to_partner(sent, pair_bits, total, kept)
    return from_rows(
        call(same_kernel, [HBM], [(864, 128)], (out,), (), HBM, limit=66_800_000, alias={0: 0})
    )


def solution(mesh):
    return jax.shard_map(
        local,
        mesh=mesh,
        in_specs=(P("grp", "slab", None), P("grp"), P("slab", None), P()),
        out_specs=P("grp", "slab", None),
        check_vma=False,
    )
```

```python
import functools
import math

import jax
import jax.numpy as jnp
import numpy as np
from jax import lax
from jax.experimental import pallas as pl
from jax.experimental.pallas import tpu as pltpu
from jax.sharding import PartitionSpec as P

G = 96
N = 192
SLABS = 16
XS = 6
KP = 6
ROWS = 112

Y_ORDER = np.array([4 * (i % 24) + i // 24 for i in range(G)])
X_ORDER = np.array([6 * (i % SLABS) + i // SLABS for i in range(G)])


WY, WI, TX, TI, LINES = 0, 640, 1280, 1472, 1664


def split(table):
    table = jnp.asarray(table, jnp.float32)
    high = table.astype(jnp.bfloat16)
    low = (table - high.astype(jnp.float32)).astype(jnp.bfloat16)
    return high, low


def np_split(table):
    bf16 = jnp.bfloat16
    high = table.astype(np.float32).astype(bf16)
    low = (table - high.astype(np.float64)).astype(np.float32).astype(bf16)
    return np.stack([high, low])


def waves(freq, cell):
    angle = (np.outer(freq, cell) % N) * (2.0 * math.pi / N)
    return np.cos(angle), np.sin(angle)


@functools.cache
def tables():
    pair_major = np.array([[12 * d + 2 * kp for d in range(SLABS)] for kp in range(KP)]).reshape(-1)
    tz = np.zeros((384, 256))
    tv = np.zeros((256, 384))
    wy = np.zeros((640, 256))
    wi = np.zeros((640, 256))
    for kz2 in range(2):
        cos, sin = waves(pair_major + kz2, np.arange(G))
        re, im = 192 * kz2, 192 * kz2 + 96
        tz[re : re + 96, 0:96], tz[re : re + 96, 128:224] = cos, sin
        tz[im : im + 96, 0:96], tz[im : im + 96, 128:224] = -sin, cos
        tv[0:96, re : re + 96], tv[0:96, im : im + 96] = cos.T / N, -sin.T / N
        tv[128:224, re : re + 96], tv[128:224, im : im + 96] = sin.T / N, cos.T / N
    cos, sin = waves(Y_ORDER, np.arange(N))
    wy[64:160, :N], wy[160:256, :N] = cos, sin
    wy[384:480, :N], wy[480:576, :N] = -sin, cos
    wi[64:256, 0:96], wi[64:256, 96:192] = cos.T / N, sin.T / N
    wi[384:576, 0:96], wi[384:576, 96:192] = -sin.T / N, cos.T / N
    cos, sin = waves(np.arange(G), X_ORDER)
    sin[0] = waves(np.array([G]), X_ORDER)[0][0]
    tx = np.concatenate([cos, sin], axis=0)
    ti = np.block([[cos.T, -sin.T], [cos.T, sin.T]]) / N
    lines = [wy, wi, widened(tx), widened(ti)]
    return [np_split(t) for t in (tz, np.concatenate(lines, axis=0), tv)]


def widened(table):
    return np.pad(table, ((0, 0), (0, 256 - table.shape[1])))


def mm(left, right, form=(1, 0)):
    def one(a, b):
        return lax.dot_general(
            a, b, (((form[0],), (form[1],)), ((), ())), preferred_element_type=jnp.float32
        )

    return one(left[0], right[0]) + (one(left[0], right[1]) + one(left[1], right[0]))


def plane(ref, x, orbital):
    base = 144 * x + orbital
    tiles = [ref[pl.ds(base + 2 * tile, 24, stride=6), :] for tile in range(3)]
    return jnp.concatenate(tiles, axis=1)


def lines(dense):
    return jnp.concatenate([dense[:, 96 * q : 96 * q + 96] for q in range(4)], axis=0)


def dense_of(rows):
    return jnp.concatenate([rows[24 * q : 24 * q + 24] for q in range(4)], axis=1)


def is_upper(mask):
    return jnp.bitwise_and(lax.axis_index("grp"), 1 << (mask.bit_length() - 1)) != 0


def near_kernel(occupation_ref, own_hbm, tz_hbm, own_ref, tz_ref, facts_ref, sems, *, mask):
    row = lax.broadcasted_iota(jnp.int32, (8, 128), 0)
    weight = [0.25 * occupation_ref[o].astype(jnp.float32) for o in range(2)]
    upper = jnp.where(is_upper(mask), 1.0, 0.0)
    facts_ref[...] = jnp.where(row == 0, weight[0], jnp.where(row == 1, weight[1], upper))
    copies = [
        pltpu.make_async_copy(own_hbm, own_ref, sems.at[0]),
        pltpu.make_async_copy(tz_hbm, tz_ref, sems.at[1]),
    ]
    for copy in copies:
        copy.start()
    for copy in copies:
        copy.wait()


def spread_kernel(
    own_ref, their_ref, tz_ref, their_hbm, out_hbm, out_ref, sems, their_sem, *, mask
):
    kept = pltpu.make_async_copy(their_ref, their_hbm, their_sem)
    kept.start()
    upper = is_upper(mask)
    pad = jnp.zeros((G, 32), jnp.float32)
    outs = []
    for x in range(XS):
        theirs = [plane(their_ref, x, o) for o in range(2)]
        first = jnp.where(upper, theirs[1], theirs[0])
        second = jnp.where(upper, theirs[0], theirs[1])
        one = lines(plane(own_ref, x, 0) * first)
        two = lines(plane(own_ref, x, 1) * second)
        density = jnp.concatenate([one, pad, two, pad], axis=1)
        lined = mm((tz_ref[0], tz_ref[1]), split(density), (1, 1))
        wide = jnp.concatenate([lined[96 * j : 96 * j + 96] for j in range(4)], axis=1)
        for kp in range(KP):
            for tile in range(3):
                out_ref[pl.ds(18 * x + 6 * tile + kp, SLABS, stride=ROWS), :] = wide[
                    16 * kp : 16 * kp + 16, 128 * tile : 128 * tile + 128
                ]
        if x in (3, 5):
            first_row, count = (0, 72) if x == 3 else (72, 40)
            if x == 5:
                for slab in range(SLABS):
                    out_ref[ROWS * slab + 108 : ROWS * slab + 112, :] = jnp.zeros((4, 128), jnp.float32)
            for slab in range(SLABS):
                place = pl.ds(ROWS * slab + first_row, count)
                outs.append(
                    pltpu.make_async_copy(out_ref.at[place], out_hbm.at[place], sems.at[len(outs)])
                )
                outs[-1].start()
    for copy in outs:
        copy.wait()
    kept.wait()


def side_by_side(left, right):
    right = pltpu.roll(right, 64, 1)
    return jnp.concatenate(
        [left[:, :128], left[:, 128:] + right[:, :128], right[:, 128:]], axis=1
    )


def line_kernel(in_ref, hat_hbm, table_hbm, out_ref, y_ref, u_ref, hat_ref, table_ref, sems):
    fetches = []
    for row, count in ((WY, WI - WY), (TX, LINES - TX), (WI, TX - WI)):
        place = (slice(None), pl.ds(row, count))
        pair = (table_hbm.at[place], table_ref.at[place])
        fetches.append(pltpu.make_async_copy(*pair, sems.at[len(fetches)]))
    fetches.insert(2, pltpu.make_async_copy(hat_hbm, hat_ref, sems.at[3]))
    for copy in fetches:
        copy.start()
    def table(row, count, columns=256):
        return [table_ref[part, row : row + count, :columns] for part in range(2)]

    def gathered(kps):
        pieces = []
        for kp in kps:
            for x in range(XS):
                place = [pl.ds(18 * x + 6 * tile + kp, SLABS, stride=ROWS) for tile in range(3)]
                pieces.append(jnp.concatenate([in_ref[p, :] for p in place], axis=1))
        return split(jnp.concatenate(pieces, axis=0))

    def y_forward(q, data):
        for c in range(2):
            result = []
            for kz2 in range(2):
                window = [part[:, 128 * kz2 : 128 * kz2 + 256] for part in data]
                result.append(mm(window, table(WY + 320 * c + 64 * (1 - kz2), 256)))
            paired = side_by_side(*result)
            for half in range(2):
                y_ref[q, c, :, 384 * half : 384 * half + 384] = paired[96 * half : 96 * half + 96]

    data = gathered((0, 1))
    fetches[0].wait()
    for q in range(3):
        coming = gathered((2 * q + 2, 2 * q + 3)) if q < 2 else None
        y_forward(q, data)
        data = coming
    for copy in fetches[1:]:
        copy.wait()
    first_row = lax.broadcasted_iota(jnp.int32, (G, 256), 0) == 0
    forward = table(TX, N, G)

    def spectra(i):
        q, hl = places[i]
        return [mm(forward, split(y_ref[q, c, :, hl])) for c in range(2)]

    def multiplied(i, re, im):
        q, hl = places[i]
        even, odd = hat_ref[q, :G, hl], hat_ref[q, G:N, hl]
        even_sin = jnp.where(first_row, hat_ref[q, N : N + 1, hl], even)
        cos_re = even * re[:G] + odd * im[G:]
        sin_im = odd * im[:G] - even_sin * re[G:]
        cos_im = even * im[:G] - odd * re[G:]
        sin_re = odd * re[:G] + even_sin * im[G:]
        return (
            split(jnp.concatenate([cos_re, sin_im], axis=0)),
            split(jnp.concatenate([cos_im, sin_re], axis=0)),
        )

    def back(i, first, second):
        q, hl = places[i]
        u_ref[q, 0, :, hl] = mm(table(TI, G, N), first)
        u_ref[q, 1, :, hl] = mm(table(TI + G, G, N), second)
    def y_back(q):
        sides = []
        for kz2 in range(2):
            parts = []
            for c in range(2):
                lane = [384 * half + 128 * kz2 for half in range(2)]
                rows = [u_ref[q, c, :, first : first + 256] for first in lane]
                window = split(jnp.concatenate(rows, axis=0))
                parts.append(mm(window, table(WI + 320 * c + 64 * (1 - kz2), 256)))
            sides.append(parts[0] + parts[1])
        wide = side_by_side(*sides)
        for half in range(2):
            for x in range(XS):
                row = 96 * half + 16 * x
                for tile in range(3):
                    place = pl.ds(18 * x + 6 * tile + 2 * q + half, SLABS, stride=ROWS)
                    out_ref[place, :] = wide[row : row + 16, 128 * tile : 128 * tile + 128]

    places = [(q, slice(w, w + 256)) for q in range(3) for w in range(0, 768, 256)]
    ahead = [spectra(i) for i in range(2)]
    for i in range(len(places)):
        product = multiplied(i, *ahead.pop(0))
        if i + 2 < len(places):
            ahead.append(spectra(i + 2))
        back(i, *product)
    for q in range(3):
        y_back(q)


def term_kernel(
    in_ref, own_ref, their_hbm, facts_ref, tv_ref, kept_ref, sent_ref, their_ref,
    field_ref, sem
):
    fetch = pltpu.make_async_copy(their_hbm, their_ref, sem)
    fetch.start()
    upper = facts_ref[2:3, :1] > 0.5
    table = (tv_ref[0], tv_ref[1])
    weight = [facts_ref[o : o + 1, :1] for o in range(2)]
    for x in range(XS):
        pieces = [
            jnp.concatenate(
                [
                    in_ref[pl.ds(18 * x + 6 * tile + kp, SLABS, stride=ROWS), :]
                    for tile in range(3)
                ],
                axis=1,
            )
            for kp in range(KP)
        ]
        wide = jnp.concatenate(pieces, axis=0)
        stacked = jnp.concatenate([wide[:, 96 * j : 96 * j + 96] for j in range(4)], axis=0)
        fields = mm(table, split(stacked)).T
        field_ref[0, x] = dense_of(fields[:, :96])
        field_ref[1, x] = dense_of(fields[:, 128:224])
    fetch.wait()
    for x in range(XS):
        one, two = field_ref[0, x], field_ref[1, x]
        theirs = [plane(their_ref, x, o) for o in range(2)]
        first = jnp.where(upper, theirs[1], theirs[0])
        second = jnp.where(upper, theirs[0], theirs[1])
        kept = [one * first, two * second]
        mine_one = one * plane(own_ref, x, 0) * weight[0]
        mine_two = two * plane(own_ref, x, 1) * weight[1]
        sent = [jnp.where(upper, mine_two, mine_one), jnp.where(upper, mine_one, mine_two)]
        for o in range(2):
            for tile in range(3):
                place = pl.ds(144 * x + o + 2 * tile, 24, stride=6)
                kept_ref[place, :] = kept[o][:, 128 * tile : 128 * tile + 128]
                sent_ref[place, :] = sent[o][:, 128 * tile : 128 * tile + 128]
    sent_ref[864:872, :] = facts_ref[...]


def sum_kernel(kept_ref, come_ref, out_hbm, out_ref, sems, *, mask):
    upper = is_upper(mask)
    odd_row = lax.broadcasted_iota(jnp.int32, (216, 128), 0) % 2 == 1
    even = jnp.where(upper, come_ref[865:866, :], come_ref[864:865, :])
    odd = jnp.where(upper, come_ref[864:865, :], come_ref[865:866, :])
    weight = jnp.where(odd_row, odd, even)
    outs = []
    for k in range(4):
        place = pl.ds(216 * k, 216)
        out_ref[place, :] = -(kept_ref[place, :] * weight + come_ref[place, :])
        outs.append(pltpu.make_async_copy(out_ref.at[place], out_hbm.at[place], sems.at[k]))
        outs[-1].start()
    for copy in outs:
        copy.wait()


def same_kernel(in_hbm, out_hbm):
    pass


SMEM = pl.BlockSpec(memory_space=pltpu.SMEM)
VMEM = pl.BlockSpec(memory_space=pltpu.VMEM)
HBM = pl.BlockSpec(memory_space=pltpu.HBM)


def call(kernel, ins, outs, args, scratch=(), out_spec=VMEM, limit=28_000_000, alias=None):
    shapes = [o if isinstance(o, jax.ShapeDtypeStruct) else jax.ShapeDtypeStruct(o, jnp.float32) for o in outs]
    many = len(shapes) > 1
    return pl.pallas_call(
        kernel,
        out_shape=shapes if many else shapes[0],
        in_specs=ins,
        out_specs=[out_spec] * len(outs) if many else out_spec,
        scratch_shapes=scratch,
        input_output_aliases=alias or {},
        compiler_params=pltpu.CompilerParams(vmem_limit_bytes=limit),
    )(*args)


def to_partner(value, pair_bits, then, *others):
    group_count = lax.axis_size("grp")

    def by_mask(mask):
        pairs = [(source, source ^ mask) for source in range(group_count)]
        return lambda given: then(mask, lax.ppermute(given[0], "grp", pairs), *given[1:])

    branches = [by_mask(mask) for mask in range(1, group_count)]
    return lax.switch(pair_bits - 1, branches, (value, *others))


def to_rows(planes):
    return planes.reshape(2, XS, 72, 128).transpose(1, 2, 0, 3).reshape(864, 128)


def from_rows(rows):
    return rows.reshape(XS, 72, 2, 128).transpose(2, 0, 1, 3).reshape(2, XS, G * G)


def exchange(chunks):
    chunks = chunks.reshape(SLABS, ROWS, 128)
    moved = lax.all_to_all(chunks, "slab", split_axis=0, concat_axis=0, tiled=True)
    return moved.reshape(SLABS * ROWS, 128)


def fold_table():
    table = np.zeros((200, N), np.float32)
    for k in range(1, G):
        table[k, k] = table[k, N - k] = 1.0
        table[G + k, k], table[G + k, N - k] = 1.0, -1.0
    table[0, 0] = table[N, G] = 1.0
    return table


def local(orbitals, occupation, kernel_hat, pair_mask):
    tz, lines_table, tv = [jnp.asarray(t) for t in tables()]
    pair_bits = pair_mask[0]
    own = to_rows(orbitals)
    chunk = (SLABS * ROWS, 128)
    rows = pltpu.VMEM((864, 128), jnp.float32)

    def spread_out(mask, theirs, own, occupation, tz):
        near = [jax.ShapeDtypeStruct(a.shape, a.dtype) for a in (own, tz)]
        own, tz, facts = call(
            functools.partial(near_kernel, mask=mask),
            [SMEM, HBM, HBM],
            near + [(8, 128)],
            (occupation, own, tz),
            [pltpu.SemaphoreType.DMA((2,))],
        )
        scratch = [pltpu.VMEM(chunk, jnp.float32), pltpu.SemaphoreType.DMA((2 * SLABS,))]
        scratch.append(pltpu.SemaphoreType.DMA)
        kernel = functools.partial(spread_kernel, mask=mask)
        outs = [(864, 128), chunk]
        return *call(kernel, [VMEM] * 3, outs, (own, theirs, tz), scratch, HBM), facts

    theirs, spread, facts = to_partner(own, pair_bits, spread_out, own, occupation, tz)
    hat = jnp.einsum(
        "rx,qnx->qrn",
        jnp.asarray(fold_table()),
        kernel_hat.reshape(3, 4 * N, N),
        precision=lax.Precision.HIGHEST,
    )
    scratch = [pltpu.VMEM((3, 2, G, 4 * N), jnp.float32)] * 2
    scratch += [pltpu.VMEM((3, 200, 4 * N), jnp.float32)]
    scratch += [pltpu.VMEM(lines_table.shape, lines_table.dtype), pltpu.SemaphoreType.DMA((4,))]
    lined = call(
        line_kernel,
        [VMEM, HBM, HBM],
        [chunk],
        (exchange(spread), hat, lines_table),
        scratch,
        limit=53_300_000,
    )
    back = exchange(lined)
    kept, sent = call(
        term_kernel,
        [VMEM, VMEM, HBM, VMEM, VMEM],
        [(864, 128), (872, 128)],
        (back, own, theirs, facts, tv),
        [rows, pltpu.VMEM((2, XS, 24, 384), jnp.float32), pltpu.SemaphoreType.DMA],
    )

    def total(mask, come, kept):
        kernel = functools.partial(sum_kernel, mask=mask)
        scratch = [rows, pltpu.SemaphoreType.DMA((4,))]
        return call(kernel, [VMEM] * 2, [(864, 128)], (kept, come), scratch, HBM)

    out = to_partner(sent, pair_bits, total, kept)
    return from_rows(
        call(same_kernel, [HBM], [(864, 128)], (out,), (), HBM, limit=66_800_000, alias={0: 0})
    )


def solution(mesh):
    return jax.shard_map(
        local,
        mesh=mesh,
        in_specs=(P("grp", "slab", None), P("grp"), P("slab", None), P()),
        out_specs=P("grp", "slab", None),
        check_vma=False,
    )
```

```python
import functools
import math

import jax
import jax.numpy as jnp
import numpy as np
from jax import lax
from jax.experimental import pallas as pl
from jax.experimental.pallas import tpu as pltpu
from jax.sharding import PartitionSpec as P

G = 96
N = 192
SLABS = 16
XS = 6
KP = 6
ROWS = 112

Y_ORDER = np.array([4 * (i % 24) + i // 24 for i in range(G)])
X_ORDER = np.array([6 * (i % SLABS) + i // SLABS for i in range(G)])


WY, WI, TX, TI, LINES = 0, 640, 1280, 1472, 1664


def split(table):
    table = jnp.asarray(table, jnp.float32)
    high = table.astype(jnp.bfloat16)
    low = (table - high.astype(jnp.float32)).astype(jnp.bfloat16)
    return high, low


def np_split(table):
    bf16 = jnp.bfloat16
    high = table.astype(np.float32).astype(bf16)
    low = (table - high.astype(np.float64)).astype(np.float32).astype(bf16)
    return np.stack([high, low])


def waves(freq, cell):
    angle = (np.outer(freq, cell) % N) * (2.0 * math.pi / N)
    return np.cos(angle), np.sin(angle)


@functools.cache
def tables():
    pair_major = np.array([[12 * d + 2 * kp for d in range(SLABS)] for kp in range(KP)]).reshape(-1)
    tz = np.zeros((384, 256))
    tv = np.zeros((256, 384))
    wy = np.zeros((640, 256))
    wi = np.zeros((640, 256))
    for kz2 in range(2):
        cos, sin = waves(pair_major + kz2, np.arange(G))
        re, im = 192 * kz2, 192 * kz2 + 96
        tz[re : re + 96, 0:96], tz[re : re + 96, 128:224] = cos, sin
        tz[im : im + 96, 0:96], tz[im : im + 96, 128:224] = -sin, cos
        tv[0:96, re : re + 96], tv[0:96, im : im + 96] = cos.T / N, -sin.T / N
        tv[128:224, re : re + 96], tv[128:224, im : im + 96] = sin.T / N, cos.T / N
    cos, sin = waves(Y_ORDER, np.arange(N))
    wy[64:160, :N], wy[160:256, :N] = cos, sin
    wy[384:480, :N], wy[480:576, :N] = -sin, cos
    wi[64:256, 0:96], wi[64:256, 96:192] = cos.T / N, sin.T / N
    wi[384:576, 0:96], wi[384:576, 96:192] = -sin.T / N, cos.T / N
    cos, sin = waves(np.arange(G), X_ORDER)
    sin[0] = waves(np.array([G]), X_ORDER)[0][0]
    tx = np.concatenate([cos, sin], axis=0)
    ti = np.block([[cos.T, -sin.T], [cos.T, sin.T]]) / N
    lines = [wy, wi, widened(tx), widened(ti)]
    return [np_split(t) for t in (tz, np.concatenate(lines, axis=0), tv)]


def widened(table):
    return np.pad(table, ((0, 0), (0, 256 - table.shape[1])))


def mm(left, right, form=(1, 0)):
    def one(a, b):
        return lax.dot_general(
            a, b, (((form[0],), (form[1],)), ((), ())), preferred_element_type=jnp.float32
        )

    return one(left[0], right[0]) + (one(left[0], right[1]) + one(left[1], right[0]))


def plane(ref, x, orbital):
    base = 144 * x + orbital
    tiles = [ref[pl.ds(base + 2 * tile, 24, stride=6), :] for tile in range(3)]
    return jnp.concatenate(tiles, axis=1)


def lines(dense):
    return jnp.concatenate([dense[:, 96 * q : 96 * q + 96] for q in range(4)], axis=0)


def dense_of(rows):
    return jnp.concatenate([rows[24 * q : 24 * q + 24] for q in range(4)], axis=1)


def is_upper(mask):
    return jnp.bitwise_and(lax.axis_index("grp"), 1 << (mask.bit_length() - 1)) != 0


def near_kernel(occupation_ref, own_hbm, tz_hbm, own_ref, tz_ref, facts_ref, sems, *, mask):
    row = lax.broadcasted_iota(jnp.int32, (8, 128), 0)
    weight = [0.25 * occupation_ref[o].astype(jnp.float32) for o in range(2)]
    upper = jnp.where(is_upper(mask), 1.0, 0.0)
    facts_ref[...] = jnp.where(row == 0, weight[0], jnp.where(row == 1, weight[1], upper))
    copies = [
        pltpu.make_async_copy(own_hbm, own_ref, sems.at[0]),
        pltpu.make_async_copy(tz_hbm, tz_ref, sems.at[1]),
    ]
    for copy in copies:
        copy.start()
    for copy in copies:
        copy.wait()


def spread_kernel(
    own_ref, their_ref, tz_ref, their_hbm, out_hbm, out_ref, sems, their_sem, *, mask
):
    kept = pltpu.make_async_copy(their_ref, their_hbm, their_sem)
    kept.start()
    upper = is_upper(mask)
    pad = jnp.zeros((G, 32), jnp.float32)
    outs = []

    def density(x):
        theirs = [plane(their_ref, x, o) for o in range(2)]
        first = jnp.where(upper, theirs[1], theirs[0])
        second = jnp.where(upper, theirs[0], theirs[1])
        one = lines(plane(own_ref, x, 0) * first)
        two = lines(plane(own_ref, x, 1) * second)
        return split(jnp.concatenate([one, pad, two, pad], axis=1))

    def spectra(x):
        parts = [density(x), density(x + 1)]
        both = [jnp.concatenate([part[k] for part in parts], axis=0) for k in range(2)]
        return mm((tz_ref[0], tz_ref[1]), both, (1, 1))

    def stored(x, lined):
        wide = jnp.concatenate([lined[96 * j : 96 * j + 96] for j in range(4)], axis=1)
        for kp in range(KP):
            for tile in range(3):
                out_ref[pl.ds(18 * x + 6 * tile + kp, SLABS, stride=ROWS), :] = wide[
                    16 * kp : 16 * kp + 16, 128 * tile : 128 * tile + 128
                ]

    for slab in range(SLABS):
        out_ref[ROWS * slab + 108 : ROWS * slab + 112, :] = jnp.zeros((4, 128), jnp.float32)
    for x in range(0, XS, 2):
        lined = spectra(x)
        stored(x, lined[:, :96])
        stored(x + 1, lined[:, 96:192])
        if x in (2, 4):
            first_row, count = (0, 72) if x == 2 else (72, 40)
            for slab in range(SLABS):
                place = pl.ds(ROWS * slab + first_row, count)
                outs.append(
                    pltpu.make_async_copy(out_ref.at[place], out_hbm.at[place], sems.at[len(outs)])
                )
                outs[-1].start()
    for copy in outs:
        copy.wait()
    kept.wait()


def side_by_side(left, right):
    right = pltpu.roll(right, 64, 1)
    return jnp.concatenate(
        [left[:, :128], left[:, 128:] + right[:, :128], right[:, 128:]], axis=1
    )


def line_kernel(in_ref, hat_hbm, table_hbm, out_ref, y_ref, u_ref, hat_ref, table_ref, sems):
    fetches = []
    for row, count in ((WY, WI - WY), (TX, LINES - TX), (WI, TX - WI)):
        place = (slice(None), pl.ds(row, count))
        pair = (table_hbm.at[place], table_ref.at[place])
        fetches.append(pltpu.make_async_copy(*pair, sems.at[len(fetches)]))
    fetches.insert(2, pltpu.make_async_copy(hat_hbm, hat_ref, sems.at[3]))
    for copy in fetches:
        copy.start()

    def table(row, count, columns=256):
        return [table_ref[part, row : row + count, :columns] for part in range(2)]

    def gathered(kps):
        pieces = []
        for kp in kps:
            for x in range(XS):
                place = [pl.ds(18 * x + 6 * tile + kp, SLABS, stride=ROWS) for tile in range(3)]
                pieces.append(jnp.concatenate([in_ref[p, :] for p in place], axis=1))
        return split(jnp.concatenate(pieces, axis=0))

    def y_forward(q, data):
        for c in range(2):
            result = []
            for kz2 in range(2):
                window = [part[:, 128 * kz2 : 128 * kz2 + 256] for part in data]
                result.append(mm(window, table(WY + 320 * c + 64 * (1 - kz2), 256)))
            paired = side_by_side(*result)
            for half in range(2):
                y_ref[q, c, :, 384 * half : 384 * half + 384] = paired[96 * half : 96 * half + 96]

    data = gathered((0, 1))
    fetches[0].wait()
    for q in range(3):
        coming = gathered((2 * q + 2, 2 * q + 3)) if q < 2 else None
        y_forward(q, data)
        data = coming
    for copy in fetches[1:]:
        copy.wait()
    first_row = lax.broadcasted_iota(jnp.int32, (G, 256), 0) == 0
    forward = table(TX, N, G)

    def spectra(i):
        q, hl = places[i]
        return [mm(forward, split(y_ref[q, c, :, hl])) for c in range(2)]

    def multiplied(i, re, im):
        q, hl = places[i]
        even, odd = hat_ref[q, :G, hl], hat_ref[q, G:N, hl]
        even_sin = jnp.where(first_row, hat_ref[q, N : N + 1, hl], even)
        cos_re = even * re[:G] + odd * im[G:]
        sin_im = odd * im[:G] - even_sin * re[G:]
        cos_im = even * im[:G] - odd * re[G:]
        sin_re = odd * re[:G] + even_sin * im[G:]
        return (
            split(jnp.concatenate([cos_re, sin_im], axis=0)),
            split(jnp.concatenate([cos_im, sin_re], axis=0)),
        )

    def back(i, first, second):
        q, hl = places[i]
        u_ref[q, 0, :, hl] = mm(table(TI, G, N), first)
        u_ref[q, 1, :, hl] = mm(table(TI + G, G, N), second)

    def y_back(q):
        sides = []
        for kz2 in range(2):
            parts = []
            for c in range(2):
                lane = [384 * half + 128 * kz2 for half in range(2)]
                rows = [u_ref[q, c, :, first : first + 256] for first in lane]
                window = split(jnp.concatenate(rows, axis=0))
                parts.append(mm(window, table(WI + 320 * c + 64 * (1 - kz2), 256)))
            sides.append(parts[0] + parts[1])
        wide = side_by_side(*sides)
        for half in range(2):
            for x in range(XS):
                row = 96 * half + 16 * x
                for tile in range(3):
                    place = pl.ds(18 * x + 6 * tile + 2 * q + half, SLABS, stride=ROWS)
                    out_ref[place, :] = wide[row : row + 16, 128 * tile : 128 * tile + 128]

    places = [(q, slice(w, w + 256)) for q in range(3) for w in range(0, 768, 256)]
    ahead = [spectra(i) for i in range(2)]
    for i in range(len(places)):
        product = multiplied(i, *ahead.pop(0))
        if i + 2 < len(places):
            ahead.append(spectra(i + 2))
        back(i, *product)
    for q in range(3):
        y_back(q)


def term_kernel(
    in_ref, own_ref, their_hbm, facts_ref, tv_ref, kept_ref, sent_ref, their_ref,
    field_ref, sem
):
    fetch = pltpu.make_async_copy(their_hbm, their_ref, sem)
    fetch.start()
    upper = facts_ref[2:3, :1] > 0.5
    table = (tv_ref[0], tv_ref[1])
    weight = [facts_ref[o : o + 1, :1] for o in range(2)]

    def gathered(x):
        pieces = [
            jnp.concatenate(
                [
                    in_ref[pl.ds(18 * x + 6 * tile + kp, SLABS, stride=ROWS), :]
                    for tile in range(3)
                ],
                axis=1,
            )
            for kp in range(KP)
        ]
        return jnp.concatenate(pieces, axis=0)

    def spectrum(x):
        pair = (gathered(x), gathered(x + 1))
        lanes = [slice(96 * j, 96 * j + 96) for j in range(4)]
        both = [jnp.concatenate([wide[:, part] for wide in pair], axis=1) for part in lanes]
        return split(jnp.concatenate(both, axis=0))

    for x in range(0, XS, 2):
        fields = mm(table, spectrum(x)).T
        for k in range(2):
            rows = fields[96 * k : 96 * k + 96]
            field_ref[0, x + k] = dense_of(rows[:, :96])
            field_ref[1, x + k] = dense_of(rows[:, 128:224])
    fetch.wait()
    for x in range(XS):
        one, two = field_ref[0, x], field_ref[1, x]
        theirs = [plane(their_ref, x, o) for o in range(2)]
        first = jnp.where(upper, theirs[1], theirs[0])
        second = jnp.where(upper, theirs[0], theirs[1])
        kept = [one * first, two * second]
        mine_one = one * plane(own_ref, x, 0) * weight[0]
        mine_two = two * plane(own_ref, x, 1) * weight[1]
        sent = [jnp.where(upper, mine_two, mine_one), jnp.where(upper, mine_one, mine_two)]
        for o in range(2):
            for tile in range(3):
                place = pl.ds(144 * x + o + 2 * tile, 24, stride=6)
                kept_ref[place, :] = kept[o][:, 128 * tile : 128 * tile + 128]
                sent_ref[place, :] = sent[o][:, 128 * tile : 128 * tile + 128]
    sent_ref[864:872, :] = facts_ref[...]


def sum_kernel(kept_ref, come_ref, out_hbm, out_ref, sems, *, mask):
    upper = is_upper(mask)
    odd_row = lax.broadcasted_iota(jnp.int32, (216, 128), 0) % 2 == 1
    even = jnp.where(upper, come_ref[865:866, :], come_ref[864:865, :])
    odd = jnp.where(upper, come_ref[864:865, :], come_ref[865:866, :])
    weight = jnp.where(odd_row, odd, even)
    outs = []
    for k in range(4):
        place = pl.ds(216 * k, 216)
        out_ref[place, :] = -(kept_ref[place, :] * weight + come_ref[place, :])
        outs.append(pltpu.make_async_copy(out_ref.at[place], out_hbm.at[place], sems.at[k]))
        outs[-1].start()
    for copy in outs:
        copy.wait()


def same_kernel(in_hbm, out_hbm):
    pass


SMEM = pl.BlockSpec(memory_space=pltpu.SMEM)
VMEM = pl.BlockSpec(memory_space=pltpu.VMEM)
HBM = pl.BlockSpec(memory_space=pltpu.HBM)


def call(kernel, ins, outs, args, scratch=(), out_spec=VMEM, limit=28_000_000, alias=None):
    shapes = [o if isinstance(o, jax.ShapeDtypeStruct) else jax.ShapeDtypeStruct(o, jnp.float32) for o in outs]
    many = len(shapes) > 1
    return pl.pallas_call(
        kernel,
        out_shape=shapes if many else shapes[0],
        in_specs=ins,
        out_specs=[out_spec] * len(outs) if many else out_spec,
        scratch_shapes=scratch,
        input_output_aliases=alias or {},
        compiler_params=pltpu.CompilerParams(vmem_limit_bytes=limit),
    )(*args)


def to_partner(value, pair_bits, then, *others):
    group_count = lax.axis_size("grp")

    def by_mask(mask):
        pairs = [(source, source ^ mask) for source in range(group_count)]
        return lambda given: then(mask, lax.ppermute(given[0], "grp", pairs), *given[1:])

    branches = [by_mask(mask) for mask in range(1, group_count)]
    return lax.switch(pair_bits - 1, branches, (value, *others))


def to_rows(planes):
    return planes.reshape(2, XS, 72, 128).transpose(1, 2, 0, 3).reshape(864, 128)


def from_rows(rows):
    return rows.reshape(XS, 72, 2, 128).transpose(2, 0, 1, 3).reshape(2, XS, G * G)


def exchange(chunks):
    chunks = chunks.reshape(SLABS, ROWS, 128)
    moved = lax.all_to_all(chunks, "slab", split_axis=0, concat_axis=0, tiled=True)
    return moved.reshape(SLABS * ROWS, 128)


def fold_table():
    table = np.zeros((200, N), np.float32)
    for k in range(1, G):
        table[k, k] = table[k, N - k] = 1.0
        table[G + k, k], table[G + k, N - k] = 1.0, -1.0
    table[0, 0] = table[N, G] = 1.0
    return table


def local(orbitals, occupation, kernel_hat, pair_mask):
    tz, lines_table, tv = [jnp.asarray(t) for t in tables()]
    pair_bits = pair_mask[0]
    own = to_rows(orbitals)
    chunk = (SLABS * ROWS, 128)
    rows = pltpu.VMEM((864, 128), jnp.float32)

    def spread_out(mask, theirs, own, occupation, tz):
        near = [jax.ShapeDtypeStruct(a.shape, a.dtype) for a in (own, tz)]
        own, tz, facts = call(
            functools.partial(near_kernel, mask=mask),
            [SMEM, HBM, HBM],
            near + [(8, 128)],
            (occupation, own, tz),
            [pltpu.SemaphoreType.DMA((2,))],
        )
        scratch = [pltpu.VMEM(chunk, jnp.float32), pltpu.SemaphoreType.DMA((2 * SLABS,))]
        scratch.append(pltpu.SemaphoreType.DMA)
        kernel = functools.partial(spread_kernel, mask=mask)
        outs = [(864, 128), chunk]
        return *call(kernel, [VMEM] * 3, outs, (own, theirs, tz), scratch, HBM), facts

    theirs, spread, facts = to_partner(own, pair_bits, spread_out, own, occupation, tz)
    hat = jnp.einsum(
        "rx,qnx->qrn",
        jnp.asarray(fold_table()),
        kernel_hat.reshape(3, 4 * N, N),
        precision=lax.Precision.HIGHEST,
    )
    scratch = [pltpu.VMEM((3, 2, G, 4 * N), jnp.float32)] * 2
    scratch += [pltpu.VMEM((3, 200, 4 * N), jnp.float32)]
    scratch += [pltpu.VMEM(lines_table.shape, lines_table.dtype), pltpu.SemaphoreType.DMA((4,))]
    lined = call(
        line_kernel,
        [VMEM, HBM, HBM],
        [chunk],
        (exchange(spread), hat, lines_table),
        scratch,
        limit=53_300_000,
    )
    back = exchange(lined)
    kept, sent = call(
        term_kernel,
        [VMEM, VMEM, HBM, VMEM, VMEM],
        [(864, 128), (872, 128)],
        (back, own, theirs, facts, tv),
        [rows, pltpu.VMEM((2, XS, 24, 384), jnp.float32), pltpu.SemaphoreType.DMA],
    )

    def total(mask, come, kept):
        kernel = functools.partial(sum_kernel, mask=mask)
        scratch = [rows, pltpu.SemaphoreType.DMA((4,))]
        return call(kernel, [VMEM] * 2, [(864, 128)], (kept, come), scratch, HBM)

    out = to_partner(sent, pair_bits, total, kept)
    return from_rows(
        call(same_kernel, [HBM], [(864, 128)], (out,), (), HBM, limit=66_800_000, alias={0: 0})
    )


def solution(mesh):
    return jax.shard_map(
        local,
        mesh=mesh,
        in_specs=(P("grp", "slab", None), P("grp"), P("slab", None), P()),
        out_specs=P("grp", "slab", None),
        check_vma=False,
    )
```

```python
import functools
import math

import jax
import jax.numpy as jnp
import numpy as np
from jax import lax
from jax.experimental import pallas as pl
from jax.experimental.pallas import tpu as pltpu
from jax.sharding import PartitionSpec as P

G = 96
N = 192
SLABS = 16
XS = 6
KP = 6
ROWS = 112

Y_ORDER = np.array([4 * (i % 24) + i // 24 for i in range(G)])
X_ORDER = np.array([6 * (i % SLABS) + i // SLABS for i in range(G)])


WY, WI, TX, TI, LINES = 0, 640, 1280, 1472, 1664


def split(table):
    table = jnp.asarray(table, jnp.float32)
    high = table.astype(jnp.bfloat16)
    low = (table - high.astype(jnp.float32)).astype(jnp.bfloat16)
    return high, low


def np_split(table):
    bf16 = jnp.bfloat16
    high = table.astype(np.float32).astype(bf16)
    low = (table - high.astype(np.float64)).astype(np.float32).astype(bf16)
    return np.stack([high, low])


def waves(freq, cell):
    angle = (np.outer(freq, cell) % N) * (2.0 * math.pi / N)
    return np.cos(angle), np.sin(angle)


@functools.cache
def tables():
    pair_major = np.array([[12 * d + 2 * kp for d in range(SLABS)] for kp in range(KP)]).reshape(-1)
    tz = np.zeros((384, 256))
    tv = np.zeros((256, 384))
    wy = np.zeros((640, 256))
    wi = np.zeros((640, 256))
    for kz2 in range(2):
        cos, sin = waves(pair_major + kz2, np.arange(G))
        re, im = 192 * kz2, 192 * kz2 + 96
        tz[re : re + 96, 0:96], tz[re : re + 96, 128:224] = cos, sin
        tz[im : im + 96, 0:96], tz[im : im + 96, 128:224] = -sin, cos
        tv[0:96, re : re + 96], tv[0:96, im : im + 96] = cos.T / N, -sin.T / N
        tv[128:224, re : re + 96], tv[128:224, im : im + 96] = sin.T / N, cos.T / N
    cos, sin = waves(Y_ORDER, np.arange(N))
    wy[64:160, :N], wy[160:256, :N] = cos, sin
    wy[384:480, :N], wy[480:576, :N] = -sin, cos
    wi[64:256, 0:96], wi[64:256, 96:192] = cos.T / N, sin.T / N
    wi[384:576, 0:96], wi[384:576, 96:192] = -sin.T / N, cos.T / N
    cos, sin = waves(np.arange(G), X_ORDER)
    sin[0] = waves(np.array([G]), X_ORDER)[0][0]
    tx = np.concatenate([cos, sin], axis=0)
    ti = np.block([[cos.T, -sin.T], [cos.T, sin.T]]) / N
    lines = [wy, wi, widened(tx), widened(ti)]
    return [np_split(t) for t in (tz, np.concatenate(lines, axis=0), tv)]


def widened(table):
    return np.pad(table, ((0, 0), (0, 256 - table.shape[1])))


def mm(left, right, form=(1, 0)):
    def one(a, b):
        return lax.dot_general(
            a, b, (((form[0],), (form[1],)), ((), ())), preferred_element_type=jnp.float32
        )

    return one(left[0], right[0]) + (one(left[0], right[1]) + one(left[1], right[0]))


def plane(ref, x, orbital):
    base = 144 * x + orbital
    tiles = [ref[pl.ds(base + 2 * tile, 24, stride=6), :] for tile in range(3)]
    return jnp.concatenate(tiles, axis=1)


def lines(dense):
    return jnp.concatenate([dense[:, 96 * q : 96 * q + 96] for q in range(4)], axis=0)


def dense_of(rows):
    return jnp.concatenate([rows[24 * q : 24 * q + 24] for q in range(4)], axis=1)


def is_upper(mask):
    return jnp.bitwise_and(lax.axis_index("grp"), 1 << (mask.bit_length() - 1)) != 0


def near_kernel(occupation_ref, own_hbm, tz_hbm, own_ref, tz_ref, facts_ref, sems, *, mask):
    row = lax.broadcasted_iota(jnp.int32, (8, 128), 0)
    weight = [0.25 * occupation_ref[o].astype(jnp.float32) for o in range(2)]
    upper = jnp.where(is_upper(mask), 1.0, 0.0)
    facts_ref[...] = jnp.where(row == 0, weight[0], jnp.where(row == 1, weight[1], upper))
    copies = [
        pltpu.make_async_copy(own_hbm, own_ref, sems.at[0]),
        pltpu.make_async_copy(tz_hbm, tz_ref, sems.at[1]),
    ]
    for copy in copies:
        copy.start()
    for copy in copies:
        copy.wait()


def spread_kernel(
    own_ref, their_ref, tz_ref, their_hbm, out_ref, their_sem, *, mask
):
    kept = pltpu.make_async_copy(their_ref, their_hbm, their_sem)
    kept.start()
    upper = is_upper(mask)
    pad = jnp.zeros((G, 32), jnp.float32)

    def density(x):
        theirs = [plane(their_ref, x, o) for o in range(2)]
        first = jnp.where(upper, theirs[1], theirs[0])
        second = jnp.where(upper, theirs[0], theirs[1])
        one = lines(plane(own_ref, x, 0) * first)
        two = lines(plane(own_ref, x, 1) * second)
        return split(jnp.concatenate([one, pad, two, pad], axis=1))

    def spectra(x):
        parts = [density(x), density(x + 1)]
        both = [jnp.concatenate([part[k] for part in parts], axis=0) for k in range(2)]
        return mm((tz_ref[0], tz_ref[1]), both, (1, 1))

    def stored(x, lined):
        wide = jnp.concatenate([lined[96 * j : 96 * j + 96] for j in range(4)], axis=1)
        for kp in range(KP):
            for tile in range(3):
                out_ref[pl.ds(18 * x + 6 * tile + kp, SLABS, stride=ROWS), :] = wide[
                    16 * kp : 16 * kp + 16, 128 * tile : 128 * tile + 128
                ]

    for slab in range(SLABS):
        out_ref[ROWS * slab + 108 : ROWS * slab + 112, :] = jnp.zeros((4, 128), jnp.float32)
    for x in range(0, XS, 2):
        lined = spectra(x)
        stored(x, lined[:, :96])
        stored(x + 1, lined[:, 96:192])
    kept.wait()


def side_by_side(left, right):
    right = pltpu.roll(right, 64, 1)
    return jnp.concatenate(
        [left[:, :128], left[:, 128:] + right[:, :128], right[:, 128:]], axis=1
    )


def line_kernel(in_ref, hat_hbm, table_hbm, out_ref, y_ref, u_ref, hat_ref, table_ref, sems):
    fetches = []
    for row, count in ((WY, WI - WY), (TX, LINES - TX), (WI, TX - WI)):
        place = (slice(None), pl.ds(row, count))
        pair = (table_hbm.at[place], table_ref.at[place])
        fetches.append(pltpu.make_async_copy(*pair, sems.at[len(fetches)]))
    fetches.insert(2, pltpu.make_async_copy(hat_hbm, hat_ref, sems.at[3]))
    for copy in fetches:
        copy.start()

    def table(row, count, columns=256):
        return [table_ref[part, row : row + count, :columns] for part in range(2)]

    def gathered(kps):
        pieces = []
        for kp in kps:
            for x in range(XS):
                place = [pl.ds(18 * x + 6 * tile + kp, SLABS, stride=ROWS) for tile in range(3)]
                pieces.append(jnp.concatenate([in_ref[p, :] for p in place], axis=1))
        return split(jnp.concatenate(pieces, axis=0))

    def y_forward(q, data):
        for c in range(2):
            result = []
            for kz2 in range(2):
                window = [part[:, 128 * kz2 : 128 * kz2 + 256] for part in data]
                result.append(mm(window, table(WY + 320 * c + 64 * (1 - kz2), 256)))
            paired = side_by_side(*result)
            for half in range(2):
                y_ref[q, c, :, 384 * half : 384 * half + 384] = paired[96 * half : 96 * half + 96]

    data = gathered((0, 1))
    fetches[0].wait()
    for q in range(3):
        coming = gathered((2 * q + 2, 2 * q + 3)) if q < 2 else None
        y_forward(q, data)
        data = coming
    for copy in fetches[1:]:
        copy.wait()
    first_row = lax.broadcasted_iota(jnp.int32, (G, 256), 0) == 0
    forward = table(TX, N, G)

    def spectra(i):
        q, hl = places[i]
        return [mm(forward, split(y_ref[q, c, :, hl])) for c in range(2)]

    def multiplied(i, re, im):
        q, hl = places[i]
        even, odd = hat_ref[q, :G, hl], hat_ref[q, G:N, hl]
        even_sin = jnp.where(first_row, hat_ref[q, N : N + 1, hl], even)
        cos_re = even * re[:G] + odd * im[G:]
        sin_im = odd * im[:G] - even_sin * re[G:]
        cos_im = even * im[:G] - odd * re[G:]
        sin_re = odd * re[:G] + even_sin * im[G:]
        return (
            split(jnp.concatenate([cos_re, sin_im], axis=0)),
            split(jnp.concatenate([cos_im, sin_re], axis=0)),
        )

    def back(i, first, second):
        q, hl = places[i]
        u_ref[q, 0, :, hl] = mm(table(TI, G, N), first)
        u_ref[q, 1, :, hl] = mm(table(TI + G, G, N), second)

    def y_back(q):
        sides = []
        for kz2 in range(2):
            parts = []
            for c in range(2):
                lane = [384 * half + 128 * kz2 for half in range(2)]
                rows = [u_ref[q, c, :, first : first + 256] for first in lane]
                window = split(jnp.concatenate(rows, axis=0))
                parts.append(mm(window, table(WI + 320 * c + 64 * (1 - kz2), 256)))
            sides.append(parts[0] + parts[1])
        wide = side_by_side(*sides)
        for half in range(2):
            for x in range(XS):
                row = 96 * half + 16 * x
                for tile in range(3):
                    place = pl.ds(18 * x + 6 * tile + 2 * q + half, SLABS, stride=ROWS)
                    out_ref[place, :] = wide[row : row + 16, 128 * tile : 128 * tile + 128]

    places = [(q, slice(w, w + 256)) for q in range(3) for w in range(0, 768, 256)]
    ahead = [spectra(i) for i in range(2)]
    for i in range(len(places)):
        product = multiplied(i, *ahead.pop(0))
        if i + 2 < len(places):
            ahead.append(spectra(i + 2))
        back(i, *product)
    for q in range(3):
        y_back(q)


def term_kernel(
    in_ref, own_ref, their_hbm, facts_ref, tv_ref, kept_ref, sent_ref, their_ref,
    field_ref, sem
):
    fetch = pltpu.make_async_copy(their_hbm, their_ref, sem)
    fetch.start()
    upper = facts_ref[2:3, :1] > 0.5
    table = (tv_ref[0], tv_ref[1])
    weight = [facts_ref[o : o + 1, :1] for o in range(2)]

    def gathered(x):
        pieces = [
            jnp.concatenate(
                [
                    in_ref[pl.ds(18 * x + 6 * tile + kp, SLABS, stride=ROWS), :]
                    for tile in range(3)
                ],
                axis=1,
            )
            for kp in range(KP)
        ]
        return jnp.concatenate(pieces, axis=0)

    def spectrum(x):
        pair = (gathered(x), gathered(x + 1))
        lanes = [slice(96 * j, 96 * j + 96) for j in range(4)]
        both = [jnp.concatenate([wide[:, part] for wide in pair], axis=1) for part in lanes]
        return split(jnp.concatenate(both, axis=0))

    for x in range(0, XS, 2):
        fields = mm(table, spectrum(x)).T
        for k in range(2):
            rows = fields[96 * k : 96 * k + 96]
            field_ref[0, x + k] = dense_of(rows[:, :96])
            field_ref[1, x + k] = dense_of(rows[:, 128:224])
    fetch.wait()
    for x in range(XS):
        one, two = field_ref[0, x], field_ref[1, x]
        theirs = [plane(their_ref, x, o) for o in range(2)]
        first = jnp.where(upper, theirs[1], theirs[0])
        second = jnp.where(upper, theirs[0], theirs[1])
        kept = [one * first, two * second]
        mine_one = one * plane(own_ref, x, 0) * weight[0]
        mine_two = two * plane(own_ref, x, 1) * weight[1]
        sent = [jnp.where(upper, mine_two, mine_one), jnp.where(upper, mine_one, mine_two)]
        for o in range(2):
            for tile in range(3):
                place = pl.ds(144 * x + o + 2 * tile, 24, stride=6)
                kept_ref[place, :] = kept[o][:, 128 * tile : 128 * tile + 128]
                sent_ref[place, :] = sent[o][:, 128 * tile : 128 * tile + 128]
    sent_ref[864:872, :] = facts_ref[...]


def sum_kernel(kept_ref, come_ref, out_hbm, out_ref, sems, *, mask):
    upper = is_upper(mask)
    odd_row = lax.broadcasted_iota(jnp.int32, (216, 128), 0) % 2 == 1
    even = jnp.where(upper, come_ref[865:866, :], come_ref[864:865, :])
    odd = jnp.where(upper, come_ref[864:865, :], come_ref[865:866, :])
    weight = jnp.where(odd_row, odd, even)
    outs = []
    for k in range(4):
        place = pl.ds(216 * k, 216)
        out_ref[place, :] = -(kept_ref[place, :] * weight + come_ref[place, :])
        outs.append(pltpu.make_async_copy(out_ref.at[place], out_hbm.at[place], sems.at[k]))
        outs[-1].start()
    for copy in outs:
        copy.wait()


def same_kernel(in_hbm, out_hbm):
    pass


SMEM = pl.BlockSpec(memory_space=pltpu.SMEM)
VMEM = pl.BlockSpec(memory_space=pltpu.VMEM)
HBM = pl.BlockSpec(memory_space=pltpu.HBM)


def call(kernel, ins, outs, args, scratch=(), out_spec=VMEM, limit=28_000_000, alias=None):
    shapes = [o if isinstance(o, jax.ShapeDtypeStruct) else jax.ShapeDtypeStruct(o, jnp.float32) for o in outs]
    many = len(shapes) > 1
    return pl.pallas_call(
        kernel,
        out_shape=shapes if many else shapes[0],
        in_specs=ins,
        out_specs=(out_spec if isinstance(out_spec, list) else [out_spec] * len(outs)) if many else out_spec,
        scratch_shapes=scratch,
        input_output_aliases=alias or {},
        compiler_params=pltpu.CompilerParams(vmem_limit_bytes=limit),
    )(*args)


def to_partner(value, pair_bits, then, *others):
    group_count = lax.axis_size("grp")

    def by_mask(mask):
        pairs = [(source, source ^ mask) for source in range(group_count)]
        return lambda given: then(mask, lax.ppermute(given[0], "grp", pairs), *given[1:])

    branches = [by_mask(mask) for mask in range(1, group_count)]
    return lax.switch(pair_bits - 1, branches, (value, *others))


def to_rows(planes):
    return planes.reshape(2, XS, 72, 128).transpose(1, 2, 0, 3).reshape(864, 128)


def from_rows(rows):
    return rows.reshape(XS, 72, 2, 128).transpose(2, 0, 1, 3).reshape(2, XS, G * G)


def exchange(chunks):
    chunks = chunks.reshape(SLABS, ROWS, 128)
    moved = lax.all_to_all(chunks, "slab", split_axis=0, concat_axis=0, tiled=True)
    return moved.reshape(SLABS * ROWS, 128)


def fold_kernel(fold_ref, hat_ref, out_ref):
    def one_group(q, carry):
        rest = hat_ref[q]
        total = jnp.zeros((200, 4 * N), jnp.float32)
        for _ in range(3):
            part = rest.astype(jnp.bfloat16)
            rest = rest - part.astype(jnp.float32)
            total = total + lax.dot_general(
                fold_ref[...], part, (((1,), (1,)), ((), ())), preferred_element_type=jnp.float32
            )
        out_ref[q] = total
        return carry

    lax.fori_loop(0, 3, one_group, 0)


def fold_table():
    table = np.zeros((200, N), np.float32)
    for k in range(1, G):
        table[k, k] = table[k, N - k] = 1.0
        table[G + k, k], table[G + k, N - k] = 1.0, -1.0
    table[0, 0] = table[N, G] = 1.0
    return table


def local(orbitals, occupation, kernel_hat, pair_mask):
    tz, lines_table, tv = [jnp.asarray(t) for t in tables()]
    pair_bits = pair_mask[0]
    own = to_rows(orbitals)
    chunk = (SLABS * ROWS, 128)
    rows = pltpu.VMEM((864, 128), jnp.float32)

    def spread_out(mask, theirs, own, occupation, tz, kernel_hat, fold):
        near = [jax.ShapeDtypeStruct(a.shape, a.dtype) for a in (own, tz)]
        own, tz, facts = call(
            functools.partial(near_kernel, mask=mask),
            [SMEM, HBM, HBM],
            near + [(8, 128)],
            (occupation, own, tz),
            [pltpu.SemaphoreType.DMA((2,))],
        )
        kernel = functools.partial(spread_kernel, mask=mask)
        outs = [(864, 128), chunk]
        scratch = [pltpu.SemaphoreType.DMA]
        spread = call(kernel, [VMEM] * 3, outs, (own, theirs, tz), scratch, [HBM, VMEM])
        lines = kernel_hat.reshape(3, 4 * N, N)
        hat = call(fold_kernel, [VMEM] * 2, [(3, 200, 4 * N)], (fold, lines))
        return *spread, facts, hat

    fold = jnp.asarray(fold_table(), jnp.bfloat16)
    theirs, spread, facts, hat = to_partner(
        own, pair_bits, spread_out, own, occupation, tz, kernel_hat, fold
    )
    scratch = [pltpu.VMEM((3, 2, G, 4 * N), jnp.float32)] * 2
    scratch += [pltpu.VMEM((3, 200, 4 * N), jnp.float32)]
    scratch += [pltpu.VMEM(lines_table.shape, lines_table.dtype), pltpu.SemaphoreType.DMA((4,))]
    lined = call(
        line_kernel,
        [VMEM, HBM, HBM],
        [chunk],
        (exchange(spread), hat, lines_table),
        scratch,
        limit=53_300_000,
    )
    back = exchange(lined)
    kept, sent = call(
        term_kernel,
        [VMEM, VMEM, HBM, VMEM, VMEM],
        [(864, 128), (872, 128)],
        (back, own, theirs, facts, tv),
        [rows, pltpu.VMEM((2, XS, 24, 384), jnp.float32), pltpu.SemaphoreType.DMA],
    )

    def total(mask, come, kept):
        kernel = functools.partial(sum_kernel, mask=mask)
        scratch = [rows, pltpu.SemaphoreType.DMA((4,))]
        return call(kernel, [VMEM] * 2, [(864, 128)], (kept, come), scratch, HBM)

    out = to_partner(sent, pair_bits, total, kept)
    return from_rows(
        call(same_kernel, [HBM], [(864, 128)], (out,), (), HBM, limit=66_800_000, alias={0: 0})
    )


def solution(mesh):
    return jax.shard_map(
        local,
        mesh=mesh,
        in_specs=(P("grp", "slab", None), P("grp"), P("slab", None), P()),
        out_specs=P("grp", "slab", None),
        check_vma=False,
    )
```

```python
import functools
import math

import jax
import jax.numpy as jnp
import numpy as np
from jax import lax
from jax.experimental import pallas as pl
from jax.experimental.pallas import tpu as pltpu
from jax.sharding import PartitionSpec as P

G = 96
N = 192
SLABS = 16
XS = 6
KP = 6
ROWS = 112

Y_ORDER = np.array([4 * (i % 24) + i // 24 for i in range(G)])
X_ORDER = np.array([6 * (i % SLABS) + i // SLABS for i in range(G)])


WY, WI, TX, TI, LINES = 0, 640, 1280, 1472, 1664


def split(table):
    table = jnp.asarray(table, jnp.float32)
    high = table.astype(jnp.bfloat16)
    low = (table - high.astype(jnp.float32)).astype(jnp.bfloat16)
    return high, low


def np_split(table):
    bf16 = jnp.bfloat16
    high = table.astype(np.float32).astype(bf16)
    low = (table - high.astype(np.float64)).astype(np.float32).astype(bf16)
    return np.stack([high, low])


def waves(freq, cell):
    angle = (np.outer(freq, cell) % N) * (2.0 * math.pi / N)
    return np.cos(angle), np.sin(angle)


@functools.cache
def tables():
    pair_major = np.array([[12 * d + 2 * kp for d in range(SLABS)] for kp in range(KP)]).reshape(-1)
    tz = np.zeros((384, 256))
    tv = np.zeros((256, 384))
    wy = np.zeros((640, 256))
    wi = np.zeros((640, 256))
    for kz2 in range(2):
        cos, sin = waves(pair_major + kz2, np.arange(G))
        re, im = 192 * kz2, 192 * kz2 + 96
        tz[re : re + 96, 0:96], tz[re : re + 96, 128:224] = cos, sin
        tz[im : im + 96, 0:96], tz[im : im + 96, 128:224] = -sin, cos
        tv[0:96, re : re + 96], tv[0:96, im : im + 96] = cos.T / N, -sin.T / N
        tv[128:224, re : re + 96], tv[128:224, im : im + 96] = sin.T / N, cos.T / N
    cos, sin = waves(Y_ORDER, np.arange(N))
    wy[64:160, :N], wy[160:256, :N] = cos, sin
    wy[384:480, :N], wy[480:576, :N] = -sin, cos
    wi[64:256, 0:96], wi[64:256, 96:192] = cos.T / N, sin.T / N
    wi[384:576, 0:96], wi[384:576, 96:192] = -sin.T / N, cos.T / N
    cos, sin = waves(np.arange(G), X_ORDER)
    sin[0] = waves(np.array([G]), X_ORDER)[0][0]
    tx = np.concatenate([cos, sin], axis=0)
    ti = np.block([[cos.T, -sin.T], [cos.T, sin.T]]) / N
    lines = [wy, wi, widened(tx), widened(ti)]
    return [np_split(t) for t in (tz, np.concatenate(lines, axis=0), tv)]


def widened(table):
    return np.pad(table, ((0, 0), (0, 256 - table.shape[1])))


def mm(left, right, form=(1, 0)):
    def one(a, b):
        return lax.dot_general(
            a, b, (((form[0],), (form[1],)), ((), ())), preferred_element_type=jnp.float32
        )

    return one(left[0], right[0]) + (one(left[0], right[1]) + one(left[1], right[0]))


def plane(ref, x, orbital):
    base = 144 * x + orbital
    tiles = [ref[pl.ds(base + 2 * tile, 24, stride=6), :] for tile in range(3)]
    return jnp.concatenate(tiles, axis=1)


def lines(dense):
    return jnp.concatenate([dense[:, 96 * q : 96 * q + 96] for q in range(4)], axis=0)


def dense_of(rows):
    return jnp.concatenate([rows[24 * q : 24 * q + 24] for q in range(4)], axis=1)


def is_upper(mask):
    return jnp.bitwise_and(lax.axis_index("grp"), 1 << (mask.bit_length() - 1)) != 0


def near_kernel(occupation_ref, own_hbm, tz_hbm, own_ref, tz_ref, facts_ref, sems, *, mask):
    row = lax.broadcasted_iota(jnp.int32, (8, 128), 0)
    weight = [0.25 * occupation_ref[o].astype(jnp.float32) for o in range(2)]
    upper = jnp.where(is_upper(mask), 1.0, 0.0)
    facts_ref[...] = jnp.where(row == 0, weight[0], jnp.where(row == 1, weight[1], upper))
    copies = [
        pltpu.make_async_copy(own_hbm, own_ref, sems.at[0]),
        pltpu.make_async_copy(tz_hbm, tz_ref, sems.at[1]),
    ]
    for copy in copies:
        copy.start()
    for copy in copies:
        copy.wait()


def spread_kernel(
    own_ref, their_ref, tz_ref, their_hbm, out_ref, their_sem, *, mask
):
    kept = pltpu.make_async_copy(their_ref, their_hbm, their_sem)
    kept.start()
    upper = is_upper(mask)
    pad = jnp.zeros((G, 32), jnp.float32)

    def density(x):
        theirs = [plane(their_ref, x, o) for o in range(2)]
        first = jnp.where(upper, theirs[1], theirs[0])
        second = jnp.where(upper, theirs[0], theirs[1])
        one = lines(plane(own_ref, x, 0) * first)
        two = lines(plane(own_ref, x, 1) * second)
        return split(jnp.concatenate([one, pad, two, pad], axis=1))

    def spectra(x):
        parts = [density(x), density(x + 1)]
        both = [jnp.concatenate([part[k] for part in parts], axis=0) for k in range(2)]
        return mm((tz_ref[0], tz_ref[1]), both, (1, 1))

    def stored(x, lined):
        wide = jnp.concatenate([lined[96 * j : 96 * j + 96] for j in range(4)], axis=1)
        for kp in range(KP):
            for tile in range(3):
                out_ref[pl.ds(18 * x + 6 * tile + kp, SLABS, stride=ROWS), :] = wide[
                    16 * kp : 16 * kp + 16, 128 * tile : 128 * tile + 128
                ]

    for slab in range(SLABS):
        out_ref[ROWS * slab + 108 : ROWS * slab + 112, :] = jnp.zeros((4, 128), jnp.float32)
    for x in range(0, XS, 2):
        lined = spectra(x)
        stored(x, lined[:, :96])
        stored(x + 1, lined[:, 96:192])
    kept.wait()


def side_by_side(left, right):
    right = pltpu.roll(right, 64, 1)
    return jnp.concatenate(
        [left[:, :128], left[:, 128:] + right[:, :128], right[:, 128:]], axis=1
    )


def line_kernel(in_ref, hat_hbm, table_hbm, out_ref, y_ref, u_ref, hat_ref, table_ref, sems):
    fetches = []
    for row, count in ((WY, WI - WY), (TX, LINES - TX), (WI, TX - WI)):
        place = (slice(None), pl.ds(row, count))
        pair = (table_hbm.at[place], table_ref.at[place])
        fetches.append(pltpu.make_async_copy(*pair, sems.at[len(fetches)]))
    fetches.insert(2, pltpu.make_async_copy(hat_hbm, hat_ref, sems.at[3]))
    for copy in fetches:
        copy.start()

    def table(row, count, columns=256):
        return [table_ref[part, row : row + count, :columns] for part in range(2)]

    def gathered(kps):
        pieces = []
        for kp in kps:
            for x in range(XS):
                place = [pl.ds(18 * x + 6 * tile + kp, SLABS, stride=ROWS) for tile in range(3)]
                pieces.append(jnp.concatenate([in_ref[p, :] for p in place], axis=1))
        return split(jnp.concatenate(pieces, axis=0))

    def y_forward(q, data):
        for c in range(2):
            result = []
            for kz2 in range(2):
                window = [part[:, 128 * kz2 : 128 * kz2 + 256] for part in data]
                result.append(mm(window, table(WY + 320 * c + 64 * (1 - kz2), 256)))
            paired = side_by_side(*result)
            for half in range(2):
                y_ref[q, c, :, 384 * half : 384 * half + 384] = paired[96 * half : 96 * half + 96]

    data = gathered((0, 1))
    fetches[0].wait()
    for q in range(3):
        coming = gathered((2 * q + 2, 2 * q + 3)) if q < 2 else None
        y_forward(q, data)
        data = coming
    for copy in fetches[1:]:
        copy.wait()
    first_row = lax.broadcasted_iota(jnp.int32, (G, 256), 0) == 0
    forward = table(TX, N, G)

    def spectra(i):
        q, hl = places[i]
        return [mm(forward, split(y_ref[q, c, :, hl])) for c in range(2)]

    def multiplied(i, re, im):
        q, hl = places[i]
        even, odd = hat_ref[q, :G, hl], hat_ref[q, G:N, hl]
        even_sin = jnp.where(first_row, hat_ref[q, N : N + 1, hl], even)
        cos_re = even * re[:G] + odd * im[G:]
        sin_im = odd * im[:G] - even_sin * re[G:]
        cos_im = even * im[:G] - odd * re[G:]
        sin_re = odd * re[:G] + even_sin * im[G:]
        return (
            split(jnp.concatenate([cos_re, sin_im], axis=0)),
            split(jnp.concatenate([cos_im, sin_re], axis=0)),
        )

    def back(i, first, second):
        q, hl = places[i]
        u_ref[q, 0, :, hl] = mm(table(TI, G, N), first)
        u_ref[q, 1, :, hl] = mm(table(TI + G, G, N), second)

    def y_back(q):
        sides = []
        for kz2 in range(2):
            parts = []
            for c in range(2):
                lane = [384 * half + 128 * kz2 for half in range(2)]
                rows = [u_ref[q, c, :, first : first + 256] for first in lane]
                window = split(jnp.concatenate(rows, axis=0))
                parts.append(mm(window, table(WI + 320 * c + 64 * (1 - kz2), 256)))
            sides.append(parts[0] + parts[1])
        wide = side_by_side(*sides)
        for half in range(2):
            for x in range(XS):
                row = 96 * half + 16 * x
                for tile in range(3):
                    place = pl.ds(18 * x + 6 * tile + 2 * q + half, SLABS, stride=ROWS)
                    out_ref[place, :] = wide[row : row + 16, 128 * tile : 128 * tile + 128]

    places = [(q, slice(w, w + 256)) for q in range(3) for w in range(0, 768, 256)]
    ahead = [spectra(i) for i in range(2)]
    for i in range(len(places)):
        product = multiplied(i, *ahead.pop(0))
        if i + 2 < len(places):
            ahead.append(spectra(i + 2))
        back(i, *product)
    for q in range(3):
        y_back(q)


def term_kernel(
    in_ref, own_ref, their_hbm, facts_ref, tv_ref, kept_ref, sent_ref, their_ref,
    field_ref, sem
):
    fetch = pltpu.make_async_copy(their_hbm, their_ref, sem)
    fetch.start()
    upper = facts_ref[2:3, :1] > 0.5
    table = (tv_ref[0], tv_ref[1])
    weight = [facts_ref[o : o + 1, :1] for o in range(2)]

    def gathered(x):
        pieces = [
            jnp.concatenate(
                [
                    in_ref[pl.ds(18 * x + 6 * tile + kp, SLABS, stride=ROWS), :]
                    for tile in range(3)
                ],
                axis=1,
            )
            for kp in range(KP)
        ]
        return jnp.concatenate(pieces, axis=0)

    def spectrum(x):
        pair = (gathered(x), gathered(x + 1))
        lanes = [slice(96 * j, 96 * j + 96) for j in range(4)]
        both = [jnp.concatenate([wide[:, part] for wide in pair], axis=1) for part in lanes]
        return split(jnp.concatenate(both, axis=0))

    for x in range(0, XS, 2):
        fields = mm(table, spectrum(x)).T
        for k in range(2):
            rows = fields[96 * k : 96 * k + 96]
            field_ref[0, x + k] = dense_of(rows[:, :96])
            field_ref[1, x + k] = dense_of(rows[:, 128:224])
    fetch.wait()
    for x in range(XS):
        one, two = field_ref[0, x], field_ref[1, x]
        theirs = [plane(their_ref, x, o) for o in range(2)]
        first = jnp.where(upper, theirs[1], theirs[0])
        second = jnp.where(upper, theirs[0], theirs[1])
        kept = [one * first, two * second]
        mine_one = one * plane(own_ref, x, 0) * weight[0]
        mine_two = two * plane(own_ref, x, 1) * weight[1]
        sent = [jnp.where(upper, mine_two, mine_one), jnp.where(upper, mine_one, mine_two)]
        for o in range(2):
            for tile in range(3):
                place = pl.ds(144 * x + o + 2 * tile, 24, stride=6)
                kept_ref[place, :] = kept[o][:, 128 * tile : 128 * tile + 128]
                sent_ref[place, :] = sent[o][:, 128 * tile : 128 * tile + 128]
    sent_ref[864:872, :] = facts_ref[...]


def sum_kernel(kept_ref, come_ref, out_hbm, out_ref, sems, *, mask):
    upper = is_upper(mask)
    odd_row = lax.broadcasted_iota(jnp.int32, (216, 128), 0) % 2 == 1
    even = jnp.where(upper, come_ref[865:866, :], come_ref[864:865, :])
    odd = jnp.where(upper, come_ref[864:865, :], come_ref[865:866, :])
    weight = jnp.where(odd_row, odd, even)
    outs = []
    for k in range(4):
        place = pl.ds(216 * k, 216)
        out_ref[place, :] = -(kept_ref[place, :] * weight + come_ref[place, :])
        outs.append(pltpu.make_async_copy(out_ref.at[place], out_hbm.at[place], sems.at[k]))
        outs[-1].start()
    for copy in outs:
        copy.wait()


def same_kernel(in_hbm, out_hbm):
    pass


SMEM = pl.BlockSpec(memory_space=pltpu.SMEM)
VMEM = pl.BlockSpec(memory_space=pltpu.VMEM)
HBM = pl.BlockSpec(memory_space=pltpu.HBM)


def call(kernel, ins, outs, args, scratch=(), out_spec=VMEM, limit=28_000_000, alias=None):
    shapes = [o if isinstance(o, jax.ShapeDtypeStruct) else jax.ShapeDtypeStruct(o, jnp.float32) for o in outs]
    many = len(shapes) > 1
    return pl.pallas_call(
        kernel,
        out_shape=shapes if many else shapes[0],
        in_specs=ins,
        out_specs=(out_spec if isinstance(out_spec, list) else [out_spec] * len(outs)) if many else out_spec,
        scratch_shapes=scratch,
        input_output_aliases=alias or {},
        compiler_params=pltpu.CompilerParams(vmem_limit_bytes=limit),
    )(*args)


def to_partner(value, pair_bits, then, *others):
    group_count = lax.axis_size("grp")

    def by_mask(mask):
        pairs = [(source, source ^ mask) for source in range(group_count)]
        return lambda given: then(mask, lax.ppermute(given[0], "grp", pairs), *given[1:])

    branches = [by_mask(mask) for mask in range(1, group_count)]
    return lax.switch(pair_bits - 1, branches, (value, *others))


def to_rows(planes):
    return planes.reshape(2, XS, 72, 128).transpose(1, 2, 0, 3).reshape(864, 128)


def from_rows(rows):
    return rows.reshape(XS, 72, 2, 128).transpose(2, 0, 1, 3).reshape(2, XS, G * G)


def exchange(chunks):
    chunks = chunks.reshape(SLABS, ROWS, 128)
    moved = lax.all_to_all(chunks, "slab", split_axis=0, concat_axis=0, tiled=True)
    return moved.reshape(SLABS * ROWS, 128)


def fold_kernel(fold_ref, hat_ref, out_hbm, out_ref, sem):
    def one_group(q, carry):
        rest = hat_ref[q]
        total = jnp.zeros((200, 4 * N), jnp.float32)
        for _ in range(3):
            part = rest.astype(jnp.bfloat16)
            rest = rest - part.astype(jnp.float32)
            total = total + lax.dot_general(
                fold_ref[...], part, (((1,), (1,)), ((), ())), preferred_element_type=jnp.float32
            )
        out_ref[q] = total
        return carry

    lax.fori_loop(0, 3, one_group, 0)
    copy = pltpu.make_async_copy(out_ref, out_hbm, sem)
    copy.start()
    copy.wait()


def fold_table():
    table = np.zeros((200, N), np.float32)
    for k in range(1, G):
        table[k, k] = table[k, N - k] = 1.0
        table[G + k, k], table[G + k, N - k] = 1.0, -1.0
    table[0, 0] = table[N, G] = 1.0
    return table


def local(orbitals, occupation, kernel_hat, pair_mask):
    tz, lines_table, tv = [jnp.asarray(t) for t in tables()]
    pair_bits = pair_mask[0]
    own = to_rows(orbitals)
    chunk = (SLABS * ROWS, 128)
    rows = pltpu.VMEM((864, 128), jnp.float32)

    def spread_out(mask, theirs, own, occupation, tz, kernel_hat, fold):
        near = [jax.ShapeDtypeStruct(a.shape, a.dtype) for a in (own, tz)]
        own, tz, facts = call(
            functools.partial(near_kernel, mask=mask),
            [SMEM, HBM, HBM],
            near + [(8, 128)],
            (occupation, own, tz),
            [pltpu.SemaphoreType.DMA((2,))],
        )
        kernel = functools.partial(spread_kernel, mask=mask)
        outs = [(864, 128), chunk]
        scratch = [pltpu.SemaphoreType.DMA]
        spread = call(kernel, [VMEM] * 3, outs, (own, theirs, tz), scratch, [HBM, VMEM])
        lines = kernel_hat.reshape(3, 4 * N, N)
        hat_shape = (3, 200, 4 * N)
        scratch = [pltpu.VMEM(hat_shape, jnp.float32), pltpu.SemaphoreType.DMA]
        hat = call(
            fold_kernel, [VMEM] * 2, [hat_shape], (fold, lines), scratch, HBM, limit=66_800_000
        )
        return *spread, facts, hat

    fold = jnp.asarray(fold_table(), jnp.bfloat16)
    theirs, spread, facts, hat = to_partner(
        own, pair_bits, spread_out, own, occupation, tz, kernel_hat, fold
    )
    scratch = [pltpu.VMEM((3, 2, G, 4 * N), jnp.float32)] * 2
    scratch += [pltpu.VMEM((3, 200, 4 * N), jnp.float32)]
    scratch += [pltpu.VMEM(lines_table.shape, lines_table.dtype), pltpu.SemaphoreType.DMA((4,))]
    lined = call(
        line_kernel,
        [VMEM, HBM, HBM],
        [chunk],
        (exchange(spread), hat, lines_table),
        scratch,
        limit=53_300_000,
    )
    back = exchange(lined)
    kept, sent = call(
        term_kernel,
        [VMEM, VMEM, HBM, VMEM, VMEM],
        [(864, 128), (872, 128)],
        (back, own, theirs, facts, tv),
        [rows, pltpu.VMEM((2, XS, 24, 384), jnp.float32), pltpu.SemaphoreType.DMA],
    )

    def total(mask, come, kept):
        kernel = functools.partial(sum_kernel, mask=mask)
        scratch = [rows, pltpu.SemaphoreType.DMA((4,))]
        return call(kernel, [VMEM] * 2, [(864, 128)], (kept, come), scratch, HBM)

    out = to_partner(sent, pair_bits, total, kept)
    return from_rows(
        call(same_kernel, [HBM], [(864, 128)], (out,), (), HBM, limit=66_800_000, alias={0: 0})
    )


def solution(mesh):
    return jax.shard_map(
        local,
        mesh=mesh,
        in_specs=(P("grp", "slab", None), P("grp"), P("slab", None), P()),
        out_specs=P("grp", "slab", None),
        check_vma=False,
    )
```
